32 devices in a mesh: groups: 2 (over y), dp: 4 (over z), section: 2 (over x), tensor: 2 (over core).
Axes of the slice: x: 2, y: 2, z: 4, core: 2. Of those that a mesh axis runs over, the one named last changes fastest.
Arguments:
- hidden: bfloat16 [128, 8, 5120], P(('groups', 'dp')), parts along dimension 0, may hold values from -6 to 6
- unembed: bfloat16 [128, 8, 5120], P(('groups', 'dp')), parts along dimension 0, may hold values from -0.02734375 to 0.02734375
- value_proj: bfloat16 [2, 5120, 512], P('section', 'dp', 'tensor'), may hold values from -0.078125 to 0.078125
- output_proj: bfloat16 [2, 512, 5120], P('section', 'tensor', 'dp'), may hold values from -0.125 to 0.125
- norm_gains: float32 [2, 5120], P('section'), may hold values from 0.1 to 1.9
- survive: int32 [8], P(('groups', 'dp')), parts along dimension 0, may hold values from 0 to 1, as said below
- lengths: int32 [128], P(('groups', 'dp')), parts along dimension 0, may hold values from 1 to 8
- assign: int32 [128], P(('groups', 'dp')), parts along dimension 0, may hold values from 0 to 16, as said below
- advantage: float32 [128], P(('groups', 'dp')), parts along dimension 0, may hold values from -4 to 4
- reference_logit: float32 [128, 8], P(('groups', 'dp')), parts along dimension 0, may hold values from -4 to 4
- recorded_gap: float32 [128, 8], P(('groups', 'dp')), parts along dimension 0, may hold values from -2 to 2
Outputs:
- grad_value: float32 [4, 5120, 512], P(('groups', 'section'), 'dp', 'tensor'), parts along dimension 0
- grad_output: float32 [4, 512, 5120], P(('groups', 'section'), 'tensor', 'dp'), parts along dimension 0
The draws below stay inside these ranges and needn't reach their ends.
There are 2 independent parts, one for each index of `groups`. The reference program is written for one: setup_inputs(seed, part) draws one part's arguments, and reference() takes and returns one part's arrays. A program takes and returns all parts, laid end to end along the dimension named above; an argument that names none is the same for every part. Nothing has to cross between parts.
Inputs may be any that keep to these rules, and one draw needn't show every extreme that they name: `survive`: 1 where the group of 16 responses is kept, 0 where it is dropped; in every draw all groups of some dp index are kept. `assign`: the 16 slots of a dp index list the local positions (0 to 15) of the responses of its kept groups, each exactly once, then hold 16 in every other slot.
All inputs are finite; a program needn't handle non-finite values.
Results may differ from the reference program's by a relative error of at most 0.029.
Values may be sent and summed in bfloat16 or wider, within the bound.
A program may use at most 64 MiB of HBM per device.

```python
import math
import jax
import jax.numpy as jnp
from jax import lax

D = 5120
VALUE_W = 512
GROUP = 16
GROUPS_DEV = 1
LMAX = 8
LAYERS = 2
RESP_DEV = 16
RESPONSES = 64
GROUPS = 4
N_DP = 4
N_TENSOR = 2


def survival_plan(key):
    base = jax.random.fold_in(key, 17)
    roll_key, force_key, order_key = jax.random.split(base, 3)
    device = jnp.arange(GROUPS, dtype=jnp.int32) // GROUPS_DEV
    threshold = 300 + 700 * device // max(N_DP - 1, 1)
    survival_roll = jax.random.randint(roll_key, (GROUPS,), 0, 1000)
    forced = jax.random.randint(force_key, (), 0, N_DP)
    alive_mask = ((survival_roll < threshold) | (device == forced)).astype(jnp.int32)
    return (alive_mask, order_key)


def draw_survive(key, part):
    alive_mask, order_key = survival_plan(key)
    return alive_mask


def draw_assign(key, part):
    alive_mask, order_key = survival_plan(key)
    per_device = jnp.repeat(alive_mask, GROUP).reshape(N_DP, RESP_DEV)
    subkeys = jax.random.split(order_key, N_DP)
    priority = jax.vmap(lambda subkey: jax.random.permutation(subkey, RESP_DEV))(subkeys).astype(jnp.int32)
    sort_key = (1 - per_device) * RESP_DEV + priority
    slot_order = jnp.argsort(sort_key, axis=1, stable=True).astype(jnp.int32)
    alive_count = jnp.sum(per_device, axis=1, keepdims=True)
    slot_index = lax.broadcasted_iota(jnp.int32, (N_DP, RESP_DEV), 1)
    return jnp.where(slot_index < alive_count, slot_order, RESP_DEV).astype(jnp.int32).reshape(RESPONSES)


def set_ends(drawn, rng, low, high):
    extent = drawn.shape
    spot = [jax.random.randint(jax.random.fold_in(rng, axis), (), 0, extent[axis]) for axis in range(len(extent))]
    drawn = drawn.at[tuple(spot)].set(low)
    longest = extent.index(max(extent))
    spot[longest] = (spot[longest] + 1) % extent[longest]
    return drawn.at[tuple(spot)].set(high)


def with_spikes(values, rng, source, target, parts, factor):
    owner, partner = [(jnp.arange(values.shape[axis_at]) // (values.shape[axis_at] // parts)).reshape([-1 if axis == axis_at else 1 for axis in range(values.ndim)]) for axis_at in (source, target)]
    chosen = jax.random.permutation(rng, parts)[partner]
    strong = (owner == chosen) | (owner == (partner + parts // 2) % parts)
    return jnp.where(strong, factor * values, values)


def shard_levels(own_key, shape, cuts, least, top_value):
    gain, own = 1.0, jax.random.fold_in(own_key, 6)
    for position, parts in cuts:
        heights = jnp.exp(jax.random.uniform(jax.random.fold_in(own, position), (parts,), jnp.float32, least / len(cuts), top_value / len(cuts)))
        gain = gain * jnp.repeat(heights, shape[position] // parts).reshape([-1 if axis == position else 1 for axis in range(len(shape))])
    return gain


def normal_values(own_key, dims, scale, limit, cuts=(), held_as=jnp.bfloat16):
    result = jax.random.normal(own_key, dims, jnp.float32) * scale
    if len(cuts) > 0:
        result = shard_levels(own_key, dims, cuts, -0.22, 0.18) * result
    return jnp.clip(result, min=-limit, max=limit).astype(held_as)


def heavy_noise(key, shape, scale, most, cuts, heavy, held_as=jnp.bfloat16):
    entries = scale * jax.random.normal(key, shape, jnp.float32)
    if cuts:
        entries = entries * shard_levels(key, shape, cuts, -0.22, 0.18)
    return jnp.clip(with_spikes(entries, jax.random.fold_in(key, 3), *heavy), -most, most).astype(held_as)


def setup_inputs(seed: int = 0, part: int = 0) -> dict:
    key_list = jax.random.split(jax.random.key(seed), 12)
    own_keys = jax.random.split(jax.random.fold_in(key_list[11], part), 12)
    return {
        "hidden": heavy_noise(own_keys[0], (RESPONSES, LMAX, D), 1.0, 6.0, ((0, 4),), (0, 2, 4, 2.0)),
        "unembed": normal_values(own_keys[1], (RESPONSES, LMAX, D), (10 * D) ** -0.5, 0.02734375, ((0, 4),)),
        "value_proj": normal_values(key_list[2], (LAYERS, D, VALUE_W), D ** -0.5, 0.078125, ((0, 2), (1, 4), (2, 2))),
        "output_proj": normal_values(key_list[3], (LAYERS, VALUE_W, D), (4 * VALUE_W) ** -0.5, 0.125, ((0, 2), (1, 2), (2, 4))),
        "norm_gains": jnp.clip(1.0 + 0.18 * jax.random.normal(key_list[4], (LAYERS, D), jnp.float32), 0.1, 1.9),
        "survive": draw_survive(jax.random.fold_in(jax.random.fold_in(key_list[11], part), 71), part),
        "lengths": set_ends(jax.random.randint(own_keys[6], (RESPONSES,), 1, LMAX + 1), jax.random.fold_in(own_keys[6], 1), 1, LMAX).astype(jnp.int32),
        "assign": draw_assign(jax.random.fold_in(jax.random.fold_in(key_list[11], part), 71), part),
        "advantage": normal_values(own_keys[8], (RESPONSES,), 1.0, 4.0, ((0, 4),), jnp.float32),
        "reference_logit": normal_values(own_keys[9], (RESPONSES, LMAX), 0.7, 4.0, ((0, 4),), jnp.float32),
        "recorded_gap": normal_values(own_keys[10], (RESPONSES, LMAX), 0.3, 2.0, ((0, 4),), jnp.float32),
    }


eps_norm = 1e-06
loss_scale = 4096.0
clip_high = math.log(1.28)
clip_low = math.log(0.8)

def norm_forward(row_block, norm_gain):
    values = row_block.astype(jnp.float32)
    inverse = lax.rsqrt(lax.optimization_barrier(jnp.mean(values * values, axis=-1, keepdims=True)) + eps_norm)
    return (values, inverse, (values * inverse * norm_gain).astype(jnp.bfloat16))

def norm_backward(values, inverse, norm_gain, upstream):
    scaled = upstream * norm_gain
    inner_sum = lax.optimization_barrier(jnp.sum(scaled * values, axis=-1, keepdims=True)) / values.shape[-1]
    return inverse * scaled - values * (inverse * inverse * inverse) * inner_sum

def contract_last(left_rows, right_rows):
    return lax.dot_general(left_rows, right_rows, (((1,), (1,)), ((), ())), preferred_element_type=jnp.float32)

def rounded(partial_piece):
    return lax.optimization_barrier(partial_piece.astype(jnp.bfloat16)).astype(jnp.float32)

def reference(hidden, unembed, value_proj, output_proj, norm_gains, survive, lengths, assign, advantage, reference_logit, recorded_gap):
    owner_index = jnp.arange(RESPONSES, dtype=jnp.int32) // RESP_DEV
    chosen = jnp.where(assign >= RESP_DEV, RESPONSES, assign + owner_index * RESP_DEV).astype(jnp.int32)

    def pick(array):
        return jnp.take(array, chosen, axis=0, mode='fill', fill_value=0)
    row_count = RESPONSES * LMAX
    block_width = VALUE_W // N_TENSOR
    current = pick(hidden).reshape(row_count, D)
    unembed_rows = pick(unembed).reshape(row_count, D).astype(jnp.float32)
    positions = lax.broadcasted_iota(jnp.int32, (RESPONSES, LMAX), 1)
    live_mask = (positions < pick(lengths)[:, None]).astype(jnp.float32)
    advantages = jnp.broadcast_to(pick(advantage)[:, None], (RESPONSES, LMAX))
    gap_rows = pick(recorded_gap)
    clipped = (advantages > 0) & (gap_rows > clip_high) | (advantages < 0) & (gap_rows < clip_low)
    kept_mask = 1.0 - clipped.astype(jnp.float32)
    alive_mask = jnp.repeat(survive, GROUP)
    token_count = jnp.sum((alive_mask * lengths).astype(jnp.float32))
    weight_rows = (-loss_scale * advantages * kept_mask * live_mask).reshape(row_count)
    logit_base = pick(reference_logit).reshape(row_count)
    saved = []
    for layer_index in range(LAYERS):
        values, inverse, normed = norm_forward(current, norm_gains[layer_index])
        projected = jnp.dot(normed, value_proj[layer_index], preferred_element_type=jnp.float32).astype(jnp.bfloat16)
        mixed_sum = jnp.zeros((row_count, D), jnp.float32)
        for tensor_part in range(N_TENSOR):
            low = tensor_part * block_width
            partial_piece = jnp.dot(projected[:, low:low + block_width], output_proj[layer_index, low:low + block_width, :], preferred_element_type=jnp.float32)
            mixed_sum = mixed_sum + rounded(partial_piece)
        saved.append((current, normed, projected))
        current = (values + mixed_sum).astype(jnp.bfloat16)
    top_rows = current.astype(jnp.float32)
    logit = lax.optimization_barrier(jnp.sum(top_rows * unembed_rows, axis=-1))
    seed_rows = weight_rows * jnp.exp(logit - logit_base)
    upstream = (seed_rows[:, None] * unembed_rows).astype(jnp.bfloat16)
    grads_value = [None] * LAYERS
    grads_output = [None] * LAYERS
    for layer_index in reversed(range(LAYERS)):
        entering, normed, projected = saved[layer_index]
        grad_projected = contract_last(upstream, output_proj[layer_index]).astype(jnp.bfloat16)
        grad_normed = jnp.zeros((row_count, D), jnp.float32)
        for tensor_part in range(N_TENSOR):
            low = tensor_part * block_width
            partial_piece = contract_last(grad_projected[:, low:low + block_width], value_proj[layer_index][:, low:low + block_width])
            grad_normed = grad_normed + rounded(partial_piece)
        grads_value[layer_index] = jnp.dot(normed.T, grad_projected, preferred_element_type=jnp.float32) / token_count
        grads_output[layer_index] = jnp.dot(projected.T, upstream, preferred_element_type=jnp.float32) / token_count
        values, inverse, unused_normed = norm_forward(entering, norm_gains[layer_index])
        upstream = (upstream.astype(jnp.float32) + norm_backward(values, inverse, norm_gains[layer_index], grad_normed)).astype(jnp.bfloat16)
    return (jnp.stack(grads_value), jnp.stack(grads_output))
```

```python
import functools
import math

import jax
import jax.numpy as jnp
from jax import lax
from jax.experimental import pallas as pl
from jax.experimental.pallas import tpu as pltpu
from jax.sharding import PartitionSpec as P

eps_norm = 1e-06
loss_scale = 4096.0
clip_high = math.log(1.28)
clip_low = math.log(0.8)
LANES = 128
KINDS = ("a", "xf", "uf", "p", "q", "pj", "pjf", "gq", "gqf", "sc", "tk", "x", "g", "w", "e", "ps")
BF = jnp.bfloat16
F32 = jnp.float32


def dot(a, b, ca=1, cb=0):
    return lax.dot_general(a, b, (((ca,), (cb,)), ((), ())), preferred_element_type=F32)


def kernel(
    n, sections, width,
    src, w1, w2, gains, survive, lengths, assign, advantage, base, gap,
    dw1, dw2,
    xs, us, xg, pb, pr, qb, qr, pj, gq, sc, w1o, w2o, yx, yg, tk, exs, exr, pacc, qacc, rkeep,
    ps, psr, rinfo, tok,
    ss, rs,
):
    j = lax.axis_index("dp")
    s = lax.axis_index("section")
    t = lax.axis_index("tensor")
    o = 1 - t
    rows = src.shape[1]
    half, v = w1.shape[1:]
    last = sections - 1
    partner = {"tensor": o}
    positions, count = base.shape

    def gain(h):
        return gains[j * 2 + h]

    def own_tokens():
        response = lax.broadcasted_iota(jnp.int32, (1, count), 1)
        group = count // survive.shape[1]
        kept = jnp.zeros((1, count), F32)
        for g in range(survive.shape[1]):
            inside = (response >= g * group) & (response < (g + 1) * group)
            kept = jnp.where(inside, survive[0:1, g:g + 1].astype(F32), kept)
        held = jnp.sum(kept * lengths[...].astype(F32), axis=1, keepdims=True)
        tok[...] = jnp.broadcast_to(held, (8, LANES))

    def row_info():
        row = lax.broadcasted_iota(jnp.int32, (rows, count), 0)
        first = lax.broadcasted_iota(jnp.int32, (rows, count), 1) * positions
        mine = (row >= first) & (row < first + positions)

        def by_response(values):
            return jnp.sum(jnp.where(mine, values, 0.0), axis=1, keepdims=True)

        def by_position(values):
            return by_response(jnp.concatenate([values] * count, axis=0))

        slots = assign[...]
        starts = slots * positions
        hit = (row >= starts) & (row < starts + positions)
        listed = jnp.sum(jnp.where(hit, 1.0, 0.0), axis=1, keepdims=True)
        start = by_response(first.astype(F32))
        place = lax.broadcasted_iota(jnp.int32, (rows, 1), 0).astype(F32) - start
        live = place < by_response(lengths[...].astype(F32))
        adv = by_response(advantage[...])
        q = by_position(gap[...])
        clipped = ((adv > 0) & (q > clip_high)) | ((adv < 0) & (q < clip_low))
        weight = jnp.where(clipped | (~live), 0.0, -loss_scale * adv * listed)
        rinfo[...] = jnp.where(lane == 0, weight, jnp.where(lane == 1, by_position(base[...]), 0.0))

    def blk(b):
        return pl.ds(pl.multiple_of(b * rows, rows), rows)

    def peer(k):
        return lax.rem(j + k, n)

    def send(kind, si, ri, a, b, dev):
        k = KINDS.index(kind)
        pltpu.make_async_remote_copy(
            src_ref=a, dst_ref=b, send_sem=ss.at[k, si], recv_sem=rs.at[k, ri],
            device_id=dev, device_id_type=pl.DeviceIdType.MESH,
        ).start()

    def handle(kind, i, a):
        k = KINDS.index(kind)
        return pltpu.make_async_remote_copy(
            src_ref=a, dst_ref=a, send_sem=ss.at[k, i], recv_sem=rs.at[k, i],
            device_id=partner, device_id_type=pl.DeviceIdType.MESH,
        )

    def got(kind, i, a):
        handle(kind, i, a).wait_recv()

    def sent(kind, i, a):
        handle(kind, i, a).wait_send()

    def others(body):
        def step(k, carry):
            body(peer(k))
            return carry
        lax.fori_loop(1, n, step, 0)

    def everyone(body):
        def step(k, carry):
            body(peer(k))
            return carry
        lax.fori_loop(0, n, step, 0)

    barrier = pltpu.get_barrier_semaphore()

    def greet(dev):
        pl.semaphore_signal(barrier, inc=1, device_id=dev, device_id_type=pl.DeviceIdType.MESH)

    for k in range(1, n):
        greet({"dp": peer(k)})
    greet(partner)

    @pl.when(s > 0)
    def _():
        greet({"section": s - 1})

    @pl.when(s < last)
    def _():
        greet({"section": s + 1})

    pl.semaphore_wait(barrier, n + jnp.where(s > 0, 1, 0) + jnp.where(s < last, 1, 0))

    def start_common():
        send("w", 0, 0, w1.at[o], w1o, partner)
        send("w", 1, 1, w2.at[o], w2o, partner)
        own_tokens()
        others(lambda b: send("tk", b, j, tok, tk.at[j], {"dp": b}))
        tk[j] = tok[...]

    def all_to_all(dst):
        others(lambda b: send("a", b, j, src.at[b * 2 + t], dst.at[t, blk(j)], {"dp": b}))
        dst[0, blk(j)] = src[j * 2]
        dst[1, blk(j)] = src[j * 2 + 1]

    def arrive(kind, fkind, buf, b):
        got(kind, b, buf.at[t, blk(b)])
        send(fkind, b, b, buf.at[t, blk(b)], buf.at[t, blk(b)], partner)
        got(fkind, b, buf.at[o, blk(b)])

    lane = lax.broadcasted_iota(jnp.int32, (rows, LANES), 1)

    def pack(values):
        packed = jnp.zeros((rows, LANES), F32)
        for i, value in enumerate(values):
            packed = jnp.where(lane == i, value, packed)
        return packed.T[:8]

    def unpack(packed):
        filled = jnp.concatenate([packed, jnp.zeros((LANES - 8, rows), F32)], axis=0)
        return filled.T

    def forward_chunk(b, with_logit):
        total = jnp.zeros((rows, v), F32)
        squares = jnp.zeros((rows, 1), F32)
        logit = jnp.zeros((rows, 1), F32)
        for h in range(2):
            x = xs[h, blk(b)].astype(F32)
            squares += jnp.sum(x * x, axis=1, keepdims=True)
            if with_logit:
                logit += jnp.sum(x * us[h, blk(b)].astype(F32), axis=1, keepdims=True)
            scaled = (x * gain(h)).astype(BF)
            xg[h, blk(b)] = scaled
            total += dot(scaled, w1[h])
        pb[blk(b)] = total.astype(BF)
        ps[b] = pack([squares, logit] if with_logit else [squares])

        @pl.when(b != j)
        def _():
            send("p", b, j, pb.at[blk(b)], pr.at[j], {"dp": b})
            send("ps", b, j, ps.at[b], psr.at[j], {"dp": b})

    def backward_chunk(b):
        total = dot(us[0, blk(b)], w2[0], 1, 1) + dot(us[1, blk(b)], w2[1], 1, 1)
        qb[blk(b)] = total.astype(BF)

        @pl.when(b != j)
        def _():
            send("q", b, j, qb.at[blk(b)], qr.at[j], {"dp": b})

    def reduce(kind, own, landed, acc):
        acc[...] = own[blk(j)].astype(F32)

        def add(b):
            got(kind, b, landed.at[b])
            acc[...] += landed[b].astype(F32)
        others(add)

    def share(kind, buf, forward):
        others(lambda b: send(kind, b, j, buf.at[t, blk(j)], buf.at[t, blk(j)], {"dp": b}))
        if forward:
            send(kind + "f", j, j, buf.at[t, blk(j)], buf.at[t, blk(j)], partner)

    def shared(kind, buf, b):
        @pl.when(b != j)
        def _():
            got(kind, b, buf.at[t, blk(b)])
            send(kind + "f", b, b, buf.at[t, blk(b)], buf.at[t, blk(b)], partner)
        got(kind + "f", b, buf.at[o, blk(b)])

    def own_inverse():
        psr[j] = ps[j]
        others(lambda b: got("ps", b, psr.at[b]))
        sums = psr[0]
        for b in range(1, n):
            sums = sums + psr[b]
        sums = unpack(sums)
        inverse = lax.rsqrt(sums[:, 0:1] / width + eps_norm)
        rkeep[...] = jnp.where(lane == 0, inverse, sums)
        return inverse

    def forward_out():
        inverse = own_inverse()
        reduce("p", pb, pr, pacc)
        pj[t, blk(j)] = (inverse * pacc[...]).astype(BF)
        share("pj", pj, True)
        got("w", 1, w2o)

        def chunk(b):
            shared("pj", pj, b)
            mixed = dot(pj[t, blk(b)], w2[t]) + dot(pj[o, blk(b)], w2o[...])
            yx[blk(b)] = (xs[t, blk(b)].astype(F32) + mixed).astype(BF)
            send("x", b, b, yx.at[blk(b)], xs.at[t, blk(b)], {"section": s + 1})
        everyone(chunk)

    def dot_over_units():
        exs[...] = jnp.broadcast_to(
            jnp.sum(pacc[...] * qacc[...], axis=1, keepdims=True), (rows, LANES)
        )
        send("e", 0, 0, exs, exr, partner)
        got("e", 0, exr)
        return exs[:, :1] + exr[:, :1]

    def backward_out(is_last):
        reduce("q", qb, qr, qacc)
        inner = dot_over_units()
        inverse = rkeep[:, :1]
        if is_last:
            logit = rkeep[:, 1:2] + inverse * inner
            seed = rinfo[:, 0:1] * jnp.exp(logit - rinfo[:, 1:2])
            scale = seed * inverse
            pj[t, blk(j)] = (scale * pacc[...]).astype(BF)
        else:
            seed = jnp.ones((rows, 1), F32)
            scale = inverse
        gq[t, blk(j)] = (scale * qacc[...]).astype(BF)
        sc[j] = pack([inverse * inverse * inverse * (seed * inner) / width, seed])
        share("gq", gq, True)
        others(lambda b: send("sc", b, j, sc.at[j], sc.at[j], {"dp": b}))
        got("w", 0, w1o)

        def chunk(b):
            shared("gq", gq, b)

            @pl.when(b != j)
            def _():
                got("sc", b, sc.at[b])
            packed = unpack(sc[b])
            grad = dot(gq[t, blk(b)], w1[t], 1, 1) + dot(gq[o, blk(b)], w1o[...], 1, 1)
            upstream = us[t, blk(b)].astype(F32)
            if is_last:
                upstream = packed[:, 1:2] * upstream
            yg[blk(b)] = (
                upstream + gain(t) * grad - packed[:, 0:1] * xs[t, blk(b)].astype(F32)
            ).astype(BF)
            send("g", b, b, yg.at[blk(b)], us.at[t, blk(b)], {"section": s - 1})
        everyone(chunk)

    def tokens():
        others(lambda b: got("tk", b, tk.at[b]))
        count = tk[0]
        for b in range(1, n):
            count = count + tk[b]
        return 1.0 / count[0:1, 0:1]

    def finish_value(scale):
        for h in range(2):
            dw1[h] = dot(xg[h], gq[t], 0, 0) * scale

    def finish_value_arriving(scale):
        def add(b, start):
            for h in range(2):
                part = dot(xg[h, blk(b)], gq[t, blk(b)], 0, 0) * scale
                dw1[h] = part if start else dw1[h] + part
        add(j, True)

        def later(b):
            got("gq", b, gq.at[t, blk(b)])
            add(b, False)
        others(later)

    def finish_output(scale):
        for h in range(2):
            dw2[:, h * half:(h + 1) * half] = dot(pj[t], us[h], 0, 0) * scale

    def drain_common():
        sent("w", 0, w1o)
        sent("w", 1, w2o)

        def one(b):
            sent("tk", b, tk.at[b])
            sent("p", b, pb.at[blk(b)])
            sent("ps", b, ps.at[b])
            sent("q", b, qb.at[blk(b)])
            sent("pj", b, pj.at[t, blk(b)])
            sent("gq", b, gq.at[t, blk(b)])
        others(one)

    def first_section():
        start_common()
        all_to_all(xs)
        forward_chunk(j, False)

        def chunk(b):
            arrive("a", "xf", xs, b)
            forward_chunk(b, False)
        others(chunk)
        forward_out()

        def back(b):
            arrive("g", "uf", us, b)
            backward_chunk(b)
        everyone(back)
        scale = tokens()
        reduce("q", qb, qr, qacc)
        gq[t, blk(j)] = (rkeep[:, :1] * qacc[...]).astype(BF)
        share("gq", gq, False)
        finish_output(scale)
        finish_value_arriving(scale)
        got("w", 0, w1o)
        drain_common()

        def rest(b):
            sent("a", b, src.at[0])
            sent("xf", b, xs.at[t, blk(b)])
        others(rest)

        def rest_all(b):
            sent("pjf", b, pj.at[t, blk(b)])
            sent("x", b, yx.at[blk(b)])
            sent("uf", b, us.at[t, blk(b)])
        everyone(rest_all)

    def middle_section():
        start_common()

        def chunk(b):
            arrive("x", "xf", xs, b)
            forward_chunk(b, False)
        everyone(chunk)
        forward_out()

        def back(b):
            arrive("g", "uf", us, b)
            backward_chunk(b)
        everyone(back)
        backward_out(False)
        scale = tokens()
        finish_output(scale)
        finish_value(scale)
        drain_common()
        sent("e", 0, exs)
        others(lambda b: sent("sc", b, sc.at[b]))

        def rest_all(b):
            sent("xf", b, xs.at[t, blk(b)])
            sent("uf", b, us.at[t, blk(b)])
            sent("pjf", b, pj.at[t, blk(b)])
            sent("gqf", b, gq.at[t, blk(b)])
            sent("x", b, yx.at[blk(b)])
            sent("g", b, yg.at[blk(b)])
        everyone(rest_all)

    def last_section():
        start_common()
        all_to_all(us)
        backward_chunk(j)
        row_info()

        def seeds(b):
            arrive("a", "uf", us, b)
            backward_chunk(b)
        others(seeds)

        def chunk(b):
            arrive("x", "xf", xs, b)
            forward_chunk(b, True)
        everyone(chunk)
        own_inverse()
        reduce("p", pb, pr, pacc)
        backward_out(True)
        share("pj", pj, False)
        scale = tokens()
        finish_value(scale)
        others(lambda b: got("pj", b, pj.at[t, blk(b)]))
        finish_output(scale)
        got("w", 1, w2o)
        drain_common()
        sent("e", 0, exs)

        def rest(b):
            sent("a", b, src.at[0])
            sent("uf", b, us.at[t, blk(b)])
            sent("sc", b, sc.at[b])
        others(rest)

        def rest_all(b):
            sent("xf", b, xs.at[t, blk(b)])
            sent("gqf", b, gq.at[t, blk(b)])
            sent("g", b, yg.at[blk(b)])
        everyone(rest_all)

    pl.when(s == 0)(first_section)
    pl.when(s == last)(last_section)
    if sections > 2:
        pl.when((s > 0) & (s < last))(middle_section)


def local_chain(
    hidden, unembed, value_proj, output_proj, norm_gains, survive, lengths, assign,
    advantage, reference_logit, recorded_gap,
):
    n = lax.axis_size("dp")
    sections = lax.axis_size("section")
    s = lax.axis_index("section")
    count, positions, width = hidden.shape
    rows = count * positions
    part = value_proj.shape[1]
    half = part // 2
    v = value_proj.shape[2]

    src = jnp.where(s == sections - 1, unembed, hidden).reshape(rows, n * 2, half)
    src = src.transpose(1, 0, 2)
    w1 = value_proj[0].reshape(2, half, v)
    w2 = output_proj[0].reshape(v, 2, half).transpose(1, 0, 2)
    gains = norm_gains[0].reshape(n * 2, 1, half)
    total = n * rows
    kinds = len(KINDS)
    vm = pl.BlockSpec(memory_space=pltpu.VMEM)
    dw1, dw2 = pl.pallas_call(
        functools.partial(kernel, n, sections, width),
        out_shape=(
            jax.ShapeDtypeStruct((2, half, v), F32),
            jax.ShapeDtypeStruct((v, part), F32),
        ),
        in_specs=[vm] * 10,
        out_specs=(vm, vm),
        scratch_shapes=[
            pltpu.VMEM((2, total, half), BF),
            pltpu.VMEM((2, total, half), BF),
            pltpu.VMEM((2, total, half), BF),
            pltpu.VMEM((total, v), BF),
            pltpu.VMEM((n, rows, v), BF),
            pltpu.VMEM((total, v), BF),
            pltpu.VMEM((n, rows, v), BF),
            pltpu.VMEM((2, total, v), BF),
            pltpu.VMEM((2, total, v), BF),
            pltpu.VMEM((n, 8, rows), F32),
            pltpu.VMEM((half, v), BF),
            pltpu.VMEM((v, half), BF),
            pltpu.VMEM((total, half), BF),
            pltpu.VMEM((total, half), BF),
            pltpu.VMEM((n, 8, LANES), F32),
            pltpu.VMEM((rows, LANES), F32),
            pltpu.VMEM((rows, LANES), F32),
            pltpu.VMEM((rows, v), F32),
            pltpu.VMEM((rows, v), F32),
            pltpu.VMEM((rows, LANES), F32),
            pltpu.VMEM((n, 8, rows), F32),
            pltpu.VMEM((n, 8, rows), F32),
            pltpu.VMEM((rows, LANES), F32),
            pltpu.VMEM((8, LANES), F32),
            pltpu.SemaphoreType.DMA((kinds, n)),
            pltpu.SemaphoreType.DMA((kinds, n)),
        ],
        compiler_params=pltpu.CompilerParams(
            collective_id=0, has_side_effects=True, vmem_limit_bytes=60 * 1024 * 1024
        ),
    )(
        src, w1, w2, gains, survive.reshape(1, -1), lengths.reshape(1, count),
        assign.reshape(1, count), advantage.reshape(1, count), reference_logit.T, recorded_gap.T,
    )
    return (
        dw1.reshape(1, part, v),
        dw2[None],
    )


PAIR_KINDS = (
    "a", "af", "ax", "axf", "bx", "bf", "ax1", "af1", "gn", "mr", "mk", "rr", "rl", "ps", "p0", "s0",
    "in", "w", "d1", "s1", "g0", "g0f", "g1", "g1f", "g2", "gs", "tk",
)


def pair_kernel(
    n, width,
    hid, une, w1, w2, gains, survive, lengths, assign, advantage, base, gap,
    dw1, dw2,
    xs, us, xg, wv1, wv2, b0f, a1f, b0g, gx, mp, mr, mk, part, own, rin, p0, dp1, gz, ga, gb,
    wr, wsend, ps, psr, scs, scr, inn, inr, sc, rinfo, tok, tk,
    ss, rs, ls,
):
    j = lax.axis_index("dp")
    s = lax.axis_index("section")
    t = lax.axis_index("tensor")
    y = lax.axis_index("groups")
    o = 1 - t
    rows = hid.shape[0]
    chunk, v = w1.shape
    half = chunk // 2
    mb = v // n
    positions, count = base.shape
    partner = {"tensor": o}
    right = {"dp": j + 1}
    left = {"dp": j - 1}
    lane = lax.broadcasted_iota(jnp.int32, (rows, LANES), 1)

    def blk(b):
        return pl.ds(pl.multiple_of(b * rows, rows), rows)

    def cols(h):
        return pl.ds(pl.multiple_of(h * half, half), half)

    def wide(b, h):
        return pl.ds(pl.multiple_of(b * chunk + h * half, half), half)

    def mrows(g, b):
        return pl.ds(pl.multiple_of(g * v + b * mb, mb), mb)

    def send(kind, si, ri, a, b, dev):
        k = PAIR_KINDS.index(kind)
        pltpu.make_async_remote_copy(
            src_ref=a, dst_ref=b, send_sem=ss.at[k, si], recv_sem=rs.at[k, ri],
            device_id=dev, device_id_type=pl.DeviceIdType.MESH,
        ).start()

    def handle(kind, i, a):
        k = PAIR_KINDS.index(kind)
        return pltpu.make_async_remote_copy(
            src_ref=a, dst_ref=a, send_sem=ss.at[k, i], recv_sem=rs.at[k, i],
            device_id=partner, device_id_type=pl.DeviceIdType.MESH,
        )

    def got(kind, i, a):
        handle(kind, i, a).wait_recv()

    def sent(kind, i, a):
        handle(kind, i, a).wait_send()

    def others(body):
        def step(k, carry):
            body(lax.rem(j + k, n))
            return carry
        lax.fori_loop(1, n, step, 0)

    def at_distance(d, body):
        pl.when(j + d < n)(lambda: body(j + d))
        pl.when(j - d >= 0)(lambda: body(j - d))

    def replicas(body):
        def step(k, carry):
            at = lax.rem(y * n + j + k, 2 * n)
            body(at // n, lax.rem(at, n))
            return carry
        lax.fori_loop(1, 2 * n, step, 0)

    def pack(values):
        packed = jnp.zeros((rows, LANES), F32)
        for i, value in enumerate(values):
            packed = jnp.where(lane == i, value, packed)
        return packed.T[:8]

    def unpack(packed):
        return jnp.concatenate([packed, jnp.zeros((LANES - 8, rows), F32)], axis=0).T

    def own_tokens():
        response = lax.broadcasted_iota(jnp.int32, (1, count), 1)
        group = count // survive.shape[1]
        kept = jnp.zeros((1, count), F32)
        for g in range(survive.shape[1]):
            inside = (response >= g * group) & (response < (g + 1) * group)
            kept = jnp.where(inside, survive[0:1, g:g + 1].astype(F32), kept)
        held = jnp.sum(kept * lengths[...].astype(F32), axis=1, keepdims=True)
        tok[...] = jnp.broadcast_to(held, (8, LANES))
        others(lambda b: send("tk", b, j, tok, tk.at[j], {"dp": b}))
        tk[j] = tok[...]

    def tokens():
        others(lambda b: got("tk", b, tk.at[b]))
        total = tk[0]
        for b in range(1, n):
            total = total + tk[b]
        return 1.0 / total[0:1, 0:1]

    def row_info():
        row = lax.broadcasted_iota(jnp.int32, (rows, count), 0)
        first = lax.broadcasted_iota(jnp.int32, (rows, count), 1) * positions
        mine = (row >= first) & (row < first + positions)

        def by_response(values):
            return jnp.sum(jnp.where(mine, values, 0.0), axis=1, keepdims=True)

        def by_position(values):
            return by_response(jnp.concatenate([values] * count, axis=0))

        slots = assign[...]
        starts = slots * positions
        hit = (row >= starts) & (row < starts + positions)
        listed = jnp.sum(jnp.where(hit, 1.0, 0.0), axis=1, keepdims=True)
        start = by_response(first.astype(F32))
        place = lax.broadcasted_iota(jnp.int32, (rows, 1), 0).astype(F32) - start
        live = place < by_response(lengths[...].astype(F32))
        adv = by_response(advantage[...])
        q = by_position(gap[...])
        clipped = ((adv > 0) & (q > clip_high)) | ((adv < 0) & (q < clip_low))
        weight = jnp.where(clipped | (~live), 0.0, -loss_scale * adv * listed)
        rinfo[...] = jnp.where(lane == 0, weight, jnp.where(lane == 1, by_position(base[...]), 0.0))

    def local_copy(i, a, b):
        return pltpu.make_async_copy(a, b, ls.at[i])

    def reduce_step(q, d):
        slot = q * n

        def rightward():
            r = j + d

            @pl.when(j > 0)
            def _():
                got("rr", slot + r, rin.at[0, q, r])
                part[q, r] = (part[q, r].astype(F32) + rin[0, q, r].astype(F32)).astype(BF)
            send("rr", slot + r, slot + r, part.at[q, r], rin.at[0, q, r], right)

        def leftward():
            r = j - d

            @pl.when(j < n - 1)
            def _():
                got("rl", slot + r, rin.at[1, q, r])
                part[q, r] = (part[q, r].astype(F32) + rin[1, q, r].astype(F32)).astype(BF)
            send("rl", slot + r, slot + r, part.at[q, r], rin.at[1, q, r], left)

        pl.when(j + d < n)(rightward)
        pl.when(j - d >= 0)(leftward)

    def reduce_own(q):
        slot = q * n + j

        @pl.when(j > 0)
        def _():
            got("rr", slot, rin.at[0, q, j])
            own[q] += rin[0, q, j].astype(F32)

        @pl.when(j < n - 1)
        def _():
            got("rl", slot, rin.at[1, q, j])
            own[q] += rin[1, q, j].astype(F32)

    def reduce_sent(q):
        for d in range(1, n):
            pl.when(j + d < n)(lambda: sent("rr", q * n + j + d, part.at[q, j + d]))
            pl.when(j - d >= 0)(lambda: sent("rl", q * n + j - d, part.at[q, j - d]))

    def gather_start(kind, at):
        pl.when(j < n - 1)(lambda: send(kind, j, j, at(j), at(j), right))
        pl.when(j > 0)(lambda: send(kind, n + j, j, at(j), at(j), left))

    def gather_step(kind, at, d, fkind):
        def pass_on(b, onward):
            got(kind, b, at(b))
            onward()
            if fkind is not None:
                send(fkind, b, b, at(b), at(b), partner)

        def from_left():
            b = j - d
            pass_on(b, lambda: pl.when(j < n - 1)(lambda: send(kind, b, b, at(b), at(b), right)))

        def from_right():
            b = j + d
            pass_on(b, lambda: pl.when(j > 0)(lambda: send(kind, n + b, b, at(b), at(b), left)))

        pl.when(j - d >= 0)(from_left)
        pl.when(j + d < n)(from_right)

    def gather_sent(kind, at):
        def one(b):
            pl.when((b <= j) & (j < n - 1))(lambda: sent(kind, b, at(b)))
            pl.when((b >= j) & (j > 0))(lambda: sent(kind, n + b, at(b)))
        for b in range(n):
            one(b)

    def at_p0(b):
        return p0.at[t, blk(b)]

    def at_dp1(b):
        return dp1.at[t, blk(b)]

    def at_gz(b):
        return gz.at[blk(b)]

    def scalar_sums():
        psr[j] = ps[j]
        others(lambda b: got("ps", b, psr.at[b]))
        sums = psr[0]
        for b in range(1, n):
            sums = sums + psr[b]
        return unpack(sums)[:, 0:1]

    def gram_send():
        others(lambda b: send("mr", b, j, mp.at[b], mr.at[j], {"dp": b}))

    def gram_reduce():
        mr[j] = mp[j]
        others(lambda b: got("mr", b, mr.at[b]))
        total = mr[0].astype(F32)
        for b in range(1, n):
            total = total + mr[b].astype(F32)
        mk[mrows(y, j)] = total.astype(BF)
        replicas(lambda g, b: send(
            "mk", g * n + b, y * n + j, mk.at[mrows(y, j)], mk.at[mrows(y, j)], {"groups": g, "dp": b}
        ))

    def gram_wait():
        replicas(lambda g, b: got("mk", g * n + b, mk.at[mrows(g, b)]))

    def store_gram(value):
        value = value.astype(BF)
        for b in range(n):
            mp[b] = value[b * mb:(b + 1) * mb]

    def main_start(src, other_src, main, other):
        for d in range(n - 1, 0, -1):
            at_distance(d, lambda b: send(
                "a", b, j, src.at[:, wide(b, t)], main.at[blk(j), cols(t)], {"dp": b}
            ))
        local_copy(0, src.at[:, pl.ds(pl.multiple_of(j * chunk, chunk), chunk)], main.at[blk(j)]).start()
        local_copy(1, other_src.at[:, pl.ds(pl.multiple_of(j * chunk, chunk), chunk)], other.at[blk(j)]).start()

    def main_wait(src, other_src, main, other):
        local_copy(0, src.at[:, pl.ds(0, chunk)], main.at[blk(j)]).wait()
        local_copy(1, other_src.at[:, pl.ds(0, chunk)], other.at[blk(j)]).wait()

    def main_arrive(main, d):
        def first(b):
            here = main.at[blk(b), cols(t)]
            got("a", b, here)
            send("ax", b, b, here, here, {"section": 1 - s})
            send("af", b, b, here, here, partner)
        at_distance(d, first)
        at_distance(d, lambda b: got("af", b, main.at[blk(b), cols(o)]))

    def other_arrive(other, d):
        def first(b):
            here = other.at[blk(b), cols(t)]
            got("ax", b, here)
            send("axf", b, b, here, here, partner)
        at_distance(d, first)
        at_distance(d, lambda b: got("axf", b, other.at[blk(b), cols(o)]))

    barrier = pltpu.get_barrier_semaphore()

    def greet(dev):
        pl.semaphore_signal(barrier, inc=1, device_id=dev, device_id_type=pl.DeviceIdType.MESH)

    def meet():
        others(lambda b: greet({"dp": b}))

        def across(b, carry):
            greet({"groups": 1 - y, "dp": b})
            return carry
        lax.fori_loop(0, n, across, 0)
        greet(partner)
        greet({"section": 1 - s})
        greet({"section": 1 - s, "tensor": o})
        pl.semaphore_wait(barrier, 2 * n + 2)

    def drain_common(main, other):
        def one(b):
            sent("a", b, main.at[blk(b), cols(t)])
            sent("ax", b, main.at[blk(b), cols(t)])
            sent("af", b, main.at[blk(b), cols(t)])
            sent("axf", b, other.at[blk(b), cols(t)])
            sent("mr", b, mp.at[b])
            sent("ps", b, ps.at[b])
            sent("tk", b, tk.at[b])
            sent("g0f", b, at_p0(b))
        others(one)
        replicas(lambda g, b: sent("mk", g * n + b, mk.at[mrows(y, j)]))
        sent("bf", 0, b0f.at[t])
        gather_sent("g0", at_p0)
        gather_sent("g1", at_dp1)
        gather_sent("g2", at_gz)

    def first_section():
        local_copy(2, w1, wv1).start()
        local_copy(3, w2, b0f.at[t]).start()
        meet()
        main_start(hid, une, xs, us)
        send("bf", 0, 0, w2, b0f.at[t], partner)

        @pl.when(t == y)
        def _():
            send("bx", 0, 0, w2, b0f.at[t], {"section": 1})
        own_tokens()
        local_copy(2, w1, wv1).wait()
        local_copy(3, w2, b0f.at[t]).wait()
        main_wait(hid, une, xs, us)

        def project(b):
            x = xs[blk(b)].astype(F32)
            ps[b] = pack([jnp.sum(x * x, axis=1, keepdims=True)])
            xg[blk(b)] = (x * gains[j]).astype(BF)
            return dot(xg[blk(b)], wv1[...]), dot(xs[blk(b)], b0f[t], 1, 1)

        def project_main(b):
            pa, pb = project(b)
            part[0, b] = pa.astype(BF)
            part[1, b] = pb.astype(BF)
            send("ps", b, j, ps.at[b], psr.at[j], {"dp": b})

        def project_other(b):
            part[2, b] = dot(us[blk(b)], b0f[t], 1, 1).astype(BF)

        own[0], own[1] = project(j)
        own[2] = dot(us[blk(j)], b0f[t], 1, 1)
        got("bf", 0, b0f.at[o])
        store_gram(dot(b0f[y], b0f[t], 1, 1))
        gram_send()
        for d in range(n - 1, 0, -1):
            main_arrive(xs, d)
            at_distance(d, project_main)

        @pl.when(t != y)
        def _():
            send("bx", 0, 0, w2, b0f.at[t], {"section": 1})
        gram_reduce()
        for d in range(n - 1, 0, -1):
            reduce_step(0, d)
        reduce_own(0)
        xx = scalar_sums()
        inverse = lax.rsqrt(xx / width + eps_norm)
        p0[t, blk(j)] = (inverse * own[0]).astype(BF)
        send("p0", 0, t, at_p0(j), at_p0(j), partner)
        for c in range(2):
            send("p0", 1 + c, t, at_p0(j), at_p0(j), {"section": 1, "tensor": c})
        gather_start("g0", at_p0)
        for d in range(n - 1, 0, -1):
            reduce_step(1, d)
        for d in range(n - 1, 0, -1):
            other_arrive(us, d)
            at_distance(d, project_other)
        for d in range(n - 1, 0, -1):
            reduce_step(2, d)
        reduce_own(1)
        reduce_own(2)
        gram_wait()
        got("p0", o, p0.at[o, blk(j)])
        kb = own[1] + dot(p0[0, blk(j)], mk[0:v]) + dot(p0[1, blk(j)], mk[v:2 * v])
        p0v = p0[t, blk(j)].astype(F32)
        scs[...] = pack([
            xx,
            jnp.sum(p0v * (own[1] + kb), axis=1, keepdims=True),
            jnp.sum(p0v * own[2], axis=1, keepdims=True),
        ])
        for c in range(2):
            send("s0", c, t, scs, scr.at[t], {"section": 1, "tensor": c})
        own[1] = kb
        for d in range(1, n):
            gather_step("g0", at_p0, d, "g0f")
        got("s1", 0, sc.at[j])
        got("w", 0, wr.at[0])
        got("w", 1, wr.at[1])
        packed = unpack(sc[j])
        seed, pull = packed[:, 0:1], packed[:, 1:2]
        grad = seed * own[2] + wr[0].astype(F32) + wr[1].astype(F32) - pull * own[1]
        gz[blk(j)] = (inverse * grad).astype(BF)
        gather_start("g2", at_gz)
        others(lambda b: send("gs", b, j, sc.at[j], sc.at[j], {"dp": b}))
        got("d1", t, at_dp1(j))
        gather_start("g1", at_dp1)
        got("d1", o, dp1.at[o, blk(j)])
        got("ax1", 0, a1f.at[t])
        send("af1", 0, 0, a1f.at[t], a1f.at[t], partner)
        got("gn", 0, gx)
        scale = tokens()
        for d in range(1, n):
            gather_step("g2", at_gz, d, None)
            gather_step("g1", at_dp1, d, "g1f")
        others(lambda b: got("g0f", b, p0.at[o, blk(b)]))
        others(lambda b: got("gs", b, sc.at[b]))
        for b in range(n):
            packed = unpack(sc[b])
            for h in range(2):
                gb[h, blk(b)] = (-packed[:, 1:2] * p0[h, blk(b)].astype(F32)).astype(BF)
            ga[blk(b)] = (packed[:, 0:1] * p0[t, blk(b)].astype(F32)).astype(BF)
        got("af1", 0, a1f.at[o])
        others(lambda b: got("g1f", b, dp1.at[o, blk(b)]))
        through = jnp.zeros((v, chunk), F32)
        pulled = jnp.zeros((v, chunk), F32)
        for h in range(2):
            through += dot(dot(p0[t], dp1[h], 0, 0).astype(BF), a1f[h], 1, 1)
            pulled += dot(dot(p0[t], gb[h], 0, 0).astype(BF), b0f[h])
        total = gx[...] * through + pulled
        total += dot(ga[...], us[...], 0, 0) + dot(gb[t], xs[...], 0, 0)
        dw2[...] = total * scale
        dw1[...] = dot(xg[...], gz[...], 0, 0) * scale
        drain_common(xs, us)
        sent("bx", 0, b0f.at[t])
        sent("af1", 0, a1f.at[t])
        for c in range(3):
            sent("p0", c, at_p0(j))
        for c in range(2):
            sent("s0", c, scs)
        others(lambda b: sent("gs", b, sc.at[b]))
        others(lambda b: sent("g1f", b, at_dp1(b)))
        for q in range(3):
            reduce_sent(q)

    def second_section():
        local_copy(2, w1, a1f.at[t]).start()
        local_copy(3, w2, wv2).start()
        meet()
        main_start(une, hid, us, xs)
        own_tokens()
        row_info()
        local_copy(2, w1, a1f.at[t]).wait()
        local_copy(3, w2, wv2).wait()
        main_wait(une, hid, us, xs)

        def project_main(b):
            part[0, b] = dot(us[blk(b)], wv2[...], 1, 1).astype(BF)

        def project(b):
            x = xs[blk(b)].astype(F32)
            ps[b] = pack([jnp.sum(x * us[blk(b)].astype(F32), axis=1, keepdims=True)])
            xg[blk(b)] = (x * gains[j]).astype(BF)
            return dot(xg[blk(b)], a1f[t])

        def project_other(b):
            part[1, b] = project(b).astype(BF)
            send("ps", b, j, ps.at[b], psr.at[j], {"dp": b})

        own[0] = dot(us[blk(j)], wv2[...], 1, 1)
        own[1] = project(j)

        def take_b0(mine):
            @pl.when(mine)
            def _():
                got("bx", 0, b0f.at[t])
                send("bf", 0, 0, b0f.at[t], b0f.at[t], partner)

            @pl.when(~mine)
            def _():
                got("bf", 0, b0f.at[o])

        for d in range(n - 1, 0, -1):
            main_arrive(us, d)
            at_distance(d, project_main)
            if d == min(2, n - 1):
                take_b0(t == y)
                b0g[y] = (b0f[y].astype(F32) * gains[j]).astype(BF)
                store_gram(dot(b0g[y], a1f[t]))
                gram_send()
        send("ax1", 0, 0, w1, a1f.at[t], {"section": 0})
        send("gn", 0, 0, gains.at[j], gx, {"section": 0})
        for d in range(n - 1, 0, -1):
            reduce_step(0, d)
        gram_reduce()
        for d in range(n - 1, 0, -1):
            other_arrive(xs, d)
            at_distance(d, project_other)
        for d in range(n - 1, 0, -1):
            reduce_step(1, d)
        reduce_own(0)
        reduce_own(1)
        dotted = scalar_sums()
        gram_wait()
        got("p0", 0, p0.at[0, blk(j)])
        got("p0", 1, p0.at[1, blk(j)])
        gather_start("g0", at_p0)
        raised = own[1] + dot(p0[0, blk(j)], mk[0:v]) + dot(p0[1, blk(j)], mk[v:2 * v])
        inn[...] = pack([jnp.sum(raised * own[0], axis=1, keepdims=True)])
        send("in", 0, 0, inn, inr, partner)
        got("s0", 0, scr.at[0])
        got("s0", 1, scr.at[1])
        got("in", 0, inr)
        inner = unpack(inn[...] + inr[...])[:, 0:1]
        sums = unpack(scr[0] + scr[1])
        squares = 0.5 * sums[:, 0:1] + sums[:, 1:2]
        inverse = lax.rsqrt(jnp.maximum(squares, 0.0) / width + eps_norm)
        logit = dotted + sums[:, 2:3] + inverse * inner
        weight = rinfo[:, 0:1]
        seed = jnp.where(weight == 0.0, 0.0, weight * jnp.exp(logit - rinfo[:, 1:2]))
        scaled = seed * inverse
        dp1[t, blk(j)] = (scaled * own[0]).astype(BF)
        back = dot(dp1[t, blk(j)], mk[...], 1, 1).astype(BF)
        for c in range(2):
            wsend[c] = back[:, c * v:(c + 1) * v]
        scs[...] = pack([seed, inverse * inverse * inverse * (seed * inner) / width])
        send("s1", 0, 0, scs, sc.at[j], {"section": 0})
        for c in range(2):
            send("w", c, t, wsend.at[c], wr.at[t], {"section": 0, "tensor": c})
        for c in range(2):
            send("d1", c, t, at_dp1(j), at_dp1(j), {"section": 0, "tensor": c})
        gz[blk(j)] = (scaled * raised).astype(BF)
        gather_start("g1", at_dp1)
        gather_start("g2", at_gz)
        take_b0(t != y)
        for h in range(2):
            b0g[h] = (b0f[h].astype(F32) * gains[j]).astype(BF)
        scale = tokens()
        for d in range(1, n):
            gather_step("g0", at_p0, d, "g0f")
        for d in range(1, n):
            gather_step("g1", at_dp1, d, None)
            gather_step("g2", at_gz, d, None)
        others(lambda b: got("g0f", b, p0.at[o, blk(b)]))
        dw2[...] = dot(gz[...], us[...], 0, 0) * scale
        total = dot(xg[...], dp1[t], 0, 0)
        for h in range(2):
            total += dot(b0g[h], dot(p0[h], dp1[t], 0, 0).astype(BF), 0, 0)
        dw1[...] = total * scale
        drain_common(us, xs)
        sent("ax1", 0, a1f.at[t])
        sent("gn", 0, gx)
        sent("in", 0, inn)
        sent("s1", 0, scs)
        for c in range(2):
            sent("w", c, wsend.at[c])
            sent("d1", c, at_dp1(j))
        for q in range(2):
            reduce_sent(q)

    pl.when(s == 0)(first_section)
    pl.when(s == 1)(second_section)


def local_pair(
    hidden, unembed, value_proj, output_proj, norm_gains, survive, lengths, assign,
    advantage, reference_logit, recorded_gap,
):
    n = lax.axis_size("dp")
    count, positions, width = hidden.shape
    rows = count * positions
    chunk, v = value_proj.shape[1:]
    total = n * rows
    kinds = len(PAIR_KINDS)
    vm = pl.BlockSpec(memory_space=pltpu.VMEM)
    hbm = pl.BlockSpec(memory_space=pl.ANY)
    dw1, dw2 = pl.pallas_call(
        functools.partial(pair_kernel, n, width),
        out_shape=(
            jax.ShapeDtypeStruct((chunk, v), F32),
            jax.ShapeDtypeStruct((v, chunk), F32),
        ),
        in_specs=[hbm] * 4 + [vm] * 7,
        out_specs=(vm, vm),
        scratch_shapes=[
            pltpu.VMEM((total, chunk), BF),
            pltpu.VMEM((total, chunk), BF),
            pltpu.VMEM((total, chunk), BF),
            pltpu.VMEM((chunk, v), BF),
            pltpu.VMEM((v, chunk), BF),
            pltpu.VMEM((2, v, chunk), BF),
            pltpu.VMEM((2, chunk, v), BF),
            pltpu.VMEM((2, v, chunk), BF),
            pltpu.VMEM((1, chunk), F32),
            pltpu.VMEM((n, v // n, v), BF),
            pltpu.VMEM((n, v // n, v), BF),
            pltpu.VMEM((2 * v, v), BF),
            pltpu.VMEM((3, n, rows, v), BF),
            pltpu.VMEM((3, rows, v), F32),
            pltpu.VMEM((2, 3, n, rows, v), BF),
            pltpu.VMEM((2, total, v), BF),
            pltpu.VMEM((2, total, v), BF),
            pltpu.VMEM((total, v), BF),
            pltpu.VMEM((total, v), BF),
            pltpu.VMEM((2, total, v), BF),
            pltpu.VMEM((2, rows, v), BF),
            pltpu.VMEM((2, rows, v), BF),
            pltpu.VMEM((n, 8, rows), F32),
            pltpu.VMEM((n, 8, rows), F32),
            pltpu.VMEM((8, rows), F32),
            pltpu.VMEM((2, 8, rows), F32),
            pltpu.VMEM((8, rows), F32),
            pltpu.VMEM((8, rows), F32),
            pltpu.VMEM((n, 8, rows), F32),
            pltpu.VMEM((rows, LANES), F32),
            pltpu.VMEM((8, LANES), F32),
            pltpu.VMEM((n, 8, LANES), F32),
            pltpu.SemaphoreType.DMA((kinds, 3 * n)),
            pltpu.SemaphoreType.DMA((kinds, 3 * n)),
            pltpu.SemaphoreType.DMA((4,)),
        ],
        compiler_params=pltpu.CompilerParams(
            collective_id=0, has_side_effects=True, vmem_limit_bytes=60 * 1024 * 1024
        ),
    )(
        hidden.reshape(rows, width), unembed.reshape(rows, width), value_proj[0], output_proj[0],
        norm_gains[0].reshape(n, 1, chunk), survive.reshape(1, -1), lengths.reshape(1, count),
        assign.reshape(1, count), advantage.reshape(1, count), reference_logit.T, recorded_gap.T,
    )
    return dw1[None], dw2[None]


def solution(mesh):
    rowwise = P(("groups", "dp"))
    placed = (
        P(("groups", "dp"), None, None),
        P(("groups", "dp"), None, None),
        P("section", "dp", "tensor"),
        P("section", "tensor", "dp"),
        P("section", None),
        rowwise,
        rowwise,
        rowwise,
        rowwise,
        P(("groups", "dp"), None),
        P(("groups", "dp"), None),
    )
    shape = mesh.shape
    paired = shape["section"] == 2 and shape["tensor"] == 2 and shape["groups"] == 2
    return jax.shard_map(
        local_pair if paired else local_chain,
        mesh=mesh,
        in_specs=placed,
        out_specs=(
            P(("groups", "section"), "dp", "tensor"),
            P(("groups", "section"), "tensor", "dp"),
        ),
        check_vma=False,
    )
```

```python
import functools
import math

import jax
import jax.numpy as jnp
from jax import lax
from jax.experimental import pallas as pl
from jax.experimental.pallas import tpu as pltpu
from jax.sharding import PartitionSpec as P

eps_norm = 1e-06
loss_scale = 4096.0
clip_high = math.log(1.28)
clip_low = math.log(0.8)
LANES = 128
KINDS = ("a", "xf", "uf", "p", "q", "pj", "pjf", "gq", "gqf", "sc", "tk", "x", "g", "w", "e", "ps")
BF = jnp.bfloat16
F32 = jnp.float32


def dot(a, b, ca=1, cb=0):
    return lax.dot_general(a, b, (((ca,), (cb,)), ((), ())), preferred_element_type=F32)


def kernel(
    n, sections, width,
    src, w1, w2, gains, survive, lengths, assign, advantage, base, gap,
    dw1, dw2,
    xs, us, xg, pb, pr, qb, qr, pj, gq, sc, w1o, w2o, yx, yg, tk, exs, exr, pacc, qacc, rkeep,
    ps, psr, rinfo, tok,
    ss, rs,
):
    j = lax.axis_index("dp")
    s = lax.axis_index("section")
    t = lax.axis_index("tensor")
    o = 1 - t
    rows = src.shape[1]
    half, v = w1.shape[1:]
    last = sections - 1
    partner = {"tensor": o}
    positions, count = base.shape

    def gain(h):
        return gains[j * 2 + h]

    def own_tokens():
        response = lax.broadcasted_iota(jnp.int32, (1, count), 1)
        group = count // survive.shape[1]
        kept = jnp.zeros((1, count), F32)
        for g in range(survive.shape[1]):
            inside = (response >= g * group) & (response < (g + 1) * group)
            kept = jnp.where(inside, survive[0:1, g:g + 1].astype(F32), kept)
        held = jnp.sum(kept * lengths[...].astype(F32), axis=1, keepdims=True)
        tok[...] = jnp.broadcast_to(held, (8, LANES))

    def row_info():
        row = lax.broadcasted_iota(jnp.int32, (rows, count), 0)
        first = lax.broadcasted_iota(jnp.int32, (rows, count), 1) * positions
        mine = (row >= first) & (row < first + positions)

        def by_response(values):
            return jnp.sum(jnp.where(mine, values, 0.0), axis=1, keepdims=True)

        def by_position(values):
            return by_response(jnp.concatenate([values] * count, axis=0))

        slots = assign[...]
        starts = slots * positions
        hit = (row >= starts) & (row < starts + positions)
        listed = jnp.sum(jnp.where(hit, 1.0, 0.0), axis=1, keepdims=True)
        start = by_response(first.astype(F32))
        place = lax.broadcasted_iota(jnp.int32, (rows, 1), 0).astype(F32) - start
        live = place < by_response(lengths[...].astype(F32))
        adv = by_response(advantage[...])
        q = by_position(gap[...])
        clipped = ((adv > 0) & (q > clip_high)) | ((adv < 0) & (q < clip_low))
        weight = jnp.where(clipped | (~live), 0.0, -loss_scale * adv * listed)
        rinfo[...] = jnp.where(lane == 0, weight, jnp.where(lane == 1, by_position(base[...]), 0.0))

    def blk(b):
        return pl.ds(pl.multiple_of(b * rows, rows), rows)

    def peer(k):
        return lax.rem(j + k, n)

    def send(kind, si, ri, a, b, dev):
        k = KINDS.index(kind)
        pltpu.make_async_remote_copy(
            src_ref=a, dst_ref=b, send_sem=ss.at[k, si], recv_sem=rs.at[k, ri],
            device_id=dev, device_id_type=pl.DeviceIdType.MESH,
        ).start()

    def handle(kind, i, a):
        k = KINDS.index(kind)
        return pltpu.make_async_remote_copy(
            src_ref=a, dst_ref=a, send_sem=ss.at[k, i], recv_sem=rs.at[k, i],
            device_id=partner, device_id_type=pl.DeviceIdType.MESH,
        )

    def got(kind, i, a):
        handle(kind, i, a).wait_recv()

    def sent(kind, i, a):
        handle(kind, i, a).wait_send()

    def others(body):
        def step(k, carry):
            body(peer(k))
            return carry
        lax.fori_loop(1, n, step, 0)

    def everyone(body):
        def step(k, carry):
            body(peer(k))
            return carry
        lax.fori_loop(0, n, step, 0)

    barrier = pltpu.get_barrier_semaphore()

    def greet(dev):
        pl.semaphore_signal(barrier, inc=1, device_id=dev, device_id_type=pl.DeviceIdType.MESH)

    for k in range(1, n):
        greet({"dp": peer(k)})
    greet(partner)

    @pl.when(s > 0)
    def _():
        greet({"section": s - 1})

    @pl.when(s < last)
    def _():
        greet({"section": s + 1})

    pl.semaphore_wait(barrier, n + jnp.where(s > 0, 1, 0) + jnp.where(s < last, 1, 0))

    def start_common():
        send("w", 0, 0, w1.at[o], w1o, partner)
        send("w", 1, 1, w2.at[o], w2o, partner)
        own_tokens()
        others(lambda b: send("tk", b, j, tok, tk.at[j], {"dp": b}))
        tk[j] = tok[...]

    def all_to_all(dst):
        others(lambda b: send("a", b, j, src.at[b * 2 + t], dst.at[t, blk(j)], {"dp": b}))
        dst[0, blk(j)] = src[j * 2]
        dst[1, blk(j)] = src[j * 2 + 1]

    def arrive(kind, fkind, buf, b):
        got(kind, b, buf.at[t, blk(b)])
        send(fkind, b, b, buf.at[t, blk(b)], buf.at[t, blk(b)], partner)
        got(fkind, b, buf.at[o, blk(b)])

    lane = lax.broadcasted_iota(jnp.int32, (rows, LANES), 1)

    def pack(values):
        packed = jnp.zeros((rows, LANES), F32)
        for i, value in enumerate(values):
            packed = jnp.where(lane == i, value, packed)
        return packed.T[:8]

    def unpack(packed):
        filled = jnp.concatenate([packed, jnp.zeros((LANES - 8, rows), F32)], axis=0)
        return filled.T

    def forward_chunk(b, with_logit):
        total = jnp.zeros((rows, v), F32)
        squares = jnp.zeros((rows, 1), F32)
        logit = jnp.zeros((rows, 1), F32)
        for h in range(2):
            x = xs[h, blk(b)].astype(F32)
            squares += jnp.sum(x * x, axis=1, keepdims=True)
            if with_logit:
                logit += jnp.sum(x * us[h, blk(b)].astype(F32), axis=1, keepdims=True)
            scaled = (x * gain(h)).astype(BF)
            xg[h, blk(b)] = scaled
            total += dot(scaled, w1[h])
        pb[blk(b)] = total.astype(BF)
        ps[b] = pack([squares, logit] if with_logit else [squares])

        @pl.when(b != j)
        def _():
            send("p", b, j, pb.at[blk(b)], pr.at[j], {"dp": b})
            send("ps", b, j, ps.at[b], psr.at[j], {"dp": b})

    def backward_chunk(b):
        total = dot(us[0, blk(b)], w2[0], 1, 1) + dot(us[1, blk(b)], w2[1], 1, 1)
        qb[blk(b)] = total.astype(BF)

        @pl.when(b != j)
        def _():
            send("q", b, j, qb.at[blk(b)], qr.at[j], {"dp": b})

    def reduce(kind, own, landed, acc):
        acc[...] = own[blk(j)].astype(F32)

        def add(b):
            got(kind, b, landed.at[b])
            acc[...] += landed[b].astype(F32)
        others(add)

    def share(kind, buf, forward):
        others(lambda b: send(kind, b, j, buf.at[t, blk(j)], buf.at[t, blk(j)], {"dp": b}))
        if forward:
            send(kind + "f", j, j, buf.at[t, blk(j)], buf.at[t, blk(j)], partner)

    def shared(kind, buf, b):
        @pl.when(b != j)
        def _():
            got(kind, b, buf.at[t, blk(b)])
            send(kind + "f", b, b, buf.at[t, blk(b)], buf.at[t, blk(b)], partner)
        got(kind + "f", b, buf.at[o, blk(b)])

    def own_inverse():
        psr[j] = ps[j]
        others(lambda b: got("ps", b, psr.at[b]))
        sums = psr[0]
        for b in range(1, n):
            sums = sums + psr[b]
        sums = unpack(sums)
        inverse = lax.rsqrt(sums[:, 0:1] / width + eps_norm)
        rkeep[...] = jnp.where(lane == 0, inverse, sums)
        return inverse

    def forward_out():
        inverse = own_inverse()
        reduce("p", pb, pr, pacc)
        pj[t, blk(j)] = (inverse * pacc[...]).astype(BF)
        share("pj", pj, True)
        got("w", 1, w2o)

        def chunk(b):
            shared("pj", pj, b)
            mixed = dot(pj[t, blk(b)], w2[t]) + dot(pj[o, blk(b)], w2o[...])
            yx[blk(b)] = (xs[t, blk(b)].astype(F32) + mixed).astype(BF)
            send("x", b, b, yx.at[blk(b)], xs.at[t, blk(b)], {"section": s + 1})
        everyone(chunk)

    def dot_over_units():
        exs[...] = jnp.broadcast_to(
            jnp.sum(pacc[...] * qacc[...], axis=1, keepdims=True), (rows, LANES)
        )
        send("e", 0, 0, exs, exr, partner)
        got("e", 0, exr)
        return exs[:, :1] + exr[:, :1]

    def backward_out(is_last):
        reduce("q", qb, qr, qacc)
        inner = dot_over_units()
        inverse = rkeep[:, :1]
        if is_last:
            logit = rkeep[:, 1:2] + inverse * inner
            seed = rinfo[:, 0:1] * jnp.exp(logit - rinfo[:, 1:2])
            scale = seed * inverse
            pj[t, blk(j)] = (scale * pacc[...]).astype(BF)
        else:
            seed = jnp.ones((rows, 1), F32)
            scale = inverse
        gq[t, blk(j)] = (scale * qacc[...]).astype(BF)
        sc[j] = pack([inverse * inverse * inverse * (seed * inner) / width, seed])
        share("gq", gq, True)
        others(lambda b: send("sc", b, j, sc.at[j], sc.at[j], {"dp": b}))
        got("w", 0, w1o)

        def chunk(b):
            shared("gq", gq, b)

            @pl.when(b != j)
            def _():
                got("sc", b, sc.at[b])
            packed = unpack(sc[b])
            grad = dot(gq[t, blk(b)], w1[t], 1, 1) + dot(gq[o, blk(b)], w1o[...], 1, 1)
            upstream = us[t, blk(b)].astype(F32)
            if is_last:
                upstream = packed[:, 1:2] * upstream
            yg[blk(b)] = (
                upstream + gain(t) * grad - packed[:, 0:1] * xs[t, blk(b)].astype(F32)
            ).astype(BF)
            send("g", b, b, yg.at[blk(b)], us.at[t, blk(b)], {"section": s - 1})
        everyone(chunk)

    def tokens():
        others(lambda b: got("tk", b, tk.at[b]))
        count = tk[0]
        for b in range(1, n):
            count = count + tk[b]
        return 1.0 / count[0:1, 0:1]

    def finish_value(scale):
        for h in range(2):
            dw1[h] = dot(xg[h], gq[t], 0, 0) * scale

    def finish_value_arriving(scale):
        def add(b, start):
            for h in range(2):
                part = dot(xg[h, blk(b)], gq[t, blk(b)], 0, 0) * scale
                dw1[h] = part if start else dw1[h] + part
        add(j, True)

        def later(b):
            got("gq", b, gq.at[t, blk(b)])
            add(b, False)
        others(later)

    def finish_output(scale):
        for h in range(2):
            dw2[:, h * half:(h + 1) * half] = dot(pj[t], us[h], 0, 0) * scale

    def drain_common():
        sent("w", 0, w1o)
        sent("w", 1, w2o)

        def one(b):
            sent("tk", b, tk.at[b])
            sent("p", b, pb.at[blk(b)])
            sent("ps", b, ps.at[b])
            sent("q", b, qb.at[blk(b)])
            sent("pj", b, pj.at[t, blk(b)])
            sent("gq", b, gq.at[t, blk(b)])
        others(one)

    def first_section():
        start_common()
        all_to_all(xs)
        forward_chunk(j, False)

        def chunk(b):
            arrive("a", "xf", xs, b)
            forward_chunk(b, False)
        others(chunk)
        forward_out()

        def back(b):
            arrive("g", "uf", us, b)
            backward_chunk(b)
        everyone(back)
        scale = tokens()
        reduce("q", qb, qr, qacc)
        gq[t, blk(j)] = (rkeep[:, :1] * qacc[...]).astype(BF)
        share("gq", gq, False)
        finish_output(scale)
        finish_value_arriving(scale)
        got("w", 0, w1o)
        drain_common()

        def rest(b):
            sent("a", b, src.at[0])
            sent("xf", b, xs.at[t, blk(b)])
        others(rest)

        def rest_all(b):
            sent("pjf", b, pj.at[t, blk(b)])
            sent("x", b, yx.at[blk(b)])
            sent("uf", b, us.at[t, blk(b)])
        everyone(rest_all)

    def middle_section():
        start_common()

        def chunk(b):
            arrive("x", "xf", xs, b)
            forward_chunk(b, False)
        everyone(chunk)
        forward_out()

        def back(b):
            arrive("g", "uf", us, b)
            backward_chunk(b)
        everyone(back)
        backward_out(False)
        scale = tokens()
        finish_output(scale)
        finish_value(scale)
        drain_common()
        sent("e", 0, exs)
        others(lambda b: sent("sc", b, sc.at[b]))

        def rest_all(b):
            sent("xf", b, xs.at[t, blk(b)])
            sent("uf", b, us.at[t, blk(b)])
            sent("pjf", b, pj.at[t, blk(b)])
            sent("gqf", b, gq.at[t, blk(b)])
            sent("x", b, yx.at[blk(b)])
            sent("g", b, yg.at[blk(b)])
        everyone(rest_all)

    def last_section():
        start_common()
        all_to_all(us)
        backward_chunk(j)
        row_info()

        def seeds(b):
            arrive("a", "uf", us, b)
            backward_chunk(b)
        others(seeds)

        def chunk(b):
            arrive("x", "xf", xs, b)
            forward_chunk(b, True)
        everyone(chunk)
        own_inverse()
        reduce("p", pb, pr, pacc)
        backward_out(True)
        share("pj", pj, False)
        scale = tokens()
        finish_value(scale)
        others(lambda b: got("pj", b, pj.at[t, blk(b)]))
        finish_output(scale)
        got("w", 1, w2o)
        drain_common()
        sent("e", 0, exs)

        def rest(b):
            sent("a", b, src.at[0])
            sent("uf", b, us.at[t, blk(b)])
            sent("sc", b, sc.at[b])
        others(rest)

        def rest_all(b):
            sent("xf", b, xs.at[t, blk(b)])
            sent("gqf", b, gq.at[t, blk(b)])
            sent("g", b, yg.at[blk(b)])
        everyone(rest_all)

    pl.when(s == 0)(first_section)
    pl.when(s == last)(last_section)
    if sections > 2:
        pl.when((s > 0) & (s < last))(middle_section)


def local_chain(
    hidden, unembed, value_proj, output_proj, norm_gains, survive, lengths, assign,
    advantage, reference_logit, recorded_gap,
):
    n = lax.axis_size("dp")
    sections = lax.axis_size("section")
    s = lax.axis_index("section")
    count, positions, width = hidden.shape
    rows = count * positions
    part = value_proj.shape[1]
    half = part // 2
    v = value_proj.shape[2]

    src = jnp.where(s == sections - 1, unembed, hidden).reshape(rows, n * 2, half)
    src = src.transpose(1, 0, 2)
    w1 = value_proj[0].reshape(2, half, v)
    w2 = output_proj[0].reshape(v, 2, half).transpose(1, 0, 2)
    gains = norm_gains[0].reshape(n * 2, 1, half)
    total = n * rows
    kinds = len(KINDS)
    vm = pl.BlockSpec(memory_space=pltpu.VMEM)
    dw1, dw2 = pl.pallas_call(
        functools.partial(kernel, n, sections, width),
        out_shape=(
            jax.ShapeDtypeStruct((2, half, v), F32),
            jax.ShapeDtypeStruct((v, part), F32),
        ),
        in_specs=[vm] * 10,
        out_specs=(vm, vm),
        scratch_shapes=[
            pltpu.VMEM((2, total, half), BF),
            pltpu.VMEM((2, total, half), BF),
            pltpu.VMEM((2, total, half), BF),
            pltpu.VMEM((total, v), BF),
            pltpu.VMEM((n, rows, v), BF),
            pltpu.VMEM((total, v), BF),
            pltpu.VMEM((n, rows, v), BF),
            pltpu.VMEM((2, total, v), BF),
            pltpu.VMEM((2, total, v), BF),
            pltpu.VMEM((n, 8, rows), F32),
            pltpu.VMEM((half, v), BF),
            pltpu.VMEM((v, half), BF),
            pltpu.VMEM((total, half), BF),
            pltpu.VMEM((total, half), BF),
            pltpu.VMEM((n, 8, LANES), F32),
            pltpu.VMEM((rows, LANES), F32),
            pltpu.VMEM((rows, LANES), F32),
            pltpu.VMEM((rows, v), F32),
            pltpu.VMEM((rows, v), F32),
            pltpu.VMEM((rows, LANES), F32),
            pltpu.VMEM((n, 8, rows), F32),
            pltpu.VMEM((n, 8, rows), F32),
            pltpu.VMEM((rows, LANES), F32),
            pltpu.VMEM((8, LANES), F32),
            pltpu.SemaphoreType.DMA((kinds, n)),
            pltpu.SemaphoreType.DMA((kinds, n)),
        ],
        compiler_params=pltpu.CompilerParams(
            collective_id=0, has_side_effects=True, vmem_limit_bytes=60 * 1024 * 1024
        ),
    )(
        src, w1, w2, gains, survive.reshape(1, -1), lengths.reshape(1, count),
        assign.reshape(1, count), advantage.reshape(1, count), reference_logit.T, recorded_gap.T,
    )
    return (
        dw1.reshape(1, part, v),
        dw2[None],
    )


def pair_slots(n):
    sizes = {
        "a": n, "af": n, "ax": n, "axf": n, "bx": 1, "bf": 1, "by": 1, "ax1": 1, "af1": 1, "ay": 1, "gn": 1,
        "mr": n, "mk": n, "my": n, "rr": 3 * n, "rl": 3 * n, "ps": n, "p0": 3, "s0": 2, "in": 1, "w": 2,
        "d1": 2, "s1": 1, "g0": n, "g0x": n, "g0f": n, "g1": n, "gx": n, "g1f": n, "g2": n, "gs": n, "tk": n,
    }
    starts, total = {}, 0
    for kind, size in sizes.items():
        starts[kind] = total
        total += size
    return starts, total


def pair_kernel(
    n, width,
    hid, une, w1, w2, gains, survive, lengths, assign, advantage, base, gap,
    dw1_out, dw2_out,
    dw1, dw2, xs, us, xg, wv1, wv2, b0f, a1f, b0g, gx, mp, mr, mk, part, own, rin, p0, dp1, gz, ga, gb, gc,
    wr, wsend, ps, psr, scs, scr, inn, inr, sc, rinfo, tok, tk,
    ss, rs, ls,
):
    j = lax.axis_index("dp")
    s = lax.axis_index("section")
    t = lax.axis_index("tensor")
    y = lax.axis_index("groups")
    o = 1 - t
    rows = hid.shape[0]
    chunk, v = w1.shape
    half = chunk // 2
    mb = v // n
    positions, count = base.shape
    partner = {"tensor": o}
    right = {"dp": j + 1}
    left = {"dp": j - 1}
    lane = lax.broadcasted_iota(jnp.int32, (rows, LANES), 1)
    starts, _ = pair_slots(n)

    def blk(b):
        return pl.ds(pl.multiple_of(b * rows, rows), rows)

    def cols(h):
        return pl.ds(pl.multiple_of(h * half, half), half)

    def wide(b, h):
        return pl.ds(pl.multiple_of(b * chunk + h * half, half), half)

    def mrows(g, b):
        return pl.ds(pl.multiple_of(g * v + b * mb, mb), mb)

    def send(kind, si, ri, a, b, dev):
        k = starts[kind]
        pltpu.make_async_remote_copy(
            src_ref=a, dst_ref=b, send_sem=ss.at[k + si], recv_sem=rs.at[k + ri],
            device_id=dev, device_id_type=pl.DeviceIdType.MESH,
        ).start()

    def handle(kind, i, a):
        k = starts[kind]
        return pltpu.make_async_remote_copy(
            src_ref=a, dst_ref=a, send_sem=ss.at[k + i], recv_sem=rs.at[k + i],
            device_id=partner, device_id_type=pl.DeviceIdType.MESH,
        )

    def got(kind, i, a):
        handle(kind, i, a).wait_recv()

    def sent(kind, i, a):
        handle(kind, i, a).wait_send()

    def others(body):
        def step(k, carry):
            body(lax.rem(j + k, n))
            return carry
        lax.fori_loop(1, n, step, 0)

    def at_distance(d, body):
        pl.when(j + d < n)(lambda: body(j + d))
        pl.when(j - d >= 0)(lambda: body(j - d))

    def pack(values):
        packed = jnp.zeros((rows, LANES), F32)
        for i, value in enumerate(values):
            packed = jnp.where(lane == i, value, packed)
        return packed.T[:8]

    def unpack(packed):
        return jnp.concatenate([packed, jnp.zeros((LANES - 8, rows), F32)], axis=0).T

    def own_tokens():
        response = lax.broadcasted_iota(jnp.int32, (1, count), 1)
        group = count // survive.shape[1]
        kept = jnp.zeros((1, count), F32)
        for g in range(survive.shape[1]):
            inside = (response >= g * group) & (response < (g + 1) * group)
            kept = jnp.where(inside, survive[0:1, g:g + 1].astype(F32), kept)
        held = jnp.sum(kept * lengths[...].astype(F32), axis=1, keepdims=True)
        tok[...] = jnp.broadcast_to(held, (8, LANES))
        others(lambda b: send("tk", b, j, tok, tk.at[j], {"dp": b}))
        tk[j] = tok[...]

    def tokens():
        others(lambda b: got("tk", b, tk.at[b]))
        total = tk[0]
        for b in range(1, n):
            total = total + tk[b]
        return 1.0 / total[0:1, 0:1]

    def row_info():
        row = lax.broadcasted_iota(jnp.int32, (rows, count), 0)
        first = lax.broadcasted_iota(jnp.int32, (rows, count), 1) * positions
        mine = (row >= first) & (row < first + positions)

        def by_response(values):
            return jnp.sum(jnp.where(mine, values, 0.0), axis=1, keepdims=True)

        def by_position(values):
            return by_response(jnp.concatenate([values] * count, axis=0))

        slots = assign[...]
        starts = slots * positions
        hit = (row >= starts) & (row < starts + positions)
        listed = jnp.sum(jnp.where(hit, 1.0, 0.0), axis=1, keepdims=True)
        start = by_response(first.astype(F32))
        place = lax.broadcasted_iota(jnp.int32, (rows, 1), 0).astype(F32) - start
        live = place < by_response(lengths[...].astype(F32))
        adv = by_response(advantage[...])
        q = by_position(gap[...])
        clipped = ((adv > 0) & (q > clip_high)) | ((adv < 0) & (q < clip_low))
        weight = jnp.where(clipped | (~live), 0.0, -loss_scale * adv * listed)
        rinfo[...] = jnp.where(lane == 0, weight, jnp.where(lane == 1, by_position(base[...]), 0.0))

    def local_copy(i, a, b):
        return pltpu.make_async_copy(a, b, ls.at[i])

    def reduce_step(q, d, at_end):
        slot = q * n

        def onward(kind, way, r, dev):
            if not at_end:
                got(kind, slot + r, rin.at[way, q, r])
                part[q, r] = (part[q, r].astype(F32) + rin[way, q, r].astype(F32)).astype(BF)
            send(kind, slot + r, slot + r, part.at[q, r], rin.at[way, q, r], dev)

        first = j == 0 if at_end else (j > 0) & (j + d < n)
        final = j == n - 1 if at_end else (j < n - 1) & (j - d >= 0)
        pl.when(first)(lambda: onward("rr", 0, j + d, right))
        pl.when(final)(lambda: onward("rl", 1, j - d, left))

    def reduce_inner(q, most, least=1):
        for d in range(most, least - 1, -1):
            reduce_step(q, d, False)

    def reduce_own(q):
        slot = q * n + j

        @pl.when(j > 0)
        def _():
            got("rr", slot, rin.at[0, q, j])
            own[q] += rin[0, q, j].astype(F32)

        @pl.when(j < n - 1)
        def _():
            got("rl", slot, rin.at[1, q, j])
            own[q] += rin[1, q, j].astype(F32)

    def reduce_sent(q):
        for d in range(1, n):
            pl.when(j + d < n)(lambda: sent("rr", q * n + j + d, part.at[q, j + d]))
            pl.when(j - d >= 0)(lambda: sent("rl", q * n + j - d, part.at[q, j - d]))

    def gather(kind, at):
        for d in range(n - 1, 0, -1):
            at_distance(d, lambda b: send(kind, b, j, at(j), at(j), {"dp": b}))

    def at_p0(b):
        return p0.at[t, blk(b)]

    def at_dp1(b):
        return dp1.at[t, blk(b)]

    def at_gz(b):
        return gz.at[blk(b)]

    def scalar_sums():
        psr[j] = ps[j]
        others(lambda b: got("ps", b, psr.at[b]))
        sums = psr[0]
        for b in range(1, n):
            sums = sums + psr[b]
        return unpack(sums)[:, 0:1]

    def gram_send():
        others(lambda b: send("mr", b, j, mp.at[b], mr.at[j], {"dp": b}))

    def gram_reduce():
        mr[j] = mp[j]
        others(lambda b: got("mr", b, mr.at[b]))
        total = mr[0].astype(F32)
        for b in range(1, n):
            total = total + mr[b].astype(F32)
        mk[mrows(y, j)] = total.astype(BF)
        here = mk.at[mrows(y, j)]
        others(lambda b: send("mk", b, j, here, here, {"dp": b}))
        send("my", j, j, here, here, {"groups": 1 - y})

    def gram_pass():
        def across(b):
            here = mk.at[mrows(y, b)]
            got("mk", b, here)
            send("my", b, b, here, here, {"groups": 1 - y})
        others(across)

    def gram_wait():
        for b in range(n):
            got("my", b, mk.at[mrows(1 - y, b)])

    def store_gram(value):
        value = value.astype(BF)
        for b in range(n):
            mp[b] = value[b * mb:(b + 1) * mb]

    def main_send(src, main, d):
        at_distance(d, lambda b: send(
            "a", b, j, src.at[:, wide(b, t)], main.at[blk(j), cols(t)], {"dp": b}
        ))

    def main_start(src, other_src, main, other):
        for d in range(n - 1, 1, -1):
            main_send(src, main, d)
        local_copy(0, src.at[:, pl.ds(pl.multiple_of(j * chunk, chunk), chunk)], main.at[blk(j)]).start()
        local_copy(1, other_src.at[:, pl.ds(pl.multiple_of(j * chunk, chunk), chunk)], other.at[blk(j)]).start()

    def main_wait(src, other_src, main, other):
        local_copy(0, src.at[:, pl.ds(0, chunk)], main.at[blk(j)]).wait()
        local_copy(1, other_src.at[:, pl.ds(0, chunk)], other.at[blk(j)]).wait()

    def main_arrive(main, d):
        def first(b):
            here = main.at[blk(b), cols(t)]
            got("a", b, here)
            send("ax", b, b, here, here, {"section": 1 - s})
            send("af", b, b, here, here, partner)
        at_distance(d, first)
        at_distance(d, lambda b: got("af", b, main.at[blk(b), cols(o)]))

    def other_arrive(other, d):
        def first(b):
            here = other.at[blk(b), cols(t)]
            got("ax", b, here)
            send("axf", b, b, here, here, partner)
        at_distance(d, first)
        at_distance(d, lambda b: got("axf", b, other.at[blk(b), cols(o)]))

    barrier = pltpu.get_barrier_semaphore()

    def greet(dev):
        pl.semaphore_signal(barrier, inc=1, device_id=dev, device_id_type=pl.DeviceIdType.MESH)

    def meet():
        others(lambda b: greet({"dp": b}))
        greet({"groups": 1 - y})
        greet(partner)
        greet({"section": 1 - s})
        greet({"section": 1 - s, "tensor": o})
        pl.semaphore_wait(barrier, n + 3)

    def drain_common(main, other):
        def one(b):
            sent("a", b, main.at[blk(b), cols(t)])
            sent("ax", b, main.at[blk(b), cols(t)])
            sent("af", b, main.at[blk(b), cols(t)])
            sent("axf", b, other.at[blk(b), cols(t)])
            sent("mr", b, mp.at[b])
            sent("ps", b, ps.at[b])
            sent("tk", b, tk.at[b])
            sent("g0f", b, at_p0(b))
            sent("g2", b, at_gz(b))
            sent("gs", b, sc.at[b])
        others(one)
        others(lambda b: sent("mk", b, mk.at[mrows(y, j)]))
        for b in range(n):
            sent("my", b, mk.at[mrows(y, b)])
        sent("bf", 0, b0f.at[t])

    def first_section():
        local_copy(2, w1, wv1).start()
        local_copy(3, w2, b0f.at[t]).start()
        meet()
        @pl.when(t == y)
        def _():
            send("bx", 0, 0, w2, b0f.at[t], {"section": 1})
        main_start(hid, une, xs, us)
        send("bf", 0, 0, w2, b0f.at[t], partner)
        own_tokens()
        local_copy(2, w1, wv1).wait()
        local_copy(3, w2, b0f.at[t]).wait()
        main_wait(hid, une, xs, us)

        def project(b):
            x = xs[blk(b)].astype(F32)
            ps[b] = pack([jnp.sum(x * x, axis=1, keepdims=True)])
            xg[blk(b)] = (x * gains[j]).astype(BF)
            return dot(xg[blk(b)], wv1[...]), dot(xs[blk(b)], b0f[t], 1, 1)

        def project_main(b):
            pa, pb = project(b)
            part[0, b] = pa.astype(BF)
            part[1, b] = pb.astype(BF)
            send("ps", b, j, ps.at[b], psr.at[j], {"dp": b})

        def project_other(b):
            part[2, b] = dot(us[blk(b)], b0f[t], 1, 1).astype(BF)

        own[0], own[1] = project(j)
        own[2] = dot(us[blk(j)], b0f[t], 1, 1)
        got("bf", 0, b0f.at[o])
        store_gram(dot(b0f[y], b0f[t], 1, 1))
        gram_send()
        main_send(hid, xs, 1)
        for d in range(n - 1, 0, -1):
            main_arrive(xs, d)
            at_distance(d, project_main)
            reduce_step(0, d, True)
            reduce_step(1, d, True)
        reduce_inner(0, n - 2)
        reduce_inner(1, n - 2, 2)
        gram_reduce()
        for d in range(n - 1, 0, -1):
            other_arrive(us, d)
            at_distance(d, project_other)
            reduce_step(2, d, True)
        reduce_inner(1, 1)
        reduce_own(0)
        xx = scalar_sums()
        inverse = lax.rsqrt(xx / width + eps_norm)
        p0[t, blk(j)] = (inverse * own[0]).astype(BF)
        send("p0", 0, t, at_p0(j), at_p0(j), partner)
        for c in range(2):
            send("p0", 1 + c, t, at_p0(j), at_p0(j), {"section": 1, "tensor": c})
        reduce_inner(2, n - 2, 2)
        gram_pass()
        reduce_inner(2, 1)

        @pl.when(t == y)
        def _():
            got("ax1", 0, a1f.at[t])
            send("ay", 0, 0, a1f.at[t], a1f.at[t], {"groups": 1 - y})
            send("af1", 0, 0, a1f.at[t], a1f.at[t], partner)
        reduce_own(1)
        reduce_own(2)
        gram_wait()
        got("p0", o, p0.at[o, blk(j)])
        kb = own[1] + dot(p0[0, blk(j)], mk[0:v]) + dot(p0[1, blk(j)], mk[v:2 * v])
        p0v = p0[t, blk(j)].astype(F32)
        scs[...] = pack([
            xx,
            jnp.sum(p0v * (own[1] + kb), axis=1, keepdims=True),
            jnp.sum(p0v * own[2], axis=1, keepdims=True),
        ])
        for c in range(2):
            send("s0", c, t, scs, scr.at[t], {"section": 1, "tensor": c})
        gather("g0", at_p0)
        own[1] = kb
        got("w", 0, wr.at[0])
        got("w", 1, wr.at[1])
        got("s1", 0, sc.at[j])
        others(lambda b: send("gs", b, j, sc.at[j], sc.at[j], {"dp": b}))
        packed = unpack(sc[j])
        grad = packed[:, 0:1] * own[2] - packed[:, 2:3] * own[1]
        grad += packed[:, 1:2] * (wr[0].astype(F32) + wr[1].astype(F32))
        gz[blk(j)] = (inverse * grad).astype(BF)
        gather("g2", at_gz)

        def pass_p0(b):
            got("g0", b, at_p0(b))
            send("g0f", b, b, at_p0(b), at_p0(b), partner)
            send("g0x", b, b, at_p0(b), at_p0(b), {"section": 1})
        others(pass_p0)

        @pl.when(t != y)
        def _():
            got("ay", 0, a1f.at[t])
            send("af1", 0, 0, a1f.at[t], a1f.at[t], partner)
        got("gn", 0, gx)
        scale = tokens()

        def pass_dp1(b):
            got("gx", b, at_dp1(b))
            send("g1f", b, b, at_dp1(b), at_dp1(b), partner)
        others(pass_dp1)
        others(lambda b: got("g0f", b, p0.at[o, blk(b)]))
        got("d1", t, at_dp1(j))
        got("d1", o, dp1.at[o, blk(j)])
        got("af1", 0, a1f.at[o])
        others(lambda b: got("g1f", b, dp1.at[o, blk(b)]))
        others(lambda b: got("gs", b, sc.at[b]))
        for b in range(n):
            packed = unpack(sc[b])
            held = p0[t, blk(b)].astype(F32)
            for h in range(2):
                gb[h, blk(b)] = (-packed[:, 2:3] * p0[h, blk(b)].astype(F32)).astype(BF)
            ga[blk(b)] = (packed[:, 0:1] * held).astype(BF)
            gc[blk(b)] = (packed[:, 1:2] * held).astype(BF)
        through = jnp.zeros((v, chunk), F32)
        for h in range(2):
            through += dot(dot(gc[...], dp1[h], 0, 0).astype(BF), a1f[h], 1, 1)
        dw2[...] = gx[...] * through
        for h in range(2):
            dw2[...] += dot(dot(p0[t], gb[h], 0, 0).astype(BF), b0f[h])
        dw2[...] = (dw2[...] + dot(ga[...], us[...], 0, 0) + dot(gb[t], xs[...], 0, 0)) * scale
        local_copy(1, dw2, dw2_out).start()
        others(lambda b: got("g2", b, at_gz(b)))
        dw1[...] = dot(xg[...], gz[...], 0, 0) * scale
        local_copy(0, dw1, dw1_out).start()
        drain_common(xs, us)

        @pl.when(t == y)
        def _():
            sent("bx", 0, b0f.at[t])
            sent("ay", 0, a1f.at[t])
        sent("af1", 0, a1f.at[t])
        for c in range(3):
            sent("p0", c, at_p0(j))
        for c in range(2):
            sent("s0", c, scs)
        others(lambda b: sent("g0", b, at_p0(b)))
        others(lambda b: sent("g0x", b, at_p0(b)))
        others(lambda b: sent("g1f", b, at_dp1(b)))
        for q in range(3):
            reduce_sent(q)
        local_copy(0, dw1, dw1_out).wait()
        local_copy(1, dw2, dw2_out).wait()

    def second_section():
        local_copy(2, w1, a1f.at[t]).start()
        local_copy(3, w2, wv2).start()
        meet()
        main_start(une, hid, us, xs)
        own_tokens()
        row_info()
        local_copy(2, w1, a1f.at[t]).wait()
        local_copy(3, w2, wv2).wait()
        main_wait(une, hid, us, xs)

        def project_main(b):
            part[0, b] = dot(us[blk(b)], wv2[...], 1, 1).astype(BF)

        def project(b):
            x = xs[blk(b)].astype(F32)
            ps[b] = pack([jnp.sum(x * us[blk(b)].astype(F32), axis=1, keepdims=True)])
            xg[blk(b)] = (x * gains[j]).astype(BF)
            return dot(xg[blk(b)], a1f[t])

        def project_other(b):
            part[1, b] = project(b).astype(BF)
            send("ps", b, j, ps.at[b], psr.at[j], {"dp": b})

        own[0] = dot(us[blk(j)], wv2[...], 1, 1)
        own[1] = project(j)
        main_send(une, us, 1)

        def take_b0():
            @pl.when(t == y)
            def _():
                got("bx", 0, b0f.at[t])
                send("bf", 0, 0, b0f.at[t], b0f.at[t], partner)
                send("by", 0, 0, b0f.at[t], b0f.at[t], {"groups": 1 - y})

            @pl.when(t != y)
            def _():
                got("bf", 0, b0f.at[o])

        def take_rest():
            @pl.when(t != y)
            def _():
                got("by", 0, b0f.at[t])
                send("bf", 0, 0, b0f.at[t], b0f.at[t], partner)

            @pl.when(t == y)
            def _():
                got("bf", 0, b0f.at[o])

        for d in range(n - 1, 0, -1):
            main_arrive(us, d)
            at_distance(d, project_main)
            reduce_step(0, d, True)
            if d == min(2, n - 1):
                take_b0()
                b0g[y] = (b0f[y].astype(F32) * gains[j]).astype(BF)
                store_gram(dot(b0g[y], a1f[t]))
                gram_send()
        @pl.when(t == y)
        def _():
            send("ax1", 0, 0, w1, a1f.at[t], {"section": 0})
        send("gn", 0, 0, gains.at[j], gx, {"section": 0})
        reduce_inner(0, n - 2)
        gram_reduce()
        for d in range(n - 1, 0, -1):
            other_arrive(xs, d)
            at_distance(d, project_other)
            reduce_step(1, d, True)
        reduce_inner(1, n - 2)
        reduce_own(0)
        dp1[t, blk(j)] = own[0].astype(BF)
        for c in range(2):
            send("d1", c, t, at_dp1(j), at_dp1(j), {"section": 0, "tensor": c})
        gram_pass()
        gram_wait()
        back = dot(dp1[t, blk(j)], mk[...], 1, 1).astype(BF)
        for c in range(2):
            wsend[c] = back[:, c * v:(c + 1) * v]
            send("w", c, t, wsend.at[c], wr.at[t], {"section": 0, "tensor": c})
        reduce_own(1)
        dotted = scalar_sums()
        gather("g1", at_dp1)
        got("p0", 0, p0.at[0, blk(j)])
        got("p0", 1, p0.at[1, blk(j)])
        raised = own[1] + dot(p0[0, blk(j)], mk[0:v]) + dot(p0[1, blk(j)], mk[v:2 * v])
        inn[...] = pack([jnp.sum(raised * own[0], axis=1, keepdims=True)])
        send("in", 0, 0, inn, inr, partner)
        gz[blk(j)] = raised.astype(BF)
        gather("g2", at_gz)
        got("in", 0, inr)
        got("s0", 0, scr.at[0])
        got("s0", 1, scr.at[1])
        inner = unpack(inn[...] + inr[...])[:, 0:1]
        sums = unpack(scr[0] + scr[1])
        squares = 0.5 * sums[:, 0:1] + sums[:, 1:2]
        inverse = lax.rsqrt(jnp.maximum(squares, 0.0) / width + eps_norm)
        logit = dotted + sums[:, 2:3] + inverse * inner
        weight = rinfo[:, 0:1]
        seed = jnp.where(weight == 0.0, 0.0, weight * jnp.exp(logit - rinfo[:, 1:2]))
        scaled = seed * inverse
        sc[j] = pack([seed, scaled, inverse * inverse * inverse * (seed * inner) / width])
        send("s1", 0, 0, sc.at[j], sc.at[j], {"section": 0})
        others(lambda b: send("gs", b, j, sc.at[j], sc.at[j], {"dp": b}))

        def pass_dp1(b):
            got("g1", b, at_dp1(b))
            send("gx", b, b, at_dp1(b), at_dp1(b), {"section": 0})
        others(pass_dp1)
        take_rest()
        for h in range(2):
            b0g[h] = (b0f[h].astype(F32) * gains[j]).astype(BF)
        scale = tokens()

        def pass_p0(b):
            got("g0x", b, at_p0(b))
            send("g0f", b, b, at_p0(b), at_p0(b), partner)
        others(pass_p0)
        others(lambda b: got("g0f", b, p0.at[o, blk(b)]))
        others(lambda b: got("g2", b, at_gz(b)))
        others(lambda b: got("gs", b, sc.at[b]))
        for b in range(n):
            scaled = unpack(sc[b])[:, 1:2]
            ga[blk(b)] = (scaled * gz[blk(b)].astype(F32)).astype(BF)
            gc[blk(b)] = (scaled * dp1[t, blk(b)].astype(F32)).astype(BF)
        dw2[...] = dot(ga[...], us[...], 0, 0) * scale
        local_copy(1, dw2, dw2_out).start()
        total = dot(xg[...], gc[...], 0, 0)
        for h in range(2):
            total += dot(b0g[h], dot(p0[h], gc[...], 0, 0).astype(BF), 0, 0)
        dw1[...] = total * scale
        local_copy(0, dw1, dw1_out).start()
        drain_common(us, xs)

        @pl.when(t == y)
        def _():
            sent("ax1", 0, a1f.at[t])
            sent("by", 0, b0f.at[t])
        sent("gn", 0, gx)
        others(lambda b: sent("g1", b, at_dp1(b)))
        others(lambda b: sent("gx", b, at_dp1(b)))
        sent("in", 0, inn)
        sent("s1", 0, sc.at[j])
        for c in range(2):
            sent("w", c, wsend.at[c])
            sent("d1", c, at_dp1(j))
        for q in range(2):
            reduce_sent(q)
        local_copy(0, dw1, dw1_out).wait()
        local_copy(1, dw2, dw2_out).wait()

    pl.when(s == 0)(first_section)
    pl.when(s == 1)(second_section)


def local_pair(
    hidden, unembed, value_proj, output_proj, norm_gains, survive, lengths, assign,
    advantage, reference_logit, recorded_gap,
):
    n = lax.axis_size("dp")
    count, positions, width = hidden.shape
    rows = count * positions
    chunk, v = value_proj.shape[1:]
    total = n * rows
    _, slots = pair_slots(n)
    vm = pl.BlockSpec(memory_space=pltpu.VMEM)
    hbm = pl.BlockSpec(memory_space=pl.ANY)
    dw1, dw2 = pl.pallas_call(
        functools.partial(pair_kernel, n, width),
        out_shape=(
            jax.ShapeDtypeStruct((chunk, v), F32),
            jax.ShapeDtypeStruct((v, chunk), F32),
        ),
        in_specs=[hbm] * 4 + [vm] * 7,
        out_specs=(hbm, hbm),
        scratch_shapes=[
            pltpu.VMEM((chunk, v), F32),
            pltpu.VMEM((v, chunk), F32),
            pltpu.VMEM((total, chunk), BF),
            pltpu.VMEM((total, chunk), BF),
            pltpu.VMEM((total, chunk), BF),
            pltpu.VMEM((chunk, v), BF),
            pltpu.VMEM((v, chunk), BF),
            pltpu.VMEM((2, v, chunk), BF),
            pltpu.VMEM((2, chunk, v), BF),
            pltpu.VMEM((2, v, chunk), BF),
            pltpu.VMEM((1, chunk), F32),
            pltpu.VMEM((n, v // n, v), BF),
            pltpu.VMEM((n, v // n, v), BF),
            pltpu.VMEM((2 * v, v), BF),
            pltpu.VMEM((3, n, rows, v), BF),
            pltpu.VMEM((3, rows, v), F32),
            pltpu.VMEM((2, 3, n, rows, v), BF),
            pltpu.VMEM((2, total, v), BF),
            pltpu.VMEM((2, total, v), BF),
            pltpu.VMEM((total, v), BF),
            pltpu.VMEM((total, v), BF),
            pltpu.VMEM((2, total, v), BF),
            pltpu.VMEM((total, v), BF),
            pltpu.VMEM((2, rows, v), BF),
            pltpu.VMEM((2, rows, v), BF),
            pltpu.VMEM((n, 8, rows), F32),
            pltpu.VMEM((n, 8, rows), F32),
            pltpu.VMEM((8, rows), F32),
            pltpu.VMEM((2, 8, rows), F32),
            pltpu.VMEM((8, rows), F32),
            pltpu.VMEM((8, rows), F32),
            pltpu.VMEM((n, 8, rows), F32),
            pltpu.VMEM((rows, LANES), F32),
            pltpu.VMEM((8, LANES), F32),
            pltpu.VMEM((n, 8, LANES), F32),
            pltpu.SemaphoreType.DMA((slots,)),
            pltpu.SemaphoreType.DMA((slots,)),
            pltpu.SemaphoreType.DMA((4,)),
        ],
        compiler_params=pltpu.CompilerParams(
            collective_id=0, has_side_effects=True, vmem_limit_bytes=60 * 1024 * 1024
        ),
    )(
        hidden.reshape(rows, width), unembed.reshape(rows, width), value_proj[0], output_proj[0],
        norm_gains[0].reshape(n, 1, chunk), survive.reshape(1, -1), lengths.reshape(1, count),
        assign.reshape(1, count), advantage.reshape(1, count), reference_logit.T, recorded_gap.T,
    )
    return dw1[None], dw2[None]


def solution(mesh):
    rowwise = P(("groups", "dp"))
    placed = (
        P(("groups", "dp"), None, None),
        P(("groups", "dp"), None, None),
        P("section", "dp", "tensor"),
        P("section", "tensor", "dp"),
        P("section", None),
        rowwise,
        rowwise,
        rowwise,
        rowwise,
        P(("groups", "dp"), None),
        P(("groups", "dp"), None),
    )
    shape = mesh.shape
    paired = shape["section"] == 2 and shape["tensor"] == 2 and shape["groups"] == 2
    return jax.shard_map(
        local_pair if paired else local_chain,
        mesh=mesh,
        in_specs=placed,
        out_specs=(
            P(("groups", "section"), "dp", "tensor"),
            P(("groups", "section"), "tensor", "dp"),
        ),
        check_vma=False,
    )
```

```python
import functools
import math

import jax
import jax.numpy as jnp
from jax import lax
from jax.experimental import pallas as pl
from jax.experimental.pallas import tpu as pltpu
from jax.sharding import PartitionSpec as P

eps_norm = 1e-06
loss_scale = 4096.0
clip_high = math.log(1.28)
clip_low = math.log(0.8)
LANES = 128
KINDS = ("a", "xf", "uf", "p", "q", "pj", "pjf", "gq", "gqf", "sc", "tk", "x", "g", "w", "e", "ps")
BF = jnp.bfloat16
F32 = jnp.float32


def dot(a, b, ca=1, cb=0):
    return lax.dot_general(a, b, (((ca,), (cb,)), ((), ())), preferred_element_type=F32)


def kernel(
    n, sections, width,
    src, w1, w2, gains, survive, lengths, assign, advantage, base, gap,
    dw1, dw2,
    xs, us, xg, pb, pr, qb, qr, pj, gq, sc, w1o, w2o, yx, yg, tk, exs, exr, pacc, qacc, rkeep,
    ps, psr, rinfo, tok,
    ss, rs,
):
    j = lax.axis_index("dp")
    s = lax.axis_index("section")
    t = lax.axis_index("tensor")
    o = 1 - t
    rows = src.shape[1]
    half, v = w1.shape[1:]
    last = sections - 1
    partner = {"tensor": o}
    positions, count = base.shape

    def gain(h):
        return gains[j * 2 + h]

    def own_tokens():
        response = lax.broadcasted_iota(jnp.int32, (1, count), 1)
        group = count // survive.shape[1]
        kept = jnp.zeros((1, count), F32)
        for g in range(survive.shape[1]):
            inside = (response >= g * group) & (response < (g + 1) * group)
            kept = jnp.where(inside, survive[0:1, g:g + 1].astype(F32), kept)
        held = jnp.sum(kept * lengths[...].astype(F32), axis=1, keepdims=True)
        tok[...] = jnp.broadcast_to(held, (8, LANES))

    def row_info():
        row = lax.broadcasted_iota(jnp.int32, (rows, count), 0)
        first = lax.broadcasted_iota(jnp.int32, (rows, count), 1) * positions
        mine = (row >= first) & (row < first + positions)

        def by_response(values):
            return jnp.sum(jnp.where(mine, values, 0.0), axis=1, keepdims=True)

        def by_position(values):
            return by_response(jnp.concatenate([values] * count, axis=0))

        slots = assign[...]
        starts = slots * positions
        hit = (row >= starts) & (row < starts + positions)
        listed = jnp.sum(jnp.where(hit, 1.0, 0.0), axis=1, keepdims=True)
        start = by_response(first.astype(F32))
        place = lax.broadcasted_iota(jnp.int32, (rows, 1), 0).astype(F32) - start
        live = place < by_response(lengths[...].astype(F32))
        adv = by_response(advantage[...])
        q = by_position(gap[...])
        clipped = ((adv > 0) & (q > clip_high)) | ((adv < 0) & (q < clip_low))
        weight = jnp.where(clipped | (~live), 0.0, -loss_scale * adv * listed)
        rinfo[...] = jnp.where(lane == 0, weight, jnp.where(lane == 1, by_position(base[...]), 0.0))

    def blk(b):
        return pl.ds(pl.multiple_of(b * rows, rows), rows)

    def peer(k):
        return lax.rem(j + k, n)

    def send(kind, si, ri, a, b, dev):
        k = KINDS.index(kind)
        pltpu.make_async_remote_copy(
            src_ref=a, dst_ref=b, send_sem=ss.at[k, si], recv_sem=rs.at[k, ri],
            device_id=dev, device_id_type=pl.DeviceIdType.MESH,
        ).start()

    def handle(kind, i, a):
        k = KINDS.index(kind)
        return pltpu.make_async_remote_copy(
            src_ref=a, dst_ref=a, send_sem=ss.at[k, i], recv_sem=rs.at[k, i],
            device_id=partner, device_id_type=pl.DeviceIdType.MESH,
        )

    def got(kind, i, a):
        handle(kind, i, a).wait_recv()

    def sent(kind, i, a):
        handle(kind, i, a).wait_send()

    def others(body):
        def step(k, carry):
            body(peer(k))
            return carry
        lax.fori_loop(1, n, step, 0)

    def everyone(body):
        def step(k, carry):
            body(peer(k))
            return carry
        lax.fori_loop(0, n, step, 0)

    barrier = pltpu.get_barrier_semaphore()

    def greet(dev):
        pl.semaphore_signal(barrier, inc=1, device_id=dev, device_id_type=pl.DeviceIdType.MESH)

    for k in range(1, n):
        greet({"dp": peer(k)})
    greet(partner)

    @pl.when(s > 0)
    def _():
        greet({"section": s - 1})

    @pl.when(s < last)
    def _():
        greet({"section": s + 1})

    pl.semaphore_wait(barrier, n + jnp.where(s > 0, 1, 0) + jnp.where(s < last, 1, 0))

    def start_common():
        send("w", 0, 0, w1.at[o], w1o, partner)
        send("w", 1, 1, w2.at[o], w2o, partner)
        own_tokens()
        others(lambda b: send("tk", b, j, tok, tk.at[j], {"dp": b}))
        tk[j] = tok[...]

    def all_to_all(dst):
        others(lambda b: send("a", b, j, src.at[b * 2 + t], dst.at[t, blk(j)], {"dp": b}))
        dst[0, blk(j)] = src[j * 2]
        dst[1, blk(j)] = src[j * 2 + 1]

    def arrive(kind, fkind, buf, b):
        got(kind, b, buf.at[t, blk(b)])
        send(fkind, b, b, buf.at[t, blk(b)], buf.at[t, blk(b)], partner)
        got(fkind, b, buf.at[o, blk(b)])

    lane = lax.broadcasted_iota(jnp.int32, (rows, LANES), 1)

    def pack(values):
        packed = jnp.zeros((rows, LANES), F32)
        for i, value in enumerate(values):
            packed = jnp.where(lane == i, value, packed)
        return packed.T[:8]

    def unpack(packed):
        filled = jnp.concatenate([packed, jnp.zeros((LANES - 8, rows), F32)], axis=0)
        return filled.T

    def forward_chunk(b, with_logit):
        total = jnp.zeros((rows, v), F32)
        squares = jnp.zeros((rows, 1), F32)
        logit = jnp.zeros((rows, 1), F32)
        for h in range(2):
            x = xs[h, blk(b)].astype(F32)
            squares += jnp.sum(x * x, axis=1, keepdims=True)
            if with_logit:
                logit += jnp.sum(x * us[h, blk(b)].astype(F32), axis=1, keepdims=True)
            scaled = (x * gain(h)).astype(BF)
            xg[h, blk(b)] = scaled
            total += dot(scaled, w1[h])
        pb[blk(b)] = total.astype(BF)
        ps[b] = pack([squares, logit] if with_logit else [squares])

        @pl.when(b != j)
        def _():
            send("p", b, j, pb.at[blk(b)], pr.at[j], {"dp": b})
            send("ps", b, j, ps.at[b], psr.at[j], {"dp": b})

    def backward_chunk(b):
        total = dot(us[0, blk(b)], w2[0], 1, 1) + dot(us[1, blk(b)], w2[1], 1, 1)
        qb[blk(b)] = total.astype(BF)

        @pl.when(b != j)
        def _():
            send("q", b, j, qb.at[blk(b)], qr.at[j], {"dp": b})

    def reduce(kind, own, landed, acc):
        acc[...] = own[blk(j)].astype(F32)

        def add(b):
            got(kind, b, landed.at[b])
            acc[...] += landed[b].astype(F32)
        others(add)

    def share(kind, buf, forward):
        others(lambda b: send(kind, b, j, buf.at[t, blk(j)], buf.at[t, blk(j)], {"dp": b}))
        if forward:
            send(kind + "f", j, j, buf.at[t, blk(j)], buf.at[t, blk(j)], partner)

    def shared(kind, buf, b):
        @pl.when(b != j)
        def _():
            got(kind, b, buf.at[t, blk(b)])
            send(kind + "f", b, b, buf.at[t, blk(b)], buf.at[t, blk(b)], partner)
        got(kind + "f", b, buf.at[o, blk(b)])

    def own_inverse():
        psr[j] = ps[j]
        others(lambda b: got("ps", b, psr.at[b]))
        sums = psr[0]
        for b in range(1, n):
            sums = sums + psr[b]
        sums = unpack(sums)
        inverse = lax.rsqrt(sums[:, 0:1] / width + eps_norm)
        rkeep[...] = jnp.where(lane == 0, inverse, sums)
        return inverse

    def forward_out():
        inverse = own_inverse()
        reduce("p", pb, pr, pacc)
        pj[t, blk(j)] = (inverse * pacc[...]).astype(BF)
        share("pj", pj, True)
        got("w", 1, w2o)

        def chunk(b):
            shared("pj", pj, b)
            mixed = dot(pj[t, blk(b)], w2[t]) + dot(pj[o, blk(b)], w2o[...])
            yx[blk(b)] = (xs[t, blk(b)].astype(F32) + mixed).astype(BF)
            send("x", b, b, yx.at[blk(b)], xs.at[t, blk(b)], {"section": s + 1})
        everyone(chunk)

    def dot_over_units():
        exs[...] = jnp.broadcast_to(
            jnp.sum(pacc[...] * qacc[...], axis=1, keepdims=True), (rows, LANES)
        )
        send("e", 0, 0, exs, exr, partner)
        got("e", 0, exr)
        return exs[:, :1] + exr[:, :1]

    def backward_out(is_last):
        reduce("q", qb, qr, qacc)
        inner = dot_over_units()
        inverse = rkeep[:, :1]
        if is_last:
            logit = rkeep[:, 1:2] + inverse * inner
            seed = rinfo[:, 0:1] * jnp.exp(logit - rinfo[:, 1:2])
            scale = seed * inverse
            pj[t, blk(j)] = (scale * pacc[...]).astype(BF)
        else:
            seed = jnp.ones((rows, 1), F32)
            scale = inverse
        gq[t, blk(j)] = (scale * qacc[...]).astype(BF)
        sc[j] = pack([inverse * inverse * inverse * (seed * inner) / width, seed])
        share("gq", gq, True)
        others(lambda b: send("sc", b, j, sc.at[j], sc.at[j], {"dp": b}))
        got("w", 0, w1o)

        def chunk(b):
            shared("gq", gq, b)

            @pl.when(b != j)
            def _():
                got("sc", b, sc.at[b])
            packed = unpack(sc[b])
            grad = dot(gq[t, blk(b)], w1[t], 1, 1) + dot(gq[o, blk(b)], w1o[...], 1, 1)
            upstream = us[t, blk(b)].astype(F32)
            if is_last:
                upstream = packed[:, 1:2] * upstream
            yg[blk(b)] = (
                upstream + gain(t) * grad - packed[:, 0:1] * xs[t, blk(b)].astype(F32)
            ).astype(BF)
            send("g", b, b, yg.at[blk(b)], us.at[t, blk(b)], {"section": s - 1})
        everyone(chunk)

    def tokens():
        others(lambda b: got("tk", b, tk.at[b]))
        count = tk[0]
        for b in range(1, n):
            count = count + tk[b]
        return 1.0 / count[0:1, 0:1]

    def finish_value(scale):
        for h in range(2):
            dw1[h] = dot(xg[h], gq[t], 0, 0) * scale

    def finish_value_arriving(scale):
        def add(b, start):
            for h in range(2):
                part = dot(xg[h, blk(b)], gq[t, blk(b)], 0, 0) * scale
                dw1[h] = part if start else dw1[h] + part
        add(j, True)

        def later(b):
            got("gq", b, gq.at[t, blk(b)])
            add(b, False)
        others(later)

    def finish_output(scale):
        for h in range(2):
            dw2[:, h * half:(h + 1) * half] = dot(pj[t], us[h], 0, 0) * scale

    def drain_common():
        sent("w", 0, w1o)
        sent("w", 1, w2o)

        def one(b):
            sent("tk", b, tk.at[b])
            sent("p", b, pb.at[blk(b)])
            sent("ps", b, ps.at[b])
            sent("q", b, qb.at[blk(b)])
            sent("pj", b, pj.at[t, blk(b)])
            sent("gq", b, gq.at[t, blk(b)])
        others(one)

    def first_section():
        start_common()
        all_to_all(xs)
        forward_chunk(j, False)

        def chunk(b):
            arrive("a", "xf", xs, b)
            forward_chunk(b, False)
        others(chunk)
        forward_out()

        def back(b):
            arrive("g", "uf", us, b)
            backward_chunk(b)
        everyone(back)
        scale = tokens()
        reduce("q", qb, qr, qacc)
        gq[t, blk(j)] = (rkeep[:, :1] * qacc[...]).astype(BF)
        share("gq", gq, False)
        finish_output(scale)
        finish_value_arriving(scale)
        got("w", 0, w1o)
        drain_common()

        def rest(b):
            sent("a", b, src.at[0])
            sent("xf", b, xs.at[t, blk(b)])
        others(rest)

        def rest_all(b):
            sent("pjf", b, pj.at[t, blk(b)])
            sent("x", b, yx.at[blk(b)])
            sent("uf", b, us.at[t, blk(b)])
        everyone(rest_all)

    def middle_section():
        start_common()

        def chunk(b):
            arrive("x", "xf", xs, b)
            forward_chunk(b, False)
        everyone(chunk)
        forward_out()

        def back(b):
            arrive("g", "uf", us, b)
            backward_chunk(b)
        everyone(back)
        backward_out(False)
        scale = tokens()
        finish_output(scale)
        finish_value(scale)
        drain_common()
        sent("e", 0, exs)
        others(lambda b: sent("sc", b, sc.at[b]))

        def rest_all(b):
            sent("xf", b, xs.at[t, blk(b)])
            sent("uf", b, us.at[t, blk(b)])
            sent("pjf", b, pj.at[t, blk(b)])
            sent("gqf", b, gq.at[t, blk(b)])
            sent("x", b, yx.at[blk(b)])
            sent("g", b, yg.at[blk(b)])
        everyone(rest_all)

    def last_section():
        start_common()
        all_to_all(us)
        backward_chunk(j)
        row_info()

        def seeds(b):
            arrive("a", "uf", us, b)
            backward_chunk(b)
        others(seeds)

        def chunk(b):
            arrive("x", "xf", xs, b)
            forward_chunk(b, True)
        everyone(chunk)
        own_inverse()
        reduce("p", pb, pr, pacc)
        backward_out(True)
        share("pj", pj, False)
        scale = tokens()
        finish_value(scale)
        others(lambda b: got("pj", b, pj.at[t, blk(b)]))
        finish_output(scale)
        got("w", 1, w2o)
        drain_common()
        sent("e", 0, exs)

        def rest(b):
            sent("a", b, src.at[0])
            sent("uf", b, us.at[t, blk(b)])
            sent("sc", b, sc.at[b])
        others(rest)

        def rest_all(b):
            sent("xf", b, xs.at[t, blk(b)])
            sent("gqf", b, gq.at[t, blk(b)])
            sent("g", b, yg.at[blk(b)])
        everyone(rest_all)

    pl.when(s == 0)(first_section)
    pl.when(s == last)(last_section)
    if sections > 2:
        pl.when((s > 0) & (s < last))(middle_section)


def local_chain(
    hidden, unembed, value_proj, output_proj, norm_gains, survive, lengths, assign,
    advantage, reference_logit, recorded_gap,
):
    n = lax.axis_size("dp")
    sections = lax.axis_size("section")
    s = lax.axis_index("section")
    count, positions, width = hidden.shape
    rows = count * positions
    part = value_proj.shape[1]
    half = part // 2
    v = value_proj.shape[2]

    src = jnp.where(s == sections - 1, unembed, hidden).reshape(rows, n * 2, half)
    src = src.transpose(1, 0, 2)
    w1 = value_proj[0].reshape(2, half, v)
    w2 = output_proj[0].reshape(v, 2, half).transpose(1, 0, 2)
    gains = norm_gains[0].reshape(n * 2, 1, half)
    total = n * rows
    kinds = len(KINDS)
    vm = pl.BlockSpec(memory_space=pltpu.VMEM)
    dw1, dw2 = pl.pallas_call(
        functools.partial(kernel, n, sections, width),
        out_shape=(
            jax.ShapeDtypeStruct((2, half, v), F32),
            jax.ShapeDtypeStruct((v, part), F32),
        ),
        in_specs=[vm] * 10,
        out_specs=(vm, vm),
        scratch_shapes=[
            pltpu.VMEM((2, total, half), BF),
            pltpu.VMEM((2, total, half), BF),
            pltpu.VMEM((2, total, half), BF),
            pltpu.VMEM((total, v), BF),
            pltpu.VMEM((n, rows, v), BF),
            pltpu.VMEM((total, v), BF),
            pltpu.VMEM((n, rows, v), BF),
            pltpu.VMEM((2, total, v), BF),
            pltpu.VMEM((2, total, v), BF),
            pltpu.VMEM((n, 8, rows), F32),
            pltpu.VMEM((half, v), BF),
            pltpu.VMEM((v, half), BF),
            pltpu.VMEM((total, half), BF),
            pltpu.VMEM((total, half), BF),
            pltpu.VMEM((n, 8, LANES), F32),
            pltpu.VMEM((rows, LANES), F32),
            pltpu.VMEM((rows, LANES), F32),
            pltpu.VMEM((rows, v), F32),
            pltpu.VMEM((rows, v), F32),
            pltpu.VMEM((rows, LANES), F32),
            pltpu.VMEM((n, 8, rows), F32),
            pltpu.VMEM((n, 8, rows), F32),
            pltpu.VMEM((rows, LANES), F32),
            pltpu.VMEM((8, LANES), F32),
            pltpu.SemaphoreType.DMA((kinds, n)),
            pltpu.SemaphoreType.DMA((kinds, n)),
        ],
        compiler_params=pltpu.CompilerParams(
            collective_id=0, has_side_effects=True, vmem_limit_bytes=60 * 1024 * 1024
        ),
    )(
        src, w1, w2, gains, survive.reshape(1, -1), lengths.reshape(1, count),
        assign.reshape(1, count), advantage.reshape(1, count), reference_logit.T, recorded_gap.T,
    )
    return (
        dw1.reshape(1, part, v),
        dw2[None],
    )


def pair_slots(n):
    sizes = {
        "a": n, "af": n, "ax": n, "axf": n, "bx": 1, "bf": 1, "by": 1, "ax1": 1, "af1": 1, "ay": 1, "gn": 1,
        "mr": n, "mk": n, "my": n, "rr": 3 * n, "rl": 3 * n, "ps": n, "p0": 2, "s0": 1, "in": 2, "w": 2,
        "d1": 2, "s1": 1, "g0": n, "g0x": n, "g0f": n, "g1": n, "gx": n, "g1f": n, "g2": n, "gs": n, "tk": n,
    }
    starts, total = {}, 0
    for kind, size in sizes.items():
        starts[kind] = total
        total += size
    return list(sizes), starts, total


def pair_kernel(
    n, width,
    hid, une, w1, w2, gains, survive, lengths, assign, advantage, base, gap,
    dw1, dw2,
    xs, us, xg, wv1, wv2, b0f, a1f, b0g, gx, mp, mr, mk, part, own, rin, p0, dp1, gz, ga, gb, gc,
    wr, wsend, ps, psr, scs, scr, inn, inr, sc, rinfo, tok, tk,
    ss, rs, ls,
):
    j = lax.axis_index("dp")
    s = lax.axis_index("section")
    t = lax.axis_index("tensor")
    y = lax.axis_index("groups")
    o = 1 - t
    rows = hid.shape[0]
    chunk, v = w1.shape
    half = chunk // 2
    mb = v // n
    positions, count = base.shape
    partner = {"tensor": o}
    right = {"dp": j + 1}
    left = {"dp": j - 1}
    lane = lax.broadcasted_iota(jnp.int32, (rows, LANES), 1)
    kinds, starts, _ = pair_slots(n)
    most = pl.ds(0, (n - 1) * rows)

    def blk(b):
        return pl.ds(pl.multiple_of(b * rows, rows), rows)

    def cols(h):
        return pl.ds(pl.multiple_of(h * half, half), half)

    def wide(b, h):
        return pl.ds(pl.multiple_of(b * chunk + h * half, half), half)

    def mrows(g, b):
        return pl.ds(pl.multiple_of(g * v + b * mb, mb), mb)

    def send(kind, ri, a, b, dev):
        slot = kinds.index("rr" if kind == "rl" else kind)
        pltpu.make_async_remote_copy(
            src_ref=a, dst_ref=b, send_sem=ss.at[slot], recv_sem=rs.at[starts[kind] + ri],
            device_id=dev, device_id_type=pl.DeviceIdType.MESH,
        ).start()

    def got(kind, i, a):
        pltpu.make_async_remote_copy(
            src_ref=a, dst_ref=a, send_sem=ss.at[kinds.index(kind)], recv_sem=rs.at[starts[kind] + i],
            device_id=partner, device_id_type=pl.DeviceIdType.MESH,
        ).wait_recv()

    def sent(kind, a):
        pltpu.make_async_remote_copy(
            src_ref=a, dst_ref=a, send_sem=ss.at[kinds.index(kind)], recv_sem=rs.at[0],
            device_id=partner, device_id_type=pl.DeviceIdType.MESH,
        ).wait_send()

    def others(body):
        def step(k, carry):
            body(lax.rem(j + k, n))
            return carry
        lax.fori_loop(1, n, step, 0)

    def at_distance(d, body):
        pl.when(j + d < n)(lambda: body(j + d))
        pl.when(j - d >= 0)(lambda: body(j - d))

    def pack(values):
        packed = jnp.zeros((rows, LANES), F32)
        for i, value in enumerate(values):
            packed = jnp.where(lane == i, value, packed)
        return packed.T[:8]

    def unpack(packed):
        return jnp.concatenate([packed, jnp.zeros((LANES - 8, rows), F32)], axis=0).T

    def own_tokens():
        response = lax.broadcasted_iota(jnp.int32, (1, count), 1)
        group = count // survive.shape[1]
        kept = jnp.zeros((1, count), F32)
        for g in range(survive.shape[1]):
            inside = (response >= g * group) & (response < (g + 1) * group)
            kept = jnp.where(inside, survive[0:1, g:g + 1].astype(F32), kept)
        held = jnp.sum(kept * lengths[...].astype(F32), axis=1, keepdims=True)
        tok[...] = jnp.broadcast_to(held, (8, LANES))
        others(lambda b: send("tk", j, tok, tk.at[j], {"dp": b}))
        tk[j] = tok[...]

    def tokens():
        others(lambda b: got("tk", b, tk.at[b]))
        total = tk[0]
        for b in range(1, n):
            total = total + tk[b]
        return 1.0 / total[0:1, 0:1]

    def row_info():
        row = lax.broadcasted_iota(jnp.int32, (rows, count), 0)
        first = lax.broadcasted_iota(jnp.int32, (rows, count), 1) * positions
        mine = (row >= first) & (row < first + positions)

        def by_response(values):
            return jnp.sum(jnp.where(mine, values, 0.0), axis=1, keepdims=True)

        def by_position(values):
            return by_response(jnp.concatenate([values] * count, axis=0))

        slots = assign[...]
        starts = slots * positions
        hit = (row >= starts) & (row < starts + positions)
        listed = jnp.sum(jnp.where(hit, 1.0, 0.0), axis=1, keepdims=True)
        start = by_response(first.astype(F32))
        place = lax.broadcasted_iota(jnp.int32, (rows, 1), 0).astype(F32) - start
        live = place < by_response(lengths[...].astype(F32))
        adv = by_response(advantage[...])
        q = by_position(gap[...])
        clipped = ((adv > 0) & (q > clip_high)) | ((adv < 0) & (q < clip_low))
        weight = jnp.where(clipped | (~live), 0.0, -loss_scale * adv * listed)
        rinfo[...] = jnp.where(lane == 0, weight, jnp.where(lane == 1, by_position(base[...]), 0.0))

    def local_copy(i, a, b):
        return pltpu.make_async_copy(a, b, ls.at[i])

    def reduce_step(q, d, at_end):
        slot = q * n

        def onward(kind, way, r, dev):
            if not at_end:
                got(kind, slot + r, rin.at[way, q, r])
                part[q, r] = (part[q, r].astype(F32) + rin[way, q, r].astype(F32)).astype(BF)
            send(kind, slot + r, part.at[q, r], rin.at[way, q, r], dev)

        first = j == 0 if at_end else (j > 0) & (j + d < n)
        final = j == n - 1 if at_end else (j < n - 1) & (j - d >= 0)
        pl.when(first)(lambda: onward("rr", 0, j + d, right))
        pl.when(final)(lambda: onward("rl", 1, j - d, left))

    def reduce_inner(q, most, least=1):
        for d in range(most, least - 1, -1):
            reduce_step(q, d, False)

    def reduce_own(q):
        slot = q * n + j

        @pl.when(j > 0)
        def _():
            got("rr", slot, rin.at[0, q, j])
            own[q] += rin[0, q, j].astype(F32)

        @pl.when(j < n - 1)
        def _():
            got("rl", slot, rin.at[1, q, j])
            own[q] += rin[1, q, j].astype(F32)

    def gather(kind, at):
        for d in range(n - 1, 0, -1):
            at_distance(d, lambda b: send(kind, j, at(j), at(j), {"dp": b}))

    def at_p0(b):
        return p0.at[t, blk(b)]

    def at_dp1(b):
        return dp1.at[t, blk(b)]

    def at_gz(b):
        return gz.at[blk(b)]

    def scalar_sums():
        psr[j] = ps[j]
        others(lambda b: got("ps", b, psr.at[b]))
        sums = psr[0]
        for b in range(1, n):
            sums = sums + psr[b]
        return unpack(sums)[:, 0:1]

    def gram_send():
        others(lambda b: send("mr", j, mp.at[b], mr.at[j], {"dp": b}))

    def gram_reduce():
        mr[j] = mp[j]
        others(lambda b: got("mr", b, mr.at[b]))
        total = mr[0].astype(F32)
        for b in range(1, n):
            total = total + mr[b].astype(F32)
        mk[mrows(y, j)] = total.astype(BF)
        here = mk.at[mrows(y, j)]
        others(lambda b: send("mk", j, here, here, {"dp": b}))
        send("my", j, here, here, {"groups": 1 - y})

    def gram_pass():
        def across(b):
            here = mk.at[mrows(y, b)]
            got("mk", b, here)
            send("my", b, here, here, {"groups": 1 - y})
        others(across)

    def gram_wait():
        for b in range(n):
            got("my", b, mk.at[mrows(1 - y, b)])

    def store_gram(value):
        value = value.astype(BF)
        for b in range(n):
            mp[b] = value[b * mb:(b + 1) * mb]

    def main_send(src, main, d):
        at_distance(d, lambda b: send(
            "a", j, src.at[:, wide(b, t)], main.at[blk(j), cols(t)], {"dp": b}
        ))

    def main_start(src, other_src, main, other):
        for d in range(n - 1, 1, -1):
            main_send(src, main, d)
        local_copy(0, src.at[:, pl.ds(pl.multiple_of(j * chunk, chunk), chunk)], main.at[blk(j)]).start()
        local_copy(1, other_src.at[:, pl.ds(pl.multiple_of(j * chunk, chunk), chunk)], other.at[blk(j)]).start()

    def main_wait(src, other_src, main, other):
        local_copy(0, src.at[:, pl.ds(0, chunk)], main.at[blk(j)]).wait()
        local_copy(1, other_src.at[:, pl.ds(0, chunk)], other.at[blk(j)]).wait()

    def main_arrive(main, d):
        def first(b):
            here = main.at[blk(b), cols(t)]
            got("a", b, here)
            send("ax", b, here, here, {"section": 1 - s})
            send("af", b, here, here, partner)
        at_distance(d, first)
        at_distance(d, lambda b: got("af", b, main.at[blk(b), cols(o)]))

    def other_take(other):
        def first(b):
            here = other.at[blk(b), cols(t)]
            got("ax", b, here)
            send("axf", b, here, here, partner)
        for d in range(n - 1, 0, -1):
            at_distance(d, first)

    def other_arrive(other, d):
        at_distance(d, lambda b: got("axf", b, other.at[blk(b), cols(o)]))

    barrier = pltpu.get_barrier_semaphore()

    def greet(dev):
        pl.semaphore_signal(barrier, inc=1, device_id=dev, device_id_type=pl.DeviceIdType.MESH)

    def meet():
        others(lambda b: greet({"dp": b}))
        greet({"groups": 1 - y})
        greet(partner)
        greet({"section": 1 - s})
        greet({"section": 1 - s, "tensor": o})
        pl.semaphore_wait(barrier, n + 3)

    def drain_common(main, other, sums):
        for kind in ("a", "ax", "af"):
            sent(kind, main.at[most, pl.ds(0, half)])
        sent("axf", other.at[most, pl.ds(0, half)])
        sent("mr", mp.at[pl.ds(0, n - 1)])
        sent("mk", mk.at[pl.ds(0, (n - 1) * mb)])
        sent("my", mk.at[pl.ds(0, n * mb)])
        sent("ps", ps.at[pl.ds(0, n - 1)])
        sent("tk", tk.at[pl.ds(0, n - 1)])
        sent("gs", sc.at[pl.ds(0, n - 1)])
        sent("rr", part.at[pl.ds(0, sums), pl.ds(0, n - 1)])
        sent("g0f", gz.at[most])
        sent("bf", b0f.at[t])

    def first_section():
        local_copy(2, w1, wv1).start()
        local_copy(3, w2, b0f.at[t]).start()
        meet()
        @pl.when(t == y)
        def _():
            send("bx", 0, w2, b0f.at[t], {"section": 1})
        main_start(hid, une, xs, us)
        send("bf", 0, w2, b0f.at[t], partner)
        own_tokens()
        row_info()
        local_copy(2, w1, wv1).wait()
        local_copy(3, w2, b0f.at[t]).wait()
        main_wait(hid, une, xs, us)

        def project(b):
            x = xs[blk(b)].astype(F32)
            ps[b] = pack([jnp.sum(x * x, axis=1, keepdims=True)])
            xg[blk(b)] = (x * gains[j]).astype(BF)
            return dot(xg[blk(b)], wv1[...]), dot(xs[blk(b)], b0f[t], 1, 1)

        def project_main(b):
            pa, pb = project(b)
            part[0, b] = pa.astype(BF)
            part[1, b] = pb.astype(BF)
            send("ps", j, ps.at[b], psr.at[j], {"dp": b})

        def project_other(b):
            part[2, b] = dot(us[blk(b)], b0f[t], 1, 1).astype(BF)

        own[0], own[1] = project(j)
        own[2] = dot(us[blk(j)], b0f[t], 1, 1)
        got("bf", 0, b0f.at[o])
        store_gram(dot(b0f[y], b0f[t], 1, 1))
        gram_send()
        main_send(hid, xs, 1)
        for d in range(n - 1, 0, -1):
            main_arrive(xs, d)
            at_distance(d, project_main)
            reduce_step(0, d, True)
            reduce_step(1, d, True)
        reduce_inner(0, n - 2)
        reduce_inner(1, n - 2, 2)
        gram_reduce()
        other_take(us)
        for d in range(n - 1, 0, -1):
            other_arrive(us, d)
            at_distance(d, project_other)
            reduce_step(2, d, True)
        reduce_inner(1, 1)
        reduce_own(0)
        xx = scalar_sums()
        inverse = lax.rsqrt(xx / width + eps_norm)
        p0[t, blk(j)] = (inverse * own[0]).astype(BF)
        send("p0", t, at_p0(j), at_p0(j), partner)
        for c in range(2):
            send("p0", t, at_p0(j), at_p0(j), {"section": 1, "tensor": c})
        reduce_inner(2, n - 2, 2)
        gram_pass()
        reduce_inner(2, 1)
        gather("g0", at_p0)

        @pl.when(t == y)
        def _():
            got("ax1", 0, a1f.at[t])
            send("ay", 0, a1f.at[t], a1f.at[t], {"groups": 1 - y})
            send("af1", 0, a1f.at[t], a1f.at[t], partner)
        reduce_own(1)
        reduce_own(2)
        gram_wait()
        got("p0", o, p0.at[o, blk(j)])
        kb = own[1] + dot(p0[0, blk(j)], mk[0:v]) + dot(p0[1, blk(j)], mk[v:2 * v])
        p0v = p0[t, blk(j)].astype(F32)
        scs[...] = pack([
            jnp.sum(p0v * (own[1] + kb), axis=1, keepdims=True),
            jnp.sum(p0v * own[2], axis=1, keepdims=True),
        ])
        send("s0", 0, scs, scr, partner)
        own[1] = kb
        got("w", 0, wr.at[0])
        got("w", 1, wr.at[1])
        got("in", 0, inr.at[0])
        got("in", 1, inr.at[1])
        got("s0", 0, scr)
        sums = unpack(scs[...] + scr[...])
        squares = xx + sums[:, 0:1]
        raised_inverse = lax.rsqrt(jnp.maximum(squares, 0.0) / width + eps_norm)
        inner = unpack(inr[0] + inr[1])[:, 0:2]
        logit = 0.5 * inner[:, 1:2] + sums[:, 1:2] + raised_inverse * inner[:, 0:1]
        weight = rinfo[:, 0:1]
        seed = jnp.where(weight == 0.0, 0.0, weight * jnp.exp(logit - rinfo[:, 1:2]))
        scaled = seed * raised_inverse
        pull = raised_inverse * raised_inverse * raised_inverse * (seed * inner[:, 0:1]) / width
        grad = seed * own[2] - pull * own[1] + scaled * (wr[0].astype(F32) + wr[1].astype(F32))
        gz[blk(j)] = (inverse * grad).astype(BF)
        sc[j] = pack([seed, scaled, pull])
        send("s1", 0, sc.at[j], sc.at[j], {"section": 1})
        others(lambda b: send("gs", j, sc.at[j], sc.at[j], {"dp": b}))
        gather("g2", at_gz)

        def pass_p0(b):
            got("g0", b, at_p0(b))
            send("g0f", b, at_p0(b), at_p0(b), partner)
            send("g0x", b, at_p0(b), at_p0(b), {"section": 1})
        for d in range(1, n):
            at_distance(d, pass_p0)

        @pl.when(t != y)
        def _():
            got("ay", 0, a1f.at[t])
            send("af1", 0, a1f.at[t], a1f.at[t], partner)
        got("gn", 0, gx)
        scale = tokens()

        def pass_dp1(b):
            got("gx", b, at_dp1(b))
            send("g1f", b, at_dp1(b), at_dp1(b), partner)
        for d in range(1, n):
            at_distance(d, pass_dp1)
        others(lambda b: got("g0f", b, p0.at[o, blk(b)]))
        got("d1", t, at_dp1(j))
        got("d1", o, dp1.at[o, blk(j)])
        got("af1", 0, a1f.at[o])
        others(lambda b: got("g1f", b, dp1.at[o, blk(b)]))
        others(lambda b: got("gs", b, sc.at[b]))
        for b in range(n):
            packed = unpack(sc[b])
            held = p0[t, blk(b)].astype(F32)
            for h in range(2):
                gb[h, blk(b)] = (-packed[:, 2:3] * p0[h, blk(b)].astype(F32)).astype(BF)
            ga[blk(b)] = (packed[:, 0:1] * held).astype(BF)
            gc[blk(b)] = (packed[:, 1:2] * held).astype(BF)
        through = jnp.zeros((v, chunk), F32)
        for h in range(2):
            through += dot(dot(gc[...], dp1[h], 0, 0).astype(BF), a1f[h], 1, 1)
        dw2[...] = gx[...] * through
        for h in range(2):
            dw2[...] += dot(dot(p0[t], gb[h], 0, 0).astype(BF), b0f[h])
        dw2[...] = (dw2[...] + dot(ga[...], us[...], 0, 0) + dot(gb[t], xs[...], 0, 0)) * scale
        others(lambda b: got("g2", b, at_gz(b)))
        dw1[...] = dot(xg[...], gz[...], 0, 0) * scale
        drain_common(xs, us, 3)

        @pl.when(t == y)
        def _():
            sent("bx", b0f.at[t])
            sent("ay", a1f.at[t])
        sent("af1", a1f.at[t])
        sent("p0", part.at[:, 0])
        sent("s0", scs)
        sent("s1", scs)
        sent("g0", gz.at[most])
        sent("g2", gz.at[most])
        sent("g0x", gz.at[most])
        sent("g1f", gz.at[most])

    def second_section():
        local_copy(2, w1, a1f.at[t]).start()
        local_copy(3, w2, wv2).start()
        meet()
        main_start(une, hid, us, xs)
        own_tokens()
        local_copy(2, w1, a1f.at[t]).wait()
        local_copy(3, w2, wv2).wait()
        main_wait(une, hid, us, xs)

        def project_main(b):
            part[0, b] = dot(us[blk(b)], wv2[...], 1, 1).astype(BF)

        def project(b):
            x = xs[blk(b)].astype(F32)
            ps[b] = pack([jnp.sum(x * us[blk(b)].astype(F32), axis=1, keepdims=True)])
            xg[blk(b)] = (x * gains[j]).astype(BF)
            return dot(xg[blk(b)], a1f[t])

        def project_other(b):
            part[1, b] = project(b).astype(BF)
            send("ps", j, ps.at[b], psr.at[j], {"dp": b})

        own[0] = dot(us[blk(j)], wv2[...], 1, 1)
        own[1] = project(j)
        main_send(une, us, 1)

        def take_b0():
            @pl.when(t == y)
            def _():
                got("bx", 0, b0f.at[t])
                send("bf", 0, b0f.at[t], b0f.at[t], partner)
                send("by", 0, b0f.at[t], b0f.at[t], {"groups": 1 - y})

            @pl.when(t != y)
            def _():
                got("bf", 0, b0f.at[o])

        def take_rest():
            @pl.when(t != y)
            def _():
                got("by", 0, b0f.at[t])
                send("bf", 0, b0f.at[t], b0f.at[t], partner)

            @pl.when(t == y)
            def _():
                got("bf", 0, b0f.at[o])

        for d in range(n - 1, 0, -1):
            main_arrive(us, d)
            at_distance(d, project_main)
            reduce_step(0, d, True)
            if d == min(2, n - 1):
                take_b0()
                b0g[y] = (b0f[y].astype(F32) * gains[j]).astype(BF)
                store_gram(dot(b0g[y], a1f[t]))
                gram_send()
        @pl.when(t == y)
        def _():
            send("ax1", 0, w1, a1f.at[t], {"section": 0})
        send("gn", 0, gains.at[j], gx, {"section": 0})
        reduce_inner(0, n - 2)
        gram_reduce()
        other_take(xs)
        for d in range(n - 1, 0, -1):
            other_arrive(xs, d)
            at_distance(d, project_other)
            reduce_step(1, d, True)
        reduce_inner(1, n - 2, 2)
        gram_pass()
        reduce_inner(1, 1)
        reduce_own(0)
        dp1[t, blk(j)] = own[0].astype(BF)
        for c in range(2):
            send("d1", t, at_dp1(j), at_dp1(j), {"section": 0, "tensor": c})
        gram_wait()
        back = dot(dp1[t, blk(j)], mk[...], 1, 1).astype(BF)
        for c in range(2):
            wsend[c] = back[:, c * v:(c + 1) * v]
            send("w", t, wsend.at[c], wr.at[t], {"section": 0, "tensor": c})
        reduce_own(1)
        dotted = scalar_sums()
        gather("g1", at_dp1)
        got("p0", 0, p0.at[0, blk(j)])
        got("p0", 1, p0.at[1, blk(j)])
        raised = own[1] + dot(p0[0, blk(j)], mk[0:v]) + dot(p0[1, blk(j)], mk[v:2 * v])
        inn[...] = pack([jnp.sum(raised * own[0], axis=1, keepdims=True), dotted])
        for c in range(2):
            send("in", t, inn, inr.at[t], {"section": 0, "tensor": c})
        gz[blk(j)] = raised.astype(BF)
        gather("g2", at_gz)

        def pass_dp1(b):
            got("g1", b, at_dp1(b))
            send("gx", b, at_dp1(b), at_dp1(b), {"section": 0})

        for d in range(1, n):
            at_distance(d, pass_dp1)
        got("s1", 0, sc.at[j])
        others(lambda b: send("gs", j, sc.at[j], sc.at[j], {"dp": b}))
        take_rest()
        for h in range(2):
            b0g[h] = (b0f[h].astype(F32) * gains[j]).astype(BF)
        scale = tokens()

        def pass_p0(b):
            got("g0x", b, at_p0(b))
            send("g0f", b, at_p0(b), at_p0(b), partner)
        for d in range(1, n):
            at_distance(d, pass_p0)
        others(lambda b: got("g0f", b, p0.at[o, blk(b)]))
        others(lambda b: got("g2", b, at_gz(b)))
        others(lambda b: got("gs", b, sc.at[b]))
        for b in range(n):
            scaled = unpack(sc[b])[:, 1:2]
            ga[blk(b)] = (scaled * gz[blk(b)].astype(F32)).astype(BF)
            gc[blk(b)] = (scaled * dp1[t, blk(b)].astype(F32)).astype(BF)
        dw2[...] = dot(ga[...], us[...], 0, 0) * scale
        total = dot(xg[...], gc[...], 0, 0)
        for h in range(2):
            total += dot(b0g[h], dot(p0[h], gc[...], 0, 0).astype(BF), 0, 0)
        dw1[...] = total * scale
        drain_common(us, xs, 2)

        @pl.when(t == y)
        def _():
            sent("ax1", a1f.at[t])
            sent("by", b0f.at[t])
        sent("gn", gx)
        sent("g1", gz.at[most])
        sent("g2", gz.at[most])
        sent("gx", ga.at[most])
        sent("in", inr)
        sent("w", wsend)
        sent("d1", part.at[pl.ds(0, 2), 0])

    pl.when(s == 0)(first_section)
    pl.when(s == 1)(second_section)


def local_pair(
    hidden, unembed, value_proj, output_proj, norm_gains, survive, lengths, assign,
    advantage, reference_logit, recorded_gap,
):
    n = lax.axis_size("dp")
    count, positions, width = hidden.shape
    rows = count * positions
    chunk, v = value_proj.shape[1:]
    total = n * rows
    kinds, _, slots = pair_slots(n)
    vm = pl.BlockSpec(memory_space=pltpu.VMEM)
    hbm = pl.BlockSpec(memory_space=pl.ANY)
    dw1, dw2 = pl.pallas_call(
        functools.partial(pair_kernel, n, width),
        out_shape=(
            pltpu.VMEM((chunk, v), F32),
            pltpu.VMEM((v, chunk), F32),
        ),
        in_specs=[hbm] * 4 + [vm] * 7,
        out_specs=(vm, vm),
        scratch_shapes=[
            pltpu.VMEM((total, chunk), BF),
            pltpu.VMEM((total, chunk), BF),
            pltpu.VMEM((total, chunk), BF),
            pltpu.VMEM((chunk, v), BF),
            pltpu.VMEM((v, chunk), BF),
            pltpu.VMEM((2, v, chunk), BF),
            pltpu.VMEM((2, chunk, v), BF),
            pltpu.VMEM((2, v, chunk), BF),
            pltpu.VMEM((1, chunk), F32),
            pltpu.VMEM((n, v // n, v), BF),
            pltpu.VMEM((n, v // n, v), BF),
            pltpu.VMEM((2 * v, v), BF),
            pltpu.VMEM((3, n, rows, v), BF),
            pltpu.VMEM((3, rows, v), F32),
            pltpu.VMEM((2, 3, n, rows, v), BF),
            pltpu.VMEM((2, total, v), BF),
            pltpu.VMEM((2, total, v), BF),
            pltpu.VMEM((total, v), BF),
            pltpu.VMEM((total, v), BF),
            pltpu.VMEM((2, total, v), BF),
            pltpu.VMEM((total, v), BF),
            pltpu.VMEM((2, rows, v), BF),
            pltpu.VMEM((2, rows, v), BF),
            pltpu.VMEM((n, 8, rows), F32),
            pltpu.VMEM((n, 8, rows), F32),
            pltpu.VMEM((8, rows), F32),
            pltpu.VMEM((8, rows), F32),
            pltpu.VMEM((8, rows), F32),
            pltpu.VMEM((2, 8, rows), F32),
            pltpu.VMEM((n, 8, rows), F32),
            pltpu.VMEM((rows, LANES), F32),
            pltpu.VMEM((8, LANES), F32),
            pltpu.VMEM((n, 8, LANES), F32),
            pltpu.SemaphoreType.DMA((len(kinds),)),
            pltpu.SemaphoreType.DMA((slots,)),
            pltpu.SemaphoreType.DMA((4,)),
        ],
        compiler_params=pltpu.CompilerParams(
            collective_id=0, has_side_effects=True, vmem_limit_bytes=60 * 1024 * 1024
        ),
    )(
        hidden.reshape(rows, width), unembed.reshape(rows, width), value_proj[0], output_proj[0],
        norm_gains[0].reshape(n, 1, chunk), survive.reshape(1, -1), lengths.reshape(1, count),
        assign.reshape(1, count), advantage.reshape(1, count), reference_logit.T, recorded_gap.T,
    )
    return dw1[None], dw2[None]


def solution(mesh):
    rowwise = P(("groups", "dp"))
    placed = (
        P(("groups", "dp"), None, None),
        P(("groups", "dp"), None, None),
        P("section", "dp", "tensor"),
        P("section", "tensor", "dp"),
        P("section", None),
        rowwise,
        rowwise,
        rowwise,
        rowwise,
        P(("groups", "dp"), None),
        P(("groups", "dp"), None),
    )
    shape = mesh.shape
    paired = shape["section"] == 2 and shape["tensor"] == 2 and shape["groups"] == 2
    return jax.shard_map(
        local_pair if paired else local_chain,
        mesh=mesh,
        in_specs=placed,
        out_specs=(
            P(("groups", "section"), "dp", "tensor"),
            P(("groups", "section"), "tensor", "dp"),
        ),
        check_vma=False,
    )
```

```python
import functools
import math

import jax
import jax.numpy as jnp
from jax import lax
from jax.experimental import pallas as pl
from jax.experimental.pallas import tpu as pltpu
from jax.sharding import PartitionSpec as P

eps_norm = 1e-06
loss_scale = 4096.0
clip_high = math.log(1.28)
clip_low = math.log(0.8)
LANES = 128
KINDS = ("a", "xf", "uf", "p", "q", "pj", "pjf", "gq", "gqf", "sc", "tk", "x", "g", "w", "e", "ps")
BF = jnp.bfloat16
F32 = jnp.float32


def dot(a, b, ca=1, cb=0):
    return lax.dot_general(a, b, (((ca,), (cb,)), ((), ())), preferred_element_type=F32)


def kernel(
    n, sections, width,
    src, w1, w2, gains, survive, lengths, assign, advantage, base, gap,
    dw1, dw2,
    xs, us, xg, pb, pr, qb, qr, pj, gq, sc, w1o, w2o, yx, yg, tk, exs, exr, pacc, qacc, rkeep,
    ps, psr, rinfo, tok,
    ss, rs,
):
    j = lax.axis_index("dp")
    s = lax.axis_index("section")
    t = lax.axis_index("tensor")
    o = 1 - t
    rows = src.shape[1]
    half, v = w1.shape[1:]
    last = sections - 1
    partner = {"tensor": o}
    positions, count = base.shape

    def gain(h):
        return gains[j * 2 + h]

    def own_tokens():
        response = lax.broadcasted_iota(jnp.int32, (1, count), 1)
        group = count // survive.shape[1]
        kept = jnp.zeros((1, count), F32)
        for g in range(survive.shape[1]):
            inside = (response >= g * group) & (response < (g + 1) * group)
            kept = jnp.where(inside, survive[0:1, g:g + 1].astype(F32), kept)
        held = jnp.sum(kept * lengths[...].astype(F32), axis=1, keepdims=True)
        tok[...] = jnp.broadcast_to(held, (8, LANES))

    def row_info():
        row = lax.broadcasted_iota(jnp.int32, (rows, count), 0)
        first = lax.broadcasted_iota(jnp.int32, (rows, count), 1) * positions
        mine = (row >= first) & (row < first + positions)

        def by_response(values):
            return jnp.sum(jnp.where(mine, values, 0.0), axis=1, keepdims=True)

        def by_position(values):
            return by_response(jnp.concatenate([values] * count, axis=0))

        slots = assign[...]
        starts = slots * positions
        hit = (row >= starts) & (row < starts + positions)
        listed = jnp.sum(jnp.where(hit, 1.0, 0.0), axis=1, keepdims=True)
        start = by_response(first.astype(F32))
        place = lax.broadcasted_iota(jnp.int32, (rows, 1), 0).astype(F32) - start
        live = place < by_response(lengths[...].astype(F32))
        adv = by_response(advantage[...])
        q = by_position(gap[...])
        clipped = ((adv > 0) & (q > clip_high)) | ((adv < 0) & (q < clip_low))
        weight = jnp.where(clipped | (~live), 0.0, -loss_scale * adv * listed)
        rinfo[...] = jnp.where(lane == 0, weight, jnp.where(lane == 1, by_position(base[...]), 0.0))

    def blk(b):
        return pl.ds(pl.multiple_of(b * rows, rows), rows)

    def peer(k):
        return lax.rem(j + k, n)

    def send(kind, si, ri, a, b, dev):
        k = KINDS.index(kind)
        pltpu.make_async_remote_copy(
            src_ref=a, dst_ref=b, send_sem=ss.at[k, si], recv_sem=rs.at[k, ri],
            device_id=dev, device_id_type=pl.DeviceIdType.MESH,
        ).start()

    def handle(kind, i, a):
        k = KINDS.index(kind)
        return pltpu.make_async_remote_copy(
            src_ref=a, dst_ref=a, send_sem=ss.at[k, i], recv_sem=rs.at[k, i],
            device_id=partner, device_id_type=pl.DeviceIdType.MESH,
        )

    def got(kind, i, a):
        handle(kind, i, a).wait_recv()

    def sent(kind, i, a):
        handle(kind, i, a).wait_send()

    def others(body):
        def step(k, carry):
            body(peer(k))
            return carry
        lax.fori_loop(1, n, step, 0)

    def everyone(body):
        def step(k, carry):
            body(peer(k))
            return carry
        lax.fori_loop(0, n, step, 0)

    barrier = pltpu.get_barrier_semaphore()

    def greet(dev):
        pl.semaphore_signal(barrier, inc=1, device_id=dev, device_id_type=pl.DeviceIdType.MESH)

    for k in range(1, n):
        greet({"dp": peer(k)})
    greet(partner)

    @pl.when(s > 0)
    def _():
        greet({"section": s - 1})

    @pl.when(s < last)
    def _():
        greet({"section": s + 1})

    pl.semaphore_wait(barrier, n + jnp.where(s > 0, 1, 0) + jnp.where(s < last, 1, 0))

    def start_common():
        send("w", 0, 0, w1.at[o], w1o, partner)
        send("w", 1, 1, w2.at[o], w2o, partner)
        own_tokens()
        others(lambda b: send("tk", b, j, tok, tk.at[j], {"dp": b}))
        tk[j] = tok[...]

    def all_to_all(dst):
        others(lambda b: send("a", b, j, src.at[b * 2 + t], dst.at[t, blk(j)], {"dp": b}))
        dst[0, blk(j)] = src[j * 2]
        dst[1, blk(j)] = src[j * 2 + 1]

    def arrive(kind, fkind, buf, b):
        got(kind, b, buf.at[t, blk(b)])
        send(fkind, b, b, buf.at[t, blk(b)], buf.at[t, blk(b)], partner)
        got(fkind, b, buf.at[o, blk(b)])

    lane = lax.broadcasted_iota(jnp.int32, (rows, LANES), 1)

    def pack(values):
        packed = jnp.zeros((rows, LANES), F32)
        for i, value in enumerate(values):
            packed = jnp.where(lane == i, value, packed)
        return packed.T[:8]

    def unpack(packed):
        filled = jnp.concatenate([packed, jnp.zeros((LANES - 8, rows), F32)], axis=0)
        return filled.T

    def forward_chunk(b, with_logit):
        total = jnp.zeros((rows, v), F32)
        squares = jnp.zeros((rows, 1), F32)
        logit = jnp.zeros((rows, 1), F32)
        for h in range(2):
            x = xs[h, blk(b)].astype(F32)
            squares += jnp.sum(x * x, axis=1, keepdims=True)
            if with_logit:
                logit += jnp.sum(x * us[h, blk(b)].astype(F32), axis=1, keepdims=True)
            scaled = (x * gain(h)).astype(BF)
            xg[h, blk(b)] = scaled
            total += dot(scaled, w1[h])
        pb[blk(b)] = total.astype(BF)
        ps[b] = pack([squares, logit] if with_logit else [squares])

        @pl.when(b != j)
        def _():
            send("p", b, j, pb.at[blk(b)], pr.at[j], {"dp": b})
            send("ps", b, j, ps.at[b], psr.at[j], {"dp": b})

    def backward_chunk(b):
        total = dot(us[0, blk(b)], w2[0], 1, 1) + dot(us[1, blk(b)], w2[1], 1, 1)
        qb[blk(b)] = total.astype(BF)

        @pl.when(b != j)
        def _():
            send("q", b, j, qb.at[blk(b)], qr.at[j], {"dp": b})

    def reduce(kind, own, landed, acc):
        acc[...] = own[blk(j)].astype(F32)

        def add(b):
            got(kind, b, landed.at[b])
            acc[...] += landed[b].astype(F32)
        others(add)

    def share(kind, buf, forward):
        others(lambda b: send(kind, b, j, buf.at[t, blk(j)], buf.at[t, blk(j)], {"dp": b}))
        if forward:
            send(kind + "f", j, j, buf.at[t, blk(j)], buf.at[t, blk(j)], partner)

    def shared(kind, buf, b):
        @pl.when(b != j)
        def _():
            got(kind, b, buf.at[t, blk(b)])
            send(kind + "f", b, b, buf.at[t, blk(b)], buf.at[t, blk(b)], partner)
        got(kind + "f", b, buf.at[o, blk(b)])

    def own_inverse():
        psr[j] = ps[j]
        others(lambda b: got("ps", b, psr.at[b]))
        sums = psr[0]
        for b in range(1, n):
            sums = sums + psr[b]
        sums = unpack(sums)
        inverse = lax.rsqrt(sums[:, 0:1] / width + eps_norm)
        rkeep[...] = jnp.where(lane == 0, inverse, sums)
        return inverse

    def forward_out():
        inverse = own_inverse()
        reduce("p", pb, pr, pacc)
        pj[t, blk(j)] = (inverse * pacc[...]).astype(BF)
        share("pj", pj, True)
        got("w", 1, w2o)

        def chunk(b):
            shared("pj", pj, b)
            mixed = dot(pj[t, blk(b)], w2[t]) + dot(pj[o, blk(b)], w2o[...])
            yx[blk(b)] = (xs[t, blk(b)].astype(F32) + mixed).astype(BF)
            send("x", b, b, yx.at[blk(b)], xs.at[t, blk(b)], {"section": s + 1})
        everyone(chunk)

    def dot_over_units():
        exs[...] = jnp.broadcast_to(
            jnp.sum(pacc[...] * qacc[...], axis=1, keepdims=True), (rows, LANES)
        )
        send("e", 0, 0, exs, exr, partner)
        got("e", 0, exr)
        return exs[:, :1] + exr[:, :1]

    def backward_out(is_last):
        reduce("q", qb, qr, qacc)
        inner = dot_over_units()
        inverse = rkeep[:, :1]
        if is_last:
            logit = rkeep[:, 1:2] + inverse * inner
            seed = rinfo[:, 0:1] * jnp.exp(logit - rinfo[:, 1:2])
            scale = seed * inverse
            pj[t, blk(j)] = (scale * pacc[...]).astype(BF)
        else:
            seed = jnp.ones((rows, 1), F32)
            scale = inverse
        gq[t, blk(j)] = (scale * qacc[...]).astype(BF)
        sc[j] = pack([inverse * inverse * inverse * (seed * inner) / width, seed])
        share("gq", gq, True)
        others(lambda b: send("sc", b, j, sc.at[j], sc.at[j], {"dp": b}))
        got("w", 0, w1o)

        def chunk(b):
            shared("gq", gq, b)

            @pl.when(b != j)
            def _():
                got("sc", b, sc.at[b])
            packed = unpack(sc[b])
            grad = dot(gq[t, blk(b)], w1[t], 1, 1) + dot(gq[o, blk(b)], w1o[...], 1, 1)
            upstream = us[t, blk(b)].astype(F32)
            if is_last:
                upstream = packed[:, 1:2] * upstream
            yg[blk(b)] = (
                upstream + gain(t) * grad - packed[:, 0:1] * xs[t, blk(b)].astype(F32)
            ).astype(BF)
            send("g", b, b, yg.at[blk(b)], us.at[t, blk(b)], {"section": s - 1})
        everyone(chunk)

    def tokens():
        others(lambda b: got("tk", b, tk.at[b]))
        count = tk[0]
        for b in range(1, n):
            count = count + tk[b]
        return 1.0 / count[0:1, 0:1]

    def finish_value(scale):
        for h in range(2):
            dw1[h] = dot(xg[h], gq[t], 0, 0) * scale

    def finish_value_arriving(scale):
        def add(b, start):
            for h in range(2):
                part = dot(xg[h, blk(b)], gq[t, blk(b)], 0, 0) * scale
                dw1[h] = part if start else dw1[h] + part
        add(j, True)

        def later(b):
            got("gq", b, gq.at[t, blk(b)])
            add(b, False)
        others(later)

    def finish_output(scale):
        for h in range(2):
            dw2[:, h * half:(h + 1) * half] = dot(pj[t], us[h], 0, 0) * scale

    def drain_common():
        sent("w", 0, w1o)
        sent("w", 1, w2o)

        def one(b):
            sent("tk", b, tk.at[b])
            sent("p", b, pb.at[blk(b)])
            sent("ps", b, ps.at[b])
            sent("q", b, qb.at[blk(b)])
            sent("pj", b, pj.at[t, blk(b)])
            sent("gq", b, gq.at[t, blk(b)])
        others(one)

    def first_section():
        start_common()
        all_to_all(xs)
        forward_chunk(j, False)

        def chunk(b):
            arrive("a", "xf", xs, b)
            forward_chunk(b, False)
        others(chunk)
        forward_out()

        def back(b):
            arrive("g", "uf", us, b)
            backward_chunk(b)
        everyone(back)
        scale = tokens()
        reduce("q", qb, qr, qacc)
        gq[t, blk(j)] = (rkeep[:, :1] * qacc[...]).astype(BF)
        share("gq", gq, False)
        finish_output(scale)
        finish_value_arriving(scale)
        got("w", 0, w1o)
        drain_common()

        def rest(b):
            sent("a", b, src.at[0])
            sent("xf", b, xs.at[t, blk(b)])
        others(rest)

        def rest_all(b):
            sent("pjf", b, pj.at[t, blk(b)])
            sent("x", b, yx.at[blk(b)])
            sent("uf", b, us.at[t, blk(b)])
        everyone(rest_all)

    def middle_section():
        start_common()

        def chunk(b):
            arrive("x", "xf", xs, b)
            forward_chunk(b, False)
        everyone(chunk)
        forward_out()

        def back(b):
            arrive("g", "uf", us, b)
            backward_chunk(b)
        everyone(back)
        backward_out(False)
        scale = tokens()
        finish_output(scale)
        finish_value(scale)
        drain_common()
        sent("e", 0, exs)
        others(lambda b: sent("sc", b, sc.at[b]))

        def rest_all(b):
            sent("xf", b, xs.at[t, blk(b)])
            sent("uf", b, us.at[t, blk(b)])
            sent("pjf", b, pj.at[t, blk(b)])
            sent("gqf", b, gq.at[t, blk(b)])
            sent("x", b, yx.at[blk(b)])
            sent("g", b, yg.at[blk(b)])
        everyone(rest_all)

    def last_section():
        start_common()
        all_to_all(us)
        backward_chunk(j)
        row_info()

        def seeds(b):
            arrive("a", "uf", us, b)
            backward_chunk(b)
        others(seeds)

        def chunk(b):
            arrive("x", "xf", xs, b)
            forward_chunk(b, True)
        everyone(chunk)
        own_inverse()
        reduce("p", pb, pr, pacc)
        backward_out(True)
        share("pj", pj, False)
        scale = tokens()
        finish_value(scale)
        others(lambda b: got("pj", b, pj.at[t, blk(b)]))
        finish_output(scale)
        got("w", 1, w2o)
        drain_common()
        sent("e", 0, exs)

        def rest(b):
            sent("a", b, src.at[0])
            sent("uf", b, us.at[t, blk(b)])
            sent("sc", b, sc.at[b])
        others(rest)

        def rest_all(b):
            sent("xf", b, xs.at[t, blk(b)])
            sent("gqf", b, gq.at[t, blk(b)])
            sent("g", b, yg.at[blk(b)])
        everyone(rest_all)

    pl.when(s == 0)(first_section)
    pl.when(s == last)(last_section)
    if sections > 2:
        pl.when((s > 0) & (s < last))(middle_section)


def local_chain(
    hidden, unembed, value_proj, output_proj, norm_gains, survive, lengths, assign,
    advantage, reference_logit, recorded_gap,
):
    n = lax.axis_size("dp")
    sections = lax.axis_size("section")
    s = lax.axis_index("section")
    count, positions, width = hidden.shape
    rows = count * positions
    part = value_proj.shape[1]
    half = part // 2
    v = value_proj.shape[2]

    src = jnp.where(s == sections - 1, unembed, hidden).reshape(rows, n * 2, half)
    src = src.transpose(1, 0, 2)
    w1 = value_proj[0].reshape(2, half, v)
    w2 = output_proj[0].reshape(v, 2, half).transpose(1, 0, 2)
    gains = norm_gains[0].reshape(n * 2, 1, half)
    total = n * rows
    kinds = len(KINDS)
    vm = pl.BlockSpec(memory_space=pltpu.VMEM)
    dw1, dw2 = pl.pallas_call(
        functools.partial(kernel, n, sections, width),
        out_shape=(
            jax.ShapeDtypeStruct((2, half, v), F32),
            jax.ShapeDtypeStruct((v, part), F32),
        ),
        in_specs=[vm] * 10,
        out_specs=(vm, vm),
        scratch_shapes=[
            pltpu.VMEM((2, total, half), BF),
            pltpu.VMEM((2, total, half), BF),
            pltpu.VMEM((2, total, half), BF),
            pltpu.VMEM((total, v), BF),
            pltpu.VMEM((n, rows, v), BF),
            pltpu.VMEM((total, v), BF),
            pltpu.VMEM((n, rows, v), BF),
            pltpu.VMEM((2, total, v), BF),
            pltpu.VMEM((2, total, v), BF),
            pltpu.VMEM((n, 8, rows), F32),
            pltpu.VMEM((half, v), BF),
            pltpu.VMEM((v, half), BF),
            pltpu.VMEM((total, half), BF),
            pltpu.VMEM((total, half), BF),
            pltpu.VMEM((n, 8, LANES), F32),
            pltpu.VMEM((rows, LANES), F32),
            pltpu.VMEM((rows, LANES), F32),
            pltpu.VMEM((rows, v), F32),
            pltpu.VMEM((rows, v), F32),
            pltpu.VMEM((rows, LANES), F32),
            pltpu.VMEM((n, 8, rows), F32),
            pltpu.VMEM((n, 8, rows), F32),
            pltpu.VMEM((rows, LANES), F32),
            pltpu.VMEM((8, LANES), F32),
            pltpu.SemaphoreType.DMA((kinds, n)),
            pltpu.SemaphoreType.DMA((kinds, n)),
        ],
        compiler_params=pltpu.CompilerParams(
            collective_id=0, has_side_effects=True, vmem_limit_bytes=60 * 1024 * 1024
        ),
    )(
        src, w1, w2, gains, survive.reshape(1, -1), lengths.reshape(1, count),
        assign.reshape(1, count), advantage.reshape(1, count), reference_logit.T, recorded_gap.T,
    )
    return (
        dw1.reshape(1, part, v),
        dw2[None],
    )


def pair_slots(n):
    sizes = {
        "a": n, "af": n, "ax": n, "axf": n, "bx": 1, "bf": 1, "by": 1, "ax1": 1, "af1": 1, "ay": 1, "gn": 1,
        "mr": n, "mk": n, "my": n, "rr": 3 * n, "rl": 3 * n, "ps": n, "p0": 2, "s0": 1, "in": 2, "w": 2,
        "d1": 2, "s1": 1, "g0": n, "g0x": n, "g0f": n, "g1": n, "gx": n, "g1f": n, "g2": n, "gs": n, "tk": n,
        "g0r": 0,
    }
    starts, total = {}, 0
    for kind, size in sizes.items():
        starts[kind] = total
        total += size
    return list(sizes), starts, total


def pair_kernel(
    n, width,
    hid, une, w1, w2, gains, survive, lengths, assign, advantage, base, gap,
    dw1, dw2,
    xs, us, xg, wv1, wv2, b0f, a1f, b0g, gx, mp, mr, mk, part, own, rin, p0, dp1, gz, ga, gb, gc,
    wr, wsend, ps, psr, scs, scr, inn, inr, sc, rinfo, tok, tk,
    ss, rs, ls,
):
    j = lax.axis_index("dp")
    s = lax.axis_index("section")
    t = lax.axis_index("tensor")
    y = lax.axis_index("groups")
    o = 1 - t
    rows = hid.shape[0]
    chunk, v = w1.shape
    half = chunk // 2
    mb = v // n
    positions, count = base.shape
    partner = {"tensor": o}
    right = {"dp": j + 1}
    left = {"dp": j - 1}
    lane = lax.broadcasted_iota(jnp.int32, (rows, LANES), 1)
    kinds, starts, _ = pair_slots(n)
    near = max(n // 2, 1)
    relayed = n == 2 * near and 0 < near * (near - 1) <= n
    side = j // near
    gate = jnp.where(side == 0, near - 1, near)
    most = pl.ds(0, (n - 1) * rows)

    def blk(b):
        return pl.ds(pl.multiple_of(b * rows, rows), rows)

    def cols(h):
        return pl.ds(pl.multiple_of(h * half, half), half)

    def wide(b, h):
        return pl.ds(pl.multiple_of(b * chunk + h * half, half), half)

    def mrows(g, b):
        return pl.ds(pl.multiple_of(g * v + b * mb, mb), mb)

    def send(kind, ri, a, b, dev, through=""):
        slot = kinds.index("rr" if kind == "rl" else kind + through)
        pltpu.make_async_remote_copy(
            src_ref=a, dst_ref=b, send_sem=ss.at[slot], recv_sem=rs.at[starts[kind] + ri],
            device_id=dev, device_id_type=pl.DeviceIdType.MESH,
        ).start()

    def got(kind, i, a):
        pltpu.make_async_remote_copy(
            src_ref=a, dst_ref=a, send_sem=ss.at[kinds.index(kind)], recv_sem=rs.at[starts[kind] + i],
            device_id=partner, device_id_type=pl.DeviceIdType.MESH,
        ).wait_recv()

    def sent(kind, a):
        pltpu.make_async_remote_copy(
            src_ref=a, dst_ref=a, send_sem=ss.at[kinds.index(kind)], recv_sem=rs.at[0],
            device_id=partner, device_id_type=pl.DeviceIdType.MESH,
        ).wait_send()

    def others(body):
        def step(k, carry):
            body(lax.rem(j + k, n))
            return carry
        lax.fori_loop(1, n, step, 0)

    def at_distance(d, body):
        pl.when(j + d < n)(lambda: body(j + d))
        pl.when(j - d >= 0)(lambda: body(j - d))

    def pack(values):
        packed = jnp.zeros((rows, LANES), F32)
        for i, value in enumerate(values):
            packed = jnp.where(lane == i, value, packed)
        return packed.T[:8]

    def unpack(packed):
        return jnp.concatenate([packed, jnp.zeros((LANES - 8, rows), F32)], axis=0).T

    def own_tokens():
        response = lax.broadcasted_iota(jnp.int32, (1, count), 1)
        group = count // survive.shape[1]
        kept = jnp.zeros((1, count), F32)
        for g in range(survive.shape[1]):
            inside = (response >= g * group) & (response < (g + 1) * group)
            kept = jnp.where(inside, survive[0:1, g:g + 1].astype(F32), kept)
        held = jnp.sum(kept * lengths[...].astype(F32), axis=1, keepdims=True)
        tok[...] = jnp.broadcast_to(held, (8, LANES))
        others(lambda b: send("tk", j, tok, tk.at[j], {"dp": b}))
        tk[j] = tok[...]

    def tokens():
        others(lambda b: got("tk", b, tk.at[b]))
        total = tk[0]
        for b in range(1, n):
            total = total + tk[b]
        return 1.0 / total[0:1, 0:1]

    def row_info():
        row = lax.broadcasted_iota(jnp.int32, (rows, count), 0)
        first = lax.broadcasted_iota(jnp.int32, (rows, count), 1) * positions
        mine = (row >= first) & (row < first + positions)

        def by_response(values):
            return jnp.sum(jnp.where(mine, values, 0.0), axis=1, keepdims=True)

        def by_position(values):
            return by_response(jnp.concatenate([values] * count, axis=0))

        slots = assign[...]
        starts = slots * positions
        hit = (row >= starts) & (row < starts + positions)
        listed = jnp.sum(jnp.where(hit, 1.0, 0.0), axis=1, keepdims=True)
        start = by_response(first.astype(F32))
        place = lax.broadcasted_iota(jnp.int32, (rows, 1), 0).astype(F32) - start
        live = place < by_response(lengths[...].astype(F32))
        adv = by_response(advantage[...])
        q = by_position(gap[...])
        clipped = ((adv > 0) & (q > clip_high)) | ((adv < 0) & (q < clip_low))
        weight = jnp.where(clipped | (~live), 0.0, -loss_scale * adv * listed)
        rinfo[...] = jnp.where(lane == 0, weight, jnp.where(lane == 1, by_position(base[...]), 0.0))

    def local_copy(i, a, b):
        return pltpu.make_async_copy(a, b, ls.at[i])

    def reduce_step(q, d, at_end):
        slot = q * n

        def onward(kind, way, r, dev):
            if not at_end:
                got(kind, slot + r, rin.at[way, q, r])
                part[q, r] = (part[q, r].astype(F32) + rin[way, q, r].astype(F32)).astype(BF)
            send(kind, slot + r, part.at[q, r], rin.at[way, q, r], dev)

        first = j == 0 if at_end else (j > 0) & (j + d < n)
        final = j == n - 1 if at_end else (j < n - 1) & (j - d >= 0)
        pl.when(first)(lambda: onward("rr", 0, j + d, right))
        pl.when(final)(lambda: onward("rl", 1, j - d, left))

    def reduce_inner(q, most, least=1):
        for d in range(most, least - 1, -1):
            reduce_step(q, d, False)

    def reduce_own(q):
        slot = q * n + j

        @pl.when(j > 0)
        def _():
            got("rr", slot, rin.at[0, q, j])
            own[q] += rin[0, q, j].astype(F32)

        @pl.when(j < n - 1)
        def _():
            got("rl", slot, rin.at[1, q, j])
            own[q] += rin[1, q, j].astype(F32)

    def gather(kind, at):
        for d in range(n - 1, 0, -1):
            at_distance(d, lambda b: send(kind, j, at(j), at(j), {"dp": b}))

    def gather_near(kind, at):
        if not relayed:
            return gather(kind, at)
        across = jnp.where(side == 0, near, near - 1)
        for d in range(n - 1, 0, -1):
            at_distance(d, lambda b: pl.when((b // near == side) | (b == across))(
                lambda: send(kind, j, at(j), at(j), {"dp": b})
            ))

    def hand_on(kind, at):
        if not relayed:
            return

        def one(b):
            got(kind, b, at(b))
            for r in range(n):
                pl.when((r // near == side) & (r != j))(
                    lambda: send(kind, b, at(b), at(b), {"dp": r}, "r")
                )
        for d in range(1, n):
            at_distance(d, lambda b: pl.when((j == gate) & (b // near != side))(lambda: one(b)))

    def handed(kind, at, b):
        if not relayed:
            return got(kind, b, at(b))
        pl.when((j != gate) | (b // near == side))(lambda: got(kind, b, at(b)))

    def gather_sent(kind, whole):
        if not relayed:
            return sent(kind, whole.at[most])
        sent(kind, whole.at[pl.ds(0, near * rows)])
        pl.when(j == gate)(lambda: sent(kind + "r", whole.at[pl.ds(0, near * (near - 1) * rows)]))

    def at_p0(b):
        return p0.at[t, blk(b)]

    def at_dp1(b):
        return dp1.at[t, blk(b)]

    def at_gz(b):
        return gz.at[blk(b)]

    def scalar_sums():
        psr[j] = ps[j]
        others(lambda b: got("ps", b, psr.at[b]))
        sums = psr[0]
        for b in range(1, n):
            sums = sums + psr[b]
        return unpack(sums)[:, 0:1]

    def gram_send():
        others(lambda b: send("mr", j, mp.at[b], mr.at[j], {"dp": b}))

    def gram_reduce():
        mr[j] = mp[j]
        others(lambda b: got("mr", b, mr.at[b]))
        total = mr[0].astype(F32)
        for b in range(1, n):
            total = total + mr[b].astype(F32)
        mk[mrows(y, j)] = total.astype(BF)
        here = mk.at[mrows(y, j)]
        others(lambda b: send("mk", j, here, here, {"dp": b}))
        send("my", j, here, here, {"groups": 1 - y})

    def gram_pass():
        def across(b):
            here = mk.at[mrows(y, b)]
            got("mk", b, here)
            send("my", b, here, here, {"groups": 1 - y})
        others(across)

    def gram_wait():
        for b in range(n):
            got("my", b, mk.at[mrows(1 - y, b)])

    def store_gram(value):
        value = value.astype(BF)
        for b in range(n):
            mp[b] = value[b * mb:(b + 1) * mb]

    def main_send(src, main, d):
        at_distance(d, lambda b: send(
            "a", j, src.at[:, wide(b, t)], main.at[blk(j), cols(t)], {"dp": b}
        ))

    def main_start(src, other_src, main, other):
        for d in range(n - 1, 1, -1):
            main_send(src, main, d)
        local_copy(0, src.at[:, pl.ds(pl.multiple_of(j * chunk, chunk), chunk)], main.at[blk(j)]).start()
        local_copy(1, other_src.at[:, pl.ds(pl.multiple_of(j * chunk, chunk), chunk)], other.at[blk(j)]).start()

    def main_wait(src, other_src, main, other):
        local_copy(0, src.at[:, pl.ds(0, chunk)], main.at[blk(j)]).wait()
        local_copy(1, other_src.at[:, pl.ds(0, chunk)], other.at[blk(j)]).wait()

    def main_arrive(main, d):
        def first(b):
            here = main.at[blk(b), cols(t)]
            got("a", b, here)
            send("ax", b, here, here, {"section": 1 - s})
            send("af", b, here, here, partner)
        at_distance(d, first)
        at_distance(d, lambda b: got("af", b, main.at[blk(b), cols(o)]))

    def other_take(other):
        def first(b):
            here = other.at[blk(b), cols(t)]
            got("ax", b, here)
            send("axf", b, here, here, partner)
        for d in range(n - 1, 0, -1):
            at_distance(d, first)

    def other_arrive(other, d):
        at_distance(d, lambda b: got("axf", b, other.at[blk(b), cols(o)]))

    barrier = pltpu.get_barrier_semaphore()

    def greet(dev):
        pl.semaphore_signal(barrier, inc=1, device_id=dev, device_id_type=pl.DeviceIdType.MESH)

    def meet():
        others(lambda b: greet({"dp": b}))
        greet({"groups": 1 - y})
        greet(partner)
        greet({"section": 1 - s})
        greet({"section": 1 - s, "tensor": o})
        pl.semaphore_wait(barrier, n + 3)

    def drain_common(main, other, sums):
        for kind in ("a", "ax", "af"):
            sent(kind, main.at[most, pl.ds(0, half)])
        sent("axf", other.at[most, pl.ds(0, half)])
        sent("mr", mp.at[pl.ds(0, n - 1)])
        sent("mk", mk.at[pl.ds(0, (n - 1) * mb)])
        sent("my", mk.at[pl.ds(0, n * mb)])
        sent("ps", ps.at[pl.ds(0, n - 1)])
        sent("tk", tk.at[pl.ds(0, n - 1)])
        sent("gs", sc.at[pl.ds(0, n - 1)])
        sent("rr", part.at[pl.ds(0, sums), pl.ds(0, n - 1)])
        sent("g0f", gz.at[most])
        sent("bf", b0f.at[t])

    def first_section():
        local_copy(2, w1, wv1).start()
        local_copy(3, w2, b0f.at[t]).start()
        meet()
        @pl.when(t == y)
        def _():
            send("bx", 0, w2, b0f.at[t], {"section": 1})
        main_start(hid, une, xs, us)
        send("bf", 0, w2, b0f.at[t], partner)
        own_tokens()
        row_info()
        local_copy(2, w1, wv1).wait()
        local_copy(3, w2, b0f.at[t]).wait()
        main_wait(hid, une, xs, us)

        def project(b):
            x = xs[blk(b)].astype(F32)
            ps[b] = pack([jnp.sum(x * x, axis=1, keepdims=True)])
            xg[blk(b)] = (x * gains[j]).astype(BF)
            return dot(xg[blk(b)], wv1[...]), dot(xs[blk(b)], b0f[t], 1, 1)

        def project_main(b):
            pa, pb = project(b)
            part[0, b] = pa.astype(BF)
            part[1, b] = pb.astype(BF)
            send("ps", j, ps.at[b], psr.at[j], {"dp": b})

        def project_other(b):
            part[2, b] = dot(us[blk(b)], b0f[t], 1, 1).astype(BF)

        own[0], own[1] = project(j)
        own[2] = dot(us[blk(j)], b0f[t], 1, 1)
        got("bf", 0, b0f.at[o])
        store_gram(dot(b0f[y], b0f[t], 1, 1))
        gram_send()
        main_send(hid, xs, 1)
        for d in range(n - 1, 0, -1):
            main_arrive(xs, d)
            at_distance(d, project_main)
            reduce_step(0, d, True)
            reduce_step(1, d, True)
        reduce_inner(0, n - 2)
        reduce_inner(1, n - 2, 2)
        gram_reduce()
        other_take(us)
        for d in range(n - 1, 0, -1):
            other_arrive(us, d)
            at_distance(d, project_other)
            reduce_step(2, d, True)
        reduce_inner(1, 1)
        reduce_own(0)
        xx = scalar_sums()
        inverse = lax.rsqrt(xx / width + eps_norm)
        p0[t, blk(j)] = (inverse * own[0]).astype(BF)
        send("p0", t, at_p0(j), at_p0(j), partner)
        for c in range(2):
            send("p0", t, at_p0(j), at_p0(j), {"section": 1, "tensor": c})
        reduce_inner(2, n - 2, 2)
        gram_pass()
        reduce_inner(2, 1)
        gather_near("g0", at_p0)

        @pl.when(t == y)
        def _():
            got("ax1", 0, a1f.at[t])
            send("ay", 0, a1f.at[t], a1f.at[t], {"groups": 1 - y})
            send("af1", 0, a1f.at[t], a1f.at[t], partner)
        hand_on("g0", at_p0)
        reduce_own(1)
        reduce_own(2)
        gram_wait()
        got("p0", o, p0.at[o, blk(j)])
        kb = own[1] + dot(p0[0, blk(j)], mk[0:v]) + dot(p0[1, blk(j)], mk[v:2 * v])
        p0v = p0[t, blk(j)].astype(F32)
        scs[...] = pack([
            jnp.sum(p0v * (own[1] + kb), axis=1, keepdims=True),
            jnp.sum(p0v * own[2], axis=1, keepdims=True),
        ])
        send("s0", 0, scs, scr, partner)
        own[1] = kb
        got("w", 0, wr.at[0])
        got("w", 1, wr.at[1])
        got("in", 0, inr.at[0])
        got("in", 1, inr.at[1])
        got("s0", 0, scr)
        sums = unpack(scs[...] + scr[...])
        squares = xx + sums[:, 0:1]
        raised_inverse = lax.rsqrt(jnp.maximum(squares, 0.0) / width + eps_norm)
        inner = unpack(inr[0] + inr[1])[:, 0:2]
        logit = 0.5 * inner[:, 1:2] + sums[:, 1:2] + raised_inverse * inner[:, 0:1]
        weight = rinfo[:, 0:1]
        seed = jnp.where(weight == 0.0, 0.0, weight * jnp.exp(logit - rinfo[:, 1:2]))
        scaled = seed * raised_inverse
        pull = raised_inverse * raised_inverse * raised_inverse * (seed * inner[:, 0:1]) / width
        grad = seed * own[2] - pull * own[1] + scaled * (wr[0].astype(F32) + wr[1].astype(F32))
        gz[blk(j)] = (inverse * grad).astype(BF)
        sc[j] = pack([seed, scaled, pull])
        send("s1", 0, sc.at[j], sc.at[j], {"section": 1})
        others(lambda b: send("gs", j, sc.at[j], sc.at[j], {"dp": b}))
        gather("g2", at_gz)

        def pass_p0(b):
            handed("g0", at_p0, b)
            send("g0f", b, at_p0(b), at_p0(b), partner)
            send("g0x", b, at_p0(b), at_p0(b), {"section": 1})
        for d in range(1, n):
            at_distance(d, pass_p0)
        scale = tokens()
        others(lambda b: got("gs", b, sc.at[b]))
        others(lambda b: got("g0f", b, p0.at[o, blk(b)]))
        for b in range(n):
            packed = unpack(sc[b])
            held = p0[t, blk(b)].astype(F32)
            for h in range(2):
                gb[h, blk(b)] = (-packed[:, 2:3] * p0[h, blk(b)].astype(F32)).astype(BF)
            ga[blk(b)] = (packed[:, 0:1] * held).astype(BF)
            gc[blk(b)] = (packed[:, 1:2] * held).astype(BF)
        dw2[...] = dot(ga[...], us[...], 0, 0) + dot(gb[t], xs[...], 0, 0)
        for h in range(2):
            dw2[...] += dot(dot(p0[t], gb[h], 0, 0).astype(BF), b0f[h])

        @pl.when(t != y)
        def _():
            got("ay", 0, a1f.at[t])
            send("af1", 0, a1f.at[t], a1f.at[t], partner)
        got("gn", 0, gx)

        def pass_dp1(b):
            got("gx", b, at_dp1(b))
            send("g1f", b, at_dp1(b), at_dp1(b), partner)
        for d in range(1, n):
            at_distance(d, pass_dp1)
        got("d1", t, at_dp1(j))
        got("d1", o, dp1.at[o, blk(j)])
        got("af1", 0, a1f.at[o])
        others(lambda b: got("g1f", b, dp1.at[o, blk(b)]))
        through = jnp.zeros((v, chunk), F32)
        for h in range(2):
            through += dot(dot(gc[...], dp1[h], 0, 0).astype(BF), a1f[h], 1, 1)
        dw2[...] = (dw2[...] + gx[...] * through) * scale
        others(lambda b: got("g2", b, at_gz(b)))
        dw1[...] = dot(xg[...], gz[...], 0, 0) * scale
        drain_common(xs, us, 3)

        @pl.when(t == y)
        def _():
            sent("bx", b0f.at[t])
            sent("ay", a1f.at[t])
        sent("af1", a1f.at[t])
        sent("p0", part.at[:, 0])
        sent("s0", scs)
        sent("s1", scs)
        gather_sent("g0", gz)
        sent("g2", gz.at[most])
        sent("g0x", gz.at[most])
        sent("g1f", gz.at[most])

    def second_section():
        local_copy(2, w1, a1f.at[t]).start()
        local_copy(3, w2, wv2).start()
        meet()
        main_start(une, hid, us, xs)
        own_tokens()
        local_copy(2, w1, a1f.at[t]).wait()
        local_copy(3, w2, wv2).wait()
        main_wait(une, hid, us, xs)

        def project_main(b):
            part[0, b] = dot(us[blk(b)], wv2[...], 1, 1).astype(BF)

        def project(b):
            x = xs[blk(b)].astype(F32)
            ps[b] = pack([jnp.sum(x * us[blk(b)].astype(F32), axis=1, keepdims=True)])
            xg[blk(b)] = (x * gains[j]).astype(BF)
            return dot(xg[blk(b)], a1f[t])

        def project_other(b):
            part[1, b] = project(b).astype(BF)
            send("ps", j, ps.at[b], psr.at[j], {"dp": b})

        own[0] = dot(us[blk(j)], wv2[...], 1, 1)
        own[1] = project(j)
        main_send(une, us, 1)

        def take_b0():
            @pl.when(t == y)
            def _():
                got("bx", 0, b0f.at[t])
                send("bf", 0, b0f.at[t], b0f.at[t], partner)
                send("by", 0, b0f.at[t], b0f.at[t], {"groups": 1 - y})

            @pl.when(t != y)
            def _():
                got("bf", 0, b0f.at[o])

        def take_rest():
            @pl.when(t != y)
            def _():
                got("by", 0, b0f.at[t])
                send("bf", 0, b0f.at[t], b0f.at[t], partner)

            @pl.when(t == y)
            def _():
                got("bf", 0, b0f.at[o])

        for d in range(n - 1, 0, -1):
            main_arrive(us, d)
            at_distance(d, project_main)
            reduce_step(0, d, True)
            if d == min(2, n - 1):
                take_b0()
                b0g[y] = (b0f[y].astype(F32) * gains[j]).astype(BF)
                store_gram(dot(b0g[y], a1f[t]))
                gram_send()
        @pl.when(t == y)
        def _():
            send("ax1", 0, w1, a1f.at[t], {"section": 0})
        send("gn", 0, gains.at[j], gx, {"section": 0})
        reduce_inner(0, n - 2)
        gram_reduce()
        other_take(xs)
        for d in range(n - 1, 0, -1):
            other_arrive(xs, d)
            at_distance(d, project_other)
            reduce_step(1, d, True)
        reduce_inner(1, n - 2, 2)
        gram_pass()
        reduce_inner(1, 1)
        reduce_own(0)
        dp1[t, blk(j)] = own[0].astype(BF)
        gram_wait()
        back = dot(dp1[t, blk(j)], mk[...], 1, 1).astype(BF)
        for c in range(2):
            wsend[c] = back[:, c * v:(c + 1) * v]
            send("w", t, wsend.at[c], wr.at[t], {"section": 0, "tensor": c})
        reduce_own(1)
        dotted = scalar_sums()
        gather("g1", at_dp1)
        got("p0", 0, p0.at[0, blk(j)])
        got("p0", 1, p0.at[1, blk(j)])
        raised = own[1] + dot(p0[0, blk(j)], mk[0:v]) + dot(p0[1, blk(j)], mk[v:2 * v])
        inn[...] = pack([jnp.sum(raised * own[0], axis=1, keepdims=True), dotted])
        for c in range(2):
            send("in", t, inn, inr.at[t], {"section": 0, "tensor": c})
        for c in range(2):
            send("d1", t, at_dp1(j), at_dp1(j), {"section": 0, "tensor": c})
        gz[blk(j)] = raised.astype(BF)
        gather("g2", at_gz)

        def pass_dp1(b):
            got("g1", b, at_dp1(b))
            send("gx", b, at_dp1(b), at_dp1(b), {"section": 0})

        for d in range(1, n):
            at_distance(d, pass_dp1)
        got("s1", 0, sc.at[j])
        others(lambda b: send("gs", j, sc.at[j], sc.at[j], {"dp": b}))
        take_rest()
        for h in range(2):
            b0g[h] = (b0f[h].astype(F32) * gains[j]).astype(BF)
        scale = tokens()

        def pass_p0(b):
            got("g0x", b, at_p0(b))
            send("g0f", b, at_p0(b), at_p0(b), partner)
        for d in range(1, n):
            at_distance(d, pass_p0)
        others(lambda b: got("g0f", b, p0.at[o, blk(b)]))
        others(lambda b: got("g2", b, at_gz(b)))
        others(lambda b: got("gs", b, sc.at[b]))
        for b in range(n):
            scaled = unpack(sc[b])[:, 1:2]
            ga[blk(b)] = (scaled * gz[blk(b)].astype(F32)).astype(BF)
            gc[blk(b)] = (scaled * dp1[t, blk(b)].astype(F32)).astype(BF)
        dw2[...] = dot(ga[...], us[...], 0, 0) * scale
        total = dot(xg[...], gc[...], 0, 0)
        for h in range(2):
            total += dot(b0g[h], dot(p0[h], gc[...], 0, 0).astype(BF), 0, 0)
        dw1[...] = total * scale
        drain_common(us, xs, 2)

        @pl.when(t == y)
        def _():
            sent("ax1", a1f.at[t])
            sent("by", b0f.at[t])
        sent("gn", gx)
        sent("g1", gz.at[most])
        sent("g2", gz.at[most])
        sent("gx", ga.at[most])
        sent("in", inr)
        sent("w", wsend)
        sent("d1", part.at[pl.ds(0, 2), 0])

    pl.when(s == 0)(first_section)
    pl.when(s == 1)(second_section)


def local_pair(
    hidden, unembed, value_proj, output_proj, norm_gains, survive, lengths, assign,
    advantage, reference_logit, recorded_gap,
):
    n = lax.axis_size("dp")
    count, positions, width = hidden.shape
    rows = count * positions
    chunk, v = value_proj.shape[1:]
    total = n * rows
    kinds, _, slots = pair_slots(n)
    vm = pl.BlockSpec(memory_space=pltpu.VMEM)
    hbm = pl.BlockSpec(memory_space=pl.ANY)
    dw1, dw2 = pl.pallas_call(
        functools.partial(pair_kernel, n, width),
        out_shape=(
            pltpu.VMEM((chunk, v), F32),
            pltpu.VMEM((v, chunk), F32),
        ),
        in_specs=[hbm] * 4 + [vm] * 7,
        out_specs=(vm, vm),
        scratch_shapes=[
            pltpu.VMEM((total, chunk), BF),
            pltpu.VMEM((total, chunk), BF),
            pltpu.VMEM((total, chunk), BF),
            pltpu.VMEM((chunk, v), BF),
            pltpu.VMEM((v, chunk), BF),
            pltpu.VMEM((2, v, chunk), BF),
            pltpu.VMEM((2, chunk, v), BF),
            pltpu.VMEM((2, v, chunk), BF),
            pltpu.VMEM((1, chunk), F32),
            pltpu.VMEM((n, v // n, v), BF),
            pltpu.VMEM((n, v // n, v), BF),
            pltpu.VMEM((2 * v, v), BF),
            pltpu.VMEM((3, n, rows, v), BF),
            pltpu.VMEM((3, rows, v), F32),
            pltpu.VMEM((2, 3, n, rows, v), BF),
            pltpu.VMEM((2, total, v), BF),
            pltpu.VMEM((2, total, v), BF),
            pltpu.VMEM((total, v), BF),
            pltpu.VMEM((total, v), BF),
            pltpu.VMEM((2, total, v), BF),
            pltpu.VMEM((total, v), BF),
            pltpu.VMEM((2, rows, v), BF),
            pltpu.VMEM((2, rows, v), BF),
            pltpu.VMEM((n, 8, rows), F32),
            pltpu.VMEM((n, 8, rows), F32),
            pltpu.VMEM((8, rows), F32),
            pltpu.VMEM((8, rows), F32),
            pltpu.VMEM((8, rows), F32),
            pltpu.VMEM((2, 8, rows), F32),
            pltpu.VMEM((n, 8, rows), F32),
            pltpu.VMEM((rows, LANES), F32),
            pltpu.VMEM((8, LANES), F32),
            pltpu.VMEM((n, 8, LANES), F32),
            pltpu.SemaphoreType.DMA((len(kinds),)),
            pltpu.SemaphoreType.DMA((slots,)),
            pltpu.SemaphoreType.DMA((4,)),
        ],
        compiler_params=pltpu.CompilerParams(
            collective_id=0, has_side_effects=True, vmem_limit_bytes=60 * 1024 * 1024
        ),
    )(
        hidden.reshape(rows, width), unembed.reshape(rows, width), value_proj[0], output_proj[0],
        norm_gains[0].reshape(n, 1, chunk), survive.reshape(1, -1), lengths.reshape(1, count),
        assign.reshape(1, count), advantage.reshape(1, count), reference_logit.T, recorded_gap.T,
    )
    return dw1[None], dw2[None]


def solution(mesh):
    rowwise = P(("groups", "dp"))
    placed = (
        P(("groups", "dp"), None, None),
        P(("groups", "dp"), None, None),
        P("section", "dp", "tensor"),
        P("section", "tensor", "dp"),
        P("section", None),
        rowwise,
        rowwise,
        rowwise,
        rowwise,
        P(("groups", "dp"), None),
        P(("groups", "dp"), None),
    )
    shape = mesh.shape
    paired = shape["section"] == 2 and shape["tensor"] == 2 and shape["groups"] == 2
    return jax.shard_map(
        local_pair if paired else local_chain,
        mesh=mesh,
        in_specs=placed,
        out_specs=(
            P(("groups", "section"), "dp", "tensor"),
            P(("groups", "section"), "tensor", "dp"),
        ),
        check_vma=False,
    )
```

```python
import functools
import math

import jax
import jax.numpy as jnp
from jax import lax
from jax.experimental import pallas as pl
from jax.experimental.pallas import tpu as pltpu
from jax.sharding import PartitionSpec as P

eps_norm = 1e-06
loss_scale = 4096.0
clip_high = math.log(1.28)
clip_low = math.log(0.8)
LANES = 128
KINDS = ("a", "xf", "uf", "p", "q", "pj", "pjf", "gq", "gqf", "sc", "tk", "x", "g", "w", "e", "ps")
BF = jnp.bfloat16
F32 = jnp.float32


def dot(a, b, ca=1, cb=0):
    return lax.dot_general(a, b, (((ca,), (cb,)), ((), ())), preferred_element_type=F32)


def kernel(
    n, sections, width,
    src, w1, w2, gains, survive, lengths, assign, advantage, base, gap,
    dw1, dw2,
    xs, us, xg, pb, pr, qb, qr, pj, gq, sc, w1o, w2o, yx, yg, tk, exs, exr, pacc, qacc, rkeep,
    ps, psr, rinfo, tok,
    ss, rs,
):
    j = lax.axis_index("dp")
    s = lax.axis_index("section")
    t = lax.axis_index("tensor")
    o = 1 - t
    rows = src.shape[1]
    half, v = w1.shape[1:]
    last = sections - 1
    partner = {"tensor": o}
    positions, count = base.shape

    def gain(h):
        return gains[j * 2 + h]

    def own_tokens():
        response = lax.broadcasted_iota(jnp.int32, (1, count), 1)
        group = count // survive.shape[1]
        kept = jnp.zeros((1, count), F32)
        for g in range(survive.shape[1]):
            inside = (response >= g * group) & (response < (g + 1) * group)
            kept = jnp.where(inside, survive[0:1, g:g + 1].astype(F32), kept)
        held = jnp.sum(kept * lengths[...].astype(F32), axis=1, keepdims=True)
        tok[...] = jnp.broadcast_to(held, (8, LANES))

    def row_info():
        row = lax.broadcasted_iota(jnp.int32, (rows, count), 0)
        first = lax.broadcasted_iota(jnp.int32, (rows, count), 1) * positions
        mine = (row >= first) & (row < first + positions)

        def by_response(values):
            return jnp.sum(jnp.where(mine, values, 0.0), axis=1, keepdims=True)

        def by_position(values):
            return by_response(jnp.concatenate([values] * count, axis=0))

        slots = assign[...]
        starts = slots * positions
        hit = (row >= starts) & (row < starts + positions)
        listed = jnp.sum(jnp.where(hit, 1.0, 0.0), axis=1, keepdims=True)
        start = by_response(first.astype(F32))
        place = lax.broadcasted_iota(jnp.int32, (rows, 1), 0).astype(F32) - start
        live = place < by_response(lengths[...].astype(F32))
        adv = by_response(advantage[...])
        q = by_position(gap[...])
        clipped = ((adv > 0) & (q > clip_high)) | ((adv < 0) & (q < clip_low))
        weight = jnp.where(clipped | (~live), 0.0, -loss_scale * adv * listed)
        rinfo[...] = jnp.where(lane == 0, weight, jnp.where(lane == 1, by_position(base[...]), 0.0))

    def blk(b):
        return pl.ds(pl.multiple_of(b * rows, rows), rows)

    def peer(k):
        return lax.rem(j + k, n)

    def send(kind, si, ri, a, b, dev):
        k = KINDS.index(kind)
        pltpu.make_async_remote_copy(
            src_ref=a, dst_ref=b, send_sem=ss.at[k, si], recv_sem=rs.at[k, ri],
            device_id=dev, device_id_type=pl.DeviceIdType.MESH,
        ).start()

    def handle(kind, i, a):
        k = KINDS.index(kind)
        return pltpu.make_async_remote_copy(
            src_ref=a, dst_ref=a, send_sem=ss.at[k, i], recv_sem=rs.at[k, i],
            device_id=partner, device_id_type=pl.DeviceIdType.MESH,
        )

    def got(kind, i, a):
        handle(kind, i, a).wait_recv()

    def sent(kind, i, a):
        handle(kind, i, a).wait_send()

    def others(body):
        def step(k, carry):
            body(peer(k))
            return carry
        lax.fori_loop(1, n, step, 0)

    def everyone(body):
        def step(k, carry):
            body(peer(k))
            return carry
        lax.fori_loop(0, n, step, 0)

    barrier = pltpu.get_barrier_semaphore()

    def greet(dev):
        pl.semaphore_signal(barrier, inc=1, device_id=dev, device_id_type=pl.DeviceIdType.MESH)

    for k in range(1, n):
        greet({"dp": peer(k)})
    greet(partner)

    @pl.when(s > 0)
    def _():
        greet({"section": s - 1})

    @pl.when(s < last)
    def _():
        greet({"section": s + 1})

    pl.semaphore_wait(barrier, n + jnp.where(s > 0, 1, 0) + jnp.where(s < last, 1, 0))

    def start_common():
        send("w", 0, 0, w1.at[o], w1o, partner)
        send("w", 1, 1, w2.at[o], w2o, partner)
        own_tokens()
        others(lambda b: send("tk", b, j, tok, tk.at[j], {"dp": b}))
        tk[j] = tok[...]

    def all_to_all(dst):
        others(lambda b: send("a", b, j, src.at[b * 2 + t], dst.at[t, blk(j)], {"dp": b}))
        dst[0, blk(j)] = src[j * 2]
        dst[1, blk(j)] = src[j * 2 + 1]

    def arrive(kind, fkind, buf, b):
        got(kind, b, buf.at[t, blk(b)])
        send(fkind, b, b, buf.at[t, blk(b)], buf.at[t, blk(b)], partner)
        got(fkind, b, buf.at[o, blk(b)])

    lane = lax.broadcasted_iota(jnp.int32, (rows, LANES), 1)

    def pack(values):
        packed = jnp.zeros((rows, LANES), F32)
        for i, value in enumerate(values):
            packed = jnp.where(lane == i, value, packed)
        return packed.T[:8]

    def unpack(packed):
        filled = jnp.concatenate([packed, jnp.zeros((LANES - 8, rows), F32)], axis=0)
        return filled.T

    def forward_chunk(b, with_logit):
        total = jnp.zeros((rows, v), F32)
        squares = jnp.zeros((rows, 1), F32)
        logit = jnp.zeros((rows, 1), F32)
        for h in range(2):
            x = xs[h, blk(b)].astype(F32)
            squares += jnp.sum(x * x, axis=1, keepdims=True)
            if with_logit:
                logit += jnp.sum(x * us[h, blk(b)].astype(F32), axis=1, keepdims=True)
            scaled = (x * gain(h)).astype(BF)
            xg[h, blk(b)] = scaled
            total += dot(scaled, w1[h])
        pb[blk(b)] = total.astype(BF)
        ps[b] = pack([squares, logit] if with_logit else [squares])

        @pl.when(b != j)
        def _():
            send("p", b, j, pb.at[blk(b)], pr.at[j], {"dp": b})
            send("ps", b, j, ps.at[b], psr.at[j], {"dp": b})

    def backward_chunk(b):
        total = dot(us[0, blk(b)], w2[0], 1, 1) + dot(us[1, blk(b)], w2[1], 1, 1)
        qb[blk(b)] = total.astype(BF)

        @pl.when(b != j)
        def _():
            send("q", b, j, qb.at[blk(b)], qr.at[j], {"dp": b})

    def reduce(kind, own, landed, acc):
        acc[...] = own[blk(j)].astype(F32)

        def add(b):
            got(kind, b, landed.at[b])
            acc[...] += landed[b].astype(F32)
        others(add)

    def share(kind, buf, forward):
        others(lambda b: send(kind, b, j, buf.at[t, blk(j)], buf.at[t, blk(j)], {"dp": b}))
        if forward:
            send(kind + "f", j, j, buf.at[t, blk(j)], buf.at[t, blk(j)], partner)

    def shared(kind, buf, b):
        @pl.when(b != j)
        def _():
            got(kind, b, buf.at[t, blk(b)])
            send(kind + "f", b, b, buf.at[t, blk(b)], buf.at[t, blk(b)], partner)
        got(kind + "f", b, buf.at[o, blk(b)])

    def own_inverse():
        psr[j] = ps[j]
        others(lambda b: got("ps", b, psr.at[b]))
        sums = psr[0]
        for b in range(1, n):
            sums = sums + psr[b]
        sums = unpack(sums)
        inverse = lax.rsqrt(sums[:, 0:1] / width + eps_norm)
        rkeep[...] = jnp.where(lane == 0, inverse, sums)
        return inverse

    def forward_out():
        inverse = own_inverse()
        reduce("p", pb, pr, pacc)
        pj[t, blk(j)] = (inverse * pacc[...]).astype(BF)
        share("pj", pj, True)
        got("w", 1, w2o)

        def chunk(b):
            shared("pj", pj, b)
            mixed = dot(pj[t, blk(b)], w2[t]) + dot(pj[o, blk(b)], w2o[...])
            yx[blk(b)] = (xs[t, blk(b)].astype(F32) + mixed).astype(BF)
            send("x", b, b, yx.at[blk(b)], xs.at[t, blk(b)], {"section": s + 1})
        everyone(chunk)

    def dot_over_units():
        exs[...] = jnp.broadcast_to(
            jnp.sum(pacc[...] * qacc[...], axis=1, keepdims=True), (rows, LANES)
        )
        send("e", 0, 0, exs, exr, partner)
        got("e", 0, exr)
        return exs[:, :1] + exr[:, :1]

    def backward_out(is_last):
        reduce("q", qb, qr, qacc)
        inner = dot_over_units()
        inverse = rkeep[:, :1]
        if is_last:
            logit = rkeep[:, 1:2] + inverse * inner
            seed = rinfo[:, 0:1] * jnp.exp(logit - rinfo[:, 1:2])
            scale = seed * inverse
            pj[t, blk(j)] = (scale * pacc[...]).astype(BF)
        else:
            seed = jnp.ones((rows, 1), F32)
            scale = inverse
        gq[t, blk(j)] = (scale * qacc[...]).astype(BF)
        sc[j] = pack([inverse * inverse * inverse * (seed * inner) / width, seed])
        share("gq", gq, True)
        others(lambda b: send("sc", b, j, sc.at[j], sc.at[j], {"dp": b}))
        got("w", 0, w1o)

        def chunk(b):
            shared("gq", gq, b)

            @pl.when(b != j)
            def _():
                got("sc", b, sc.at[b])
            packed = unpack(sc[b])
            grad = dot(gq[t, blk(b)], w1[t], 1, 1) + dot(gq[o, blk(b)], w1o[...], 1, 1)
            upstream = us[t, blk(b)].astype(F32)
            if is_last:
                upstream = packed[:, 1:2] * upstream
            yg[blk(b)] = (
                upstream + gain(t) * grad - packed[:, 0:1] * xs[t, blk(b)].astype(F32)
            ).astype(BF)
            send("g", b, b, yg.at[blk(b)], us.at[t, blk(b)], {"section": s - 1})
        everyone(chunk)

    def tokens():
        others(lambda b: got("tk", b, tk.at[b]))
        count = tk[0]
        for b in range(1, n):
            count = count + tk[b]
        return 1.0 / count[0:1, 0:1]

    def finish_value(scale):
        for h in range(2):
            dw1[h] = dot(xg[h], gq[t], 0, 0) * scale

    def finish_value_arriving(scale):
        def add(b, start):
            for h in range(2):
                part = dot(xg[h, blk(b)], gq[t, blk(b)], 0, 0) * scale
                dw1[h] = part if start else dw1[h] + part
        add(j, True)

        def later(b):
            got("gq", b, gq.at[t, blk(b)])
            add(b, False)
        others(later)

    def finish_output(scale):
        for h in range(2):
            dw2[:, h * half:(h + 1) * half] = dot(pj[t], us[h], 0, 0) * scale

    def drain_common():
        sent("w", 0, w1o)
        sent("w", 1, w2o)

        def one(b):
            sent("tk", b, tk.at[b])
            sent("p", b, pb.at[blk(b)])
            sent("ps", b, ps.at[b])
            sent("q", b, qb.at[blk(b)])
            sent("pj", b, pj.at[t, blk(b)])
            sent("gq", b, gq.at[t, blk(b)])
        others(one)

    def first_section():
        start_common()
        all_to_all(xs)
        forward_chunk(j, False)

        def chunk(b):
            arrive("a", "xf", xs, b)
            forward_chunk(b, False)
        others(chunk)
        forward_out()

        def back(b):
            arrive("g", "uf", us, b)
            backward_chunk(b)
        everyone(back)
        scale = tokens()
        reduce("q", qb, qr, qacc)
        gq[t, blk(j)] = (rkeep[:, :1] * qacc[...]).astype(BF)
        share("gq", gq, False)
        finish_output(scale)
        finish_value_arriving(scale)
        got("w", 0, w1o)
        drain_common()

        def rest(b):
            sent("a", b, src.at[0])
            sent("xf", b, xs.at[t, blk(b)])
        others(rest)

        def rest_all(b):
            sent("pjf", b, pj.at[t, blk(b)])
            sent("x", b, yx.at[blk(b)])
            sent("uf", b, us.at[t, blk(b)])
        everyone(rest_all)

    def middle_section():
        start_common()

        def chunk(b):
            arrive("x", "xf", xs, b)
            forward_chunk(b, False)
        everyone(chunk)
        forward_out()

        def back(b):
            arrive("g", "uf", us, b)
            backward_chunk(b)
        everyone(back)
        backward_out(False)
        scale = tokens()
        finish_output(scale)
        finish_value(scale)
        drain_common()
        sent("e", 0, exs)
        others(lambda b: sent("sc", b, sc.at[b]))

        def rest_all(b):
            sent("xf", b, xs.at[t, blk(b)])
            sent("uf", b, us.at[t, blk(b)])
            sent("pjf", b, pj.at[t, blk(b)])
            sent("gqf", b, gq.at[t, blk(b)])
            sent("x", b, yx.at[blk(b)])
            sent("g", b, yg.at[blk(b)])
        everyone(rest_all)

    def last_section():
        start_common()
        all_to_all(us)
        backward_chunk(j)
        row_info()

        def seeds(b):
            arrive("a", "uf", us, b)
            backward_chunk(b)
        others(seeds)

        def chunk(b):
            arrive("x", "xf", xs, b)
            forward_chunk(b, True)
        everyone(chunk)
        own_inverse()
        reduce("p", pb, pr, pacc)
        backward_out(True)
        share("pj", pj, False)
        scale = tokens()
        finish_value(scale)
        others(lambda b: got("pj", b, pj.at[t, blk(b)]))
        finish_output(scale)
        got("w", 1, w2o)
        drain_common()
        sent("e", 0, exs)

        def rest(b):
            sent("a", b, src.at[0])
            sent("uf", b, us.at[t, blk(b)])
            sent("sc", b, sc.at[b])
        others(rest)

        def rest_all(b):
            sent("xf", b, xs.at[t, blk(b)])
            sent("gqf", b, gq.at[t, blk(b)])
            sent("g", b, yg.at[blk(b)])
        everyone(rest_all)

    pl.when(s == 0)(first_section)
    pl.when(s == last)(last_section)
    if sections > 2:
        pl.when((s > 0) & (s < last))(middle_section)


def local_chain(
    hidden, unembed, value_proj, output_proj, norm_gains, survive, lengths, assign,
    advantage, reference_logit, recorded_gap,
):
    n = lax.axis_size("dp")
    sections = lax.axis_size("section")
    s = lax.axis_index("section")
    count, positions, width = hidden.shape
    rows = count * positions
    part = value_proj.shape[1]
    half = part // 2
    v = value_proj.shape[2]

    src = jnp.where(s == sections - 1, unembed, hidden).reshape(rows, n * 2, half)
    src = src.transpose(1, 0, 2)
    w1 = value_proj[0].reshape(2, half, v)
    w2 = output_proj[0].reshape(v, 2, half).transpose(1, 0, 2)
    gains = norm_gains[0].reshape(n * 2, 1, half)
    total = n * rows
    kinds = len(KINDS)
    vm = pl.BlockSpec(memory_space=pltpu.VMEM)
    dw1, dw2 = pl.pallas_call(
        functools.partial(kernel, n, sections, width),
        out_shape=(
            jax.ShapeDtypeStruct((2, half, v), F32),
            jax.ShapeDtypeStruct((v, part), F32),
        ),
        in_specs=[vm] * 10,
        out_specs=(vm, vm),
        scratch_shapes=[
            pltpu.VMEM((2, total, half), BF),
            pltpu.VMEM((2, total, half), BF),
            pltpu.VMEM((2, total, half), BF),
            pltpu.VMEM((total, v), BF),
            pltpu.VMEM((n, rows, v), BF),
            pltpu.VMEM((total, v), BF),
            pltpu.VMEM((n, rows, v), BF),
            pltpu.VMEM((2, total, v), BF),
            pltpu.VMEM((2, total, v), BF),
            pltpu.VMEM((n, 8, rows), F32),
            pltpu.VMEM((half, v), BF),
            pltpu.VMEM((v, half), BF),
            pltpu.VMEM((total, half), BF),
            pltpu.VMEM((total, half), BF),
            pltpu.VMEM((n, 8, LANES), F32),
            pltpu.VMEM((rows, LANES), F32),
            pltpu.VMEM((rows, LANES), F32),
            pltpu.VMEM((rows, v), F32),
            pltpu.VMEM((rows, v), F32),
            pltpu.VMEM((rows, LANES), F32),
            pltpu.VMEM((n, 8, rows), F32),
            pltpu.VMEM((n, 8, rows), F32),
            pltpu.VMEM((rows, LANES), F32),
            pltpu.VMEM((8, LANES), F32),
            pltpu.SemaphoreType.DMA((kinds, n)),
            pltpu.SemaphoreType.DMA((kinds, n)),
        ],
        compiler_params=pltpu.CompilerParams(
            collective_id=0, has_side_effects=True, vmem_limit_bytes=60 * 1024 * 1024
        ),
    )(
        src, w1, w2, gains, survive.reshape(1, -1), lengths.reshape(1, count),
        assign.reshape(1, count), advantage.reshape(1, count), reference_logit.T, recorded_gap.T,
    )
    return (
        dw1.reshape(1, part, v),
        dw2[None],
    )


def pair_slots(n):
    sizes = {
        "a": n, "af": n, "ax": n, "axf": n, "bx": 1, "bf": 1, "by": 1, "ax1": 1, "af1": 1, "ay": 1, "gn": 1,
        "mr": 1, "mk": n, "my": 1, "rr": 3 * n, "rl": 3 * n, "ps": 1, "p0": 2, "s0": 1, "in": 2, "w": 2,
        "d1": 2, "s1": 1, "g0": n, "g0x": n, "g0f": 1, "g1": n, "gx": n, "g1f": 1, "g2": 1, "gs": 1, "tk": 1,
        "g0r": 0,
    }
    starts, total = {}, 0
    for kind, size in sizes.items():
        starts[kind] = total
        total += size
    return list(sizes), starts, total


def pair_kernel(
    n, width,
    hid, une, w1, w2, gains, survive, lengths, assign, advantage, base, gap,
    dw1, dw2,
    xs, us, xg, wv1, wv2, b0f, a1f, b0g, gx, mp, mr, mk, part, own, rin, p0, dp1, gz, ga, gb, gc,
    wr, wsend, ps, psr, scs, scr, inn, inr, sc, rinfo, tok, tk,
    ss, rs, ls,
):
    j = lax.axis_index("dp")
    s = lax.axis_index("section")
    t = lax.axis_index("tensor")
    y = lax.axis_index("groups")
    o = 1 - t
    rows = hid.shape[0]
    chunk, v = w1.shape
    half = chunk // 2
    mb = v // n
    positions, count = base.shape
    partner = {"tensor": o}
    right = {"dp": j + 1}
    left = {"dp": j - 1}
    lane = lax.broadcasted_iota(jnp.int32, (rows, LANES), 1)
    kinds, starts, _ = pair_slots(n)
    near = max(n // 2, 1)
    relayed = n == 2 * near and 0 < near * (near - 1) <= n
    side = j // near
    gate = jnp.where(side == 0, near - 1, near)
    most = pl.ds(0, (n - 1) * rows)

    def blk(b):
        return pl.ds(pl.multiple_of(b * rows, rows), rows)

    def cols(h):
        return pl.ds(pl.multiple_of(h * half, half), half)

    def wide(b, h):
        return pl.ds(pl.multiple_of(b * chunk + h * half, half), half)

    def mrows(g, b):
        return pl.ds(pl.multiple_of(g * v + b * mb, mb), mb)

    def send(kind, ri, a, b, dev, through=""):
        slot = kinds.index("rr" if kind == "rl" else kind + through)
        if kind in ("mr", "my", "ps", "g0f", "g1f", "g2", "gs", "tk"):
            ri = 0
        pltpu.make_async_remote_copy(
            src_ref=a, dst_ref=b, send_sem=ss.at[slot], recv_sem=rs.at[starts[kind] + ri],
            device_id=dev, device_id_type=pl.DeviceIdType.MESH,
        ).start()

    def got(kind, i, a):
        pltpu.make_async_remote_copy(
            src_ref=a, dst_ref=a, send_sem=ss.at[kinds.index(kind)], recv_sem=rs.at[starts[kind] + i],
            device_id=partner, device_id_type=pl.DeviceIdType.MESH,
        ).wait_recv()

    def sent(kind, a):
        pltpu.make_async_remote_copy(
            src_ref=a, dst_ref=a, send_sem=ss.at[kinds.index(kind)], recv_sem=rs.at[0],
            device_id=partner, device_id_type=pl.DeviceIdType.MESH,
        ).wait_send()

    def others(body):
        def step(k, carry):
            body(lax.rem(j + k, n))
            return carry
        lax.fori_loop(1, n, step, 0)

    def at_distance(d, body):
        pl.when(j + d < n)(lambda: body(j + d))
        pl.when(j - d >= 0)(lambda: body(j - d))

    def pack(values):
        packed = jnp.zeros((rows, LANES), F32)
        for i, value in enumerate(values):
            packed = jnp.where(lane == i, value, packed)
        return packed.T[:8]

    def unpack(packed):
        return jnp.concatenate([packed, jnp.zeros((LANES - 8, rows), F32)], axis=0).T

    def own_tokens():
        response = lax.broadcasted_iota(jnp.int32, (1, count), 1)
        group = count // survive.shape[1]
        kept = jnp.zeros((1, count), F32)
        for g in range(survive.shape[1]):
            inside = (response >= g * group) & (response < (g + 1) * group)
            kept = jnp.where(inside, survive[0:1, g:g + 1].astype(F32), kept)
        held = jnp.sum(kept * lengths[...].astype(F32), axis=1, keepdims=True)
        tok[...] = jnp.broadcast_to(held, (8, LANES))
        others(lambda b: send("tk", j, tok, tk.at[j], {"dp": b}))
        tk[j] = tok[...]

    def tokens():
        got("tk", 0, tk.at[pl.ds(0, n - 1)])
        total = tk[0]
        for b in range(1, n):
            total = total + tk[b]
        return 1.0 / total[0:1, 0:1]

    def row_info():
        row = lax.broadcasted_iota(jnp.int32, (rows, count), 0)
        first = lax.broadcasted_iota(jnp.int32, (rows, count), 1) * positions
        mine = (row >= first) & (row < first + positions)

        def by_response(values):
            return jnp.sum(jnp.where(mine, values, 0.0), axis=1, keepdims=True)

        def by_position(values):
            return by_response(jnp.concatenate([values] * count, axis=0))

        slots = assign[...]
        starts = slots * positions
        hit = (row >= starts) & (row < starts + positions)
        listed = jnp.sum(jnp.where(hit, 1.0, 0.0), axis=1, keepdims=True)
        start = by_response(first.astype(F32))
        place = lax.broadcasted_iota(jnp.int32, (rows, 1), 0).astype(F32) - start
        live = place < by_response(lengths[...].astype(F32))
        adv = by_response(advantage[...])
        q = by_position(gap[...])
        clipped = ((adv > 0) & (q > clip_high)) | ((adv < 0) & (q < clip_low))
        weight = jnp.where(clipped | (~live), 0.0, -loss_scale * adv * listed)
        rinfo[...] = jnp.where(lane == 0, weight, jnp.where(lane == 1, by_position(base[...]), 0.0))

    def local_copy(i, a, b):
        return pltpu.make_async_copy(a, b, ls.at[i])

    def reduce_step(q, d, at_end):
        slot = q * n

        def onward(kind, way, r, dev):
            if not at_end:
                got(kind, slot + r, rin.at[way, q, r])
                part[q, r] = (part[q, r].astype(F32) + rin[way, q, r].astype(F32)).astype(BF)
            send(kind, slot + r, part.at[q, r], rin.at[way, q, r], dev)

        first = j == 0 if at_end else (j > 0) & (j + d < n)
        final = j == n - 1 if at_end else (j < n - 1) & (j - d >= 0)
        pl.when(first)(lambda: onward("rr", 0, j + d, right))
        pl.when(final)(lambda: onward("rl", 1, j - d, left))

    def reduce_inner(q, most, least=1):
        for d in range(most, least - 1, -1):
            reduce_step(q, d, False)

    def reduce_own(q):
        slot = q * n + j

        @pl.when(j > 0)
        def _():
            got("rr", slot, rin.at[0, q, j])
            own[q] += rin[0, q, j].astype(F32)

        @pl.when(j < n - 1)
        def _():
            got("rl", slot, rin.at[1, q, j])
            own[q] += rin[1, q, j].astype(F32)

    def gather(kind, at):
        for d in range(n - 1, 0, -1):
            at_distance(d, lambda b: send(kind, j, at(j), at(j), {"dp": b}))

    def gather_near(kind, at):
        if not relayed:
            return gather(kind, at)
        across = jnp.where(side == 0, near, near - 1)
        for d in range(n - 1, 0, -1):
            at_distance(d, lambda b: pl.when((b // near == side) | (b == across))(
                lambda: send(kind, j, at(j), at(j), {"dp": b})
            ))

    def hand_on(kind, at):
        if not relayed:
            return

        def one(b):
            got(kind, b, at(b))
            for r in range(n):
                pl.when((r // near == side) & (r != j))(
                    lambda: send(kind, b, at(b), at(b), {"dp": r}, "r")
                )
        for d in range(1, n):
            at_distance(d, lambda b: pl.when((j == gate) & (b // near != side))(lambda: one(b)))

    def handed(kind, at, b):
        if not relayed:
            return got(kind, b, at(b))
        pl.when((j != gate) | (b // near == side))(lambda: got(kind, b, at(b)))

    def gather_sent(kind, whole):
        if not relayed:
            return sent(kind, whole.at[most])
        sent(kind, whole.at[pl.ds(0, near * rows)])
        pl.when(j == gate)(lambda: sent(kind + "r", whole.at[pl.ds(0, near * (near - 1) * rows)]))

    def at_p0(b):
        return p0.at[t, blk(b)]

    def at_dp1(b):
        return dp1.at[t, blk(b)]

    def at_gz(b):
        return gz.at[blk(b)]

    def scalar_sums():
        psr[j] = ps[j]
        got("ps", 0, psr.at[pl.ds(0, n - 1)])
        sums = psr[0]
        for b in range(1, n):
            sums = sums + psr[b]
        return unpack(sums)[:, 0:1]

    def gram_send():
        others(lambda b: send("mr", j, mp.at[b], mr.at[j], {"dp": b}))

    def gram_reduce():
        mr[j] = mp[j]
        got("mr", 0, mr.at[pl.ds(0, n - 1)])
        total = mr[0].astype(F32)
        for b in range(1, n):
            total = total + mr[b].astype(F32)
        mk[mrows(y, j)] = total.astype(BF)
        here = mk.at[mrows(y, j)]
        others(lambda b: send("mk", j, here, here, {"dp": b}))
        send("my", j, here, here, {"groups": 1 - y})

    def gram_pass():
        def across(b):
            here = mk.at[mrows(y, b)]
            got("mk", b, here)
            send("my", b, here, here, {"groups": 1 - y})
        others(across)

    def gram_wait():
        got("my", 0, mk.at[pl.ds(0, n * mb)])

    def store_gram(value):
        value = value.astype(BF)
        for b in range(n):
            mp[b] = value[b * mb:(b + 1) * mb]

    def main_send(src, main, d):
        at_distance(d, lambda b: send(
            "a", j, src.at[:, wide(b, t)], main.at[blk(j), cols(t)], {"dp": b}
        ))

    def main_start(src, other_src, main, other):
        for d in range(n - 1, 1, -1):
            main_send(src, main, d)
        local_copy(0, src.at[:, pl.ds(pl.multiple_of(j * chunk, chunk), chunk)], main.at[blk(j)]).start()
        local_copy(1, other_src.at[:, pl.ds(pl.multiple_of(j * chunk, chunk), chunk)], other.at[blk(j)]).start()

    def main_wait(src, other_src, main, other):
        local_copy(0, src.at[:, pl.ds(0, chunk)], main.at[blk(j)]).wait()
        local_copy(1, other_src.at[:, pl.ds(0, chunk)], other.at[blk(j)]).wait()

    def main_arrive(main, d):
        def first(b):
            here = main.at[blk(b), cols(t)]
            got("a", b, here)
            send("ax", b, here, here, {"section": 1 - s})
            send("af", b, here, here, partner)
        at_distance(d, first)
        at_distance(d, lambda b: got("af", b, main.at[blk(b), cols(o)]))

    def other_take(other):
        def first(b):
            here = other.at[blk(b), cols(t)]
            got("ax", b, here)
            send("axf", b, here, here, partner)
        for d in range(n - 1, 0, -1):
            at_distance(d, first)

    def other_arrive(other, d):
        at_distance(d, lambda b: got("axf", b, other.at[blk(b), cols(o)]))

    barrier = pltpu.get_barrier_semaphore()

    def greet(dev):
        pl.semaphore_signal(barrier, inc=1, device_id=dev, device_id_type=pl.DeviceIdType.MESH)

    def meet():
        others(lambda b: greet({"dp": b}))
        greet({"groups": 1 - y})
        greet(partner)
        greet({"section": 1 - s})
        greet({"section": 1 - s, "tensor": o})
        pl.semaphore_wait(barrier, n + 3)

    def drain_common(main, other, sums):
        for kind in ("a", "ax", "af"):
            sent(kind, main.at[most, pl.ds(0, half)])
        sent("axf", other.at[most, pl.ds(0, half)])
        sent("mr", mp.at[pl.ds(0, n - 1)])
        sent("mk", mk.at[pl.ds(0, (n - 1) * mb)])
        sent("my", mk.at[pl.ds(0, n * mb)])
        sent("ps", ps.at[pl.ds(0, n - 1)])
        sent("tk", tk.at[pl.ds(0, n - 1)])
        sent("gs", sc.at[pl.ds(0, n - 1)])
        sent("rr", part.at[pl.ds(0, sums), pl.ds(0, n - 1)])
        sent("g0f", gz.at[most])
        sent("bf", b0f.at[t])

    def first_section():
        local_copy(2, w1, wv1).start()
        local_copy(3, w2, b0f.at[t]).start()
        meet()
        @pl.when(t == y)
        def _():
            send("bx", 0, w2, b0f.at[t], {"section": 1})
        main_start(hid, une, xs, us)
        send("bf", 0, w2, b0f.at[t], partner)
        own_tokens()
        row_info()
        local_copy(2, w1, wv1).wait()
        local_copy(3, w2, b0f.at[t]).wait()
        main_wait(hid, une, xs, us)

        def project(b):
            x = xs[blk(b)].astype(F32)
            ps[b] = pack([jnp.sum(x * x, axis=1, keepdims=True)])
            xg[blk(b)] = (x * gains[j]).astype(BF)
            return dot(xg[blk(b)], wv1[...]), dot(xs[blk(b)], b0f[t], 1, 1)

        def project_main(b):
            pa, pb = project(b)
            part[0, b] = pa.astype(BF)
            part[1, b] = pb.astype(BF)
            send("ps", j, ps.at[b], psr.at[j], {"dp": b})

        def project_other(b):
            part[2, b] = dot(us[blk(b)], b0f[t], 1, 1).astype(BF)

        own[0], own[1] = project(j)
        own[2] = dot(us[blk(j)], b0f[t], 1, 1)
        got("bf", 0, b0f.at[o])
        store_gram(dot(b0f[y], b0f[t], 1, 1))
        gram_send()
        main_send(hid, xs, 1)
        for d in range(n - 1, 0, -1):
            main_arrive(xs, d)
            at_distance(d, project_main)
            reduce_step(0, d, True)
            reduce_step(1, d, True)
        reduce_inner(0, n - 2)
        reduce_inner(1, n - 2, 2)
        gram_reduce()
        other_take(us)
        for d in range(n - 1, 0, -1):
            other_arrive(us, d)
            at_distance(d, project_other)
            reduce_step(2, d, True)
        reduce_inner(1, 1)
        reduce_own(0)
        xx = scalar_sums()
        inverse = lax.rsqrt(xx / width + eps_norm)
        p0[t, blk(j)] = (inverse * own[0]).astype(BF)
        send("p0", t, at_p0(j), at_p0(j), partner)
        for c in range(2):
            send("p0", t, at_p0(j), at_p0(j), {"section": 1, "tensor": c})
        reduce_inner(2, n - 2, 2)
        gram_pass()
        reduce_inner(2, 1)
        gather_near("g0", at_p0)

        @pl.when(t == y)
        def _():
            got("ax1", 0, a1f.at[t])
            send("ay", 0, a1f.at[t], a1f.at[t], {"groups": 1 - y})
            send("af1", 0, a1f.at[t], a1f.at[t], partner)
        hand_on("g0", at_p0)
        reduce_own(1)
        reduce_own(2)
        gram_wait()
        got("p0", o, p0.at[o, blk(j)])
        kb = own[1] + dot(p0[0, blk(j)], mk[0:v]) + dot(p0[1, blk(j)], mk[v:2 * v])
        p0v = p0[t, blk(j)].astype(F32)
        scs[...] = pack([
            jnp.sum(p0v * (own[1] + kb), axis=1, keepdims=True),
            jnp.sum(p0v * own[2], axis=1, keepdims=True),
        ])
        send("s0", 0, scs, scr, partner)
        own[1] = kb
        got("w", 0, wr.at[0])
        got("w", 1, wr.at[1])
        got("in", 0, inr.at[0])
        got("in", 1, inr.at[1])
        got("s0", 0, scr)
        sums = unpack(scs[...] + scr[...])
        squares = xx + sums[:, 0:1]
        raised_inverse = lax.rsqrt(jnp.maximum(squares, 0.0) / width + eps_norm)
        inner = unpack(inr[0] + inr[1])[:, 0:2]
        logit = 0.5 * inner[:, 1:2] + sums[:, 1:2] + raised_inverse * inner[:, 0:1]
        weight = rinfo[:, 0:1]
        seed = jnp.where(weight == 0.0, 0.0, weight * jnp.exp(logit - rinfo[:, 1:2]))
        scaled = seed * raised_inverse
        pull = raised_inverse * raised_inverse * raised_inverse * (seed * inner[:, 0:1]) / width
        grad = seed * own[2] - pull * own[1] + scaled * (wr[0].astype(F32) + wr[1].astype(F32))
        gz[blk(j)] = (inverse * grad).astype(BF)
        sc[j] = pack([seed, scaled, pull])
        send("s1", 0, sc.at[j], sc.at[j], {"section": 1})
        others(lambda b: send("gs", j, sc.at[j], sc.at[j], {"dp": b}))
        gather("g2", at_gz)

        def pass_p0(b):
            handed("g0", at_p0, b)
            send("g0f", b, at_p0(b), at_p0(b), partner)
            send("g0x", b, at_p0(b), at_p0(b), {"section": 1})
        for d in range(1, n):
            at_distance(d, pass_p0)
        scale = tokens()
        got("gs", 0, sc.at[pl.ds(0, n - 1)])
        got("g0f", 0, p0.at[o, most])
        for b in range(n):
            packed = unpack(sc[b])
            held = p0[t, blk(b)].astype(F32)
            for h in range(2):
                gb[h, blk(b)] = (-packed[:, 2:3] * p0[h, blk(b)].astype(F32)).astype(BF)
            ga[blk(b)] = (packed[:, 0:1] * held).astype(BF)
            gc[blk(b)] = (packed[:, 1:2] * held).astype(BF)
        dw2[...] = dot(ga[...], us[...], 0, 0) + dot(gb[t], xs[...], 0, 0)
        for h in range(2):
            dw2[...] += dot(dot(p0[t], gb[h], 0, 0).astype(BF), b0f[h])

        @pl.when(t != y)
        def _():
            got("ay", 0, a1f.at[t])
            send("af1", 0, a1f.at[t], a1f.at[t], partner)
        got("gn", 0, gx)

        def pass_dp1(b):
            got("gx", b, at_dp1(b))
            send("g1f", b, at_dp1(b), at_dp1(b), partner)
        for d in range(1, n):
            at_distance(d, pass_dp1)
        got("d1", t, at_dp1(j))
        got("d1", o, dp1.at[o, blk(j)])
        got("af1", 0, a1f.at[o])
        got("g1f", 0, dp1.at[o, most])
        through = jnp.zeros((v, chunk), F32)
        for h in range(2):
            through += dot(dot(gc[...], dp1[h], 0, 0).astype(BF), a1f[h], 1, 1)
        dw2[...] = (dw2[...] + gx[...] * through) * scale
        got("g2", 0, gz.at[most])
        dw1[...] = dot(xg[...], gz[...], 0, 0) * scale
        drain_common(xs, us, 3)

        @pl.when(t == y)
        def _():
            sent("bx", b0f.at[t])
            sent("ay", a1f.at[t])
        sent("af1", a1f.at[t])
        sent("p0", part.at[:, 0])
        sent("s0", scs)
        sent("s1", scs)
        gather_sent("g0", gz)
        sent("g2", gz.at[most])
        sent("g0x", gz.at[most])
        sent("g1f", gz.at[most])

    def second_section():
        local_copy(2, w1, a1f.at[t]).start()
        local_copy(3, w2, wv2).start()
        meet()
        main_start(une, hid, us, xs)
        own_tokens()
        local_copy(2, w1, a1f.at[t]).wait()
        local_copy(3, w2, wv2).wait()
        main_wait(une, hid, us, xs)

        def project_main(b):
            part[0, b] = dot(us[blk(b)], wv2[...], 1, 1).astype(BF)

        def project(b):
            x = xs[blk(b)].astype(F32)
            ps[b] = pack([jnp.sum(x * us[blk(b)].astype(F32), axis=1, keepdims=True)])
            xg[blk(b)] = (x * gains[j]).astype(BF)
            return dot(xg[blk(b)], a1f[t])

        def project_other(b):
            part[1, b] = project(b).astype(BF)
            send("ps", j, ps.at[b], psr.at[j], {"dp": b})

        own[0] = dot(us[blk(j)], wv2[...], 1, 1)
        own[1] = project(j)
        main_send(une, us, 1)

        def take_b0():
            @pl.when(t == y)
            def _():
                got("bx", 0, b0f.at[t])
                send("bf", 0, b0f.at[t], b0f.at[t], partner)
                send("by", 0, b0f.at[t], b0f.at[t], {"groups": 1 - y})

            @pl.when(t != y)
            def _():
                got("bf", 0, b0f.at[o])

        def take_rest():
            @pl.when(t != y)
            def _():
                got("by", 0, b0f.at[t])
                send("bf", 0, b0f.at[t], b0f.at[t], partner)

            @pl.when(t == y)
            def _():
                got("bf", 0, b0f.at[o])

        for d in range(n - 1, 0, -1):
            main_arrive(us, d)
            at_distance(d, project_main)
            reduce_step(0, d, True)
            if d == min(2, n - 1):
                take_b0()
                b0g[y] = (b0f[y].astype(F32) * gains[j]).astype(BF)
                store_gram(dot(b0g[y], a1f[t]))
                gram_send()
        @pl.when(t == y)
        def _():
            send("ax1", 0, w1, a1f.at[t], {"section": 0})
        send("gn", 0, gains.at[j], gx, {"section": 0})
        reduce_inner(0, n - 2)
        gram_reduce()
        other_take(xs)
        for d in range(n - 1, 0, -1):
            other_arrive(xs, d)
            at_distance(d, project_other)
            reduce_step(1, d, True)
        reduce_inner(1, n - 2, 2)
        gram_pass()
        reduce_inner(1, 1)
        reduce_own(0)
        dp1[t, blk(j)] = own[0].astype(BF)
        gram_wait()
        back = dot(dp1[t, blk(j)], mk[...], 1, 1).astype(BF)
        for c in range(2):
            wsend[c] = back[:, c * v:(c + 1) * v]
            send("w", t, wsend.at[c], wr.at[t], {"section": 0, "tensor": c})
        reduce_own(1)
        dotted = scalar_sums()
        gather("g1", at_dp1)
        got("p0", 0, p0.at[0, blk(j)])
        got("p0", 1, p0.at[1, blk(j)])
        raised = own[1] + dot(p0[0, blk(j)], mk[0:v]) + dot(p0[1, blk(j)], mk[v:2 * v])
        inn[...] = pack([jnp.sum(raised * own[0], axis=1, keepdims=True), dotted])
        for c in range(2):
            send("in", t, inn, inr.at[t], {"section": 0, "tensor": c})
        for c in range(2):
            send("d1", t, at_dp1(j), at_dp1(j), {"section": 0, "tensor": c})
        gz[blk(j)] = raised.astype(BF)
        gather("g2", at_gz)

        def pass_dp1(b):
            got("g1", b, at_dp1(b))
            send("gx", b, at_dp1(b), at_dp1(b), {"section": 0})

        for d in range(1, n):
            at_distance(d, pass_dp1)
        got("s1", 0, sc.at[j])
        others(lambda b: send("gs", j, sc.at[j], sc.at[j], {"dp": b}))
        take_rest()
        for h in range(2):
            b0g[h] = (b0f[h].astype(F32) * gains[j]).astype(BF)
        scale = tokens()

        def pass_p0(b):
            got("g0x", b, at_p0(b))
            send("g0f", b, at_p0(b), at_p0(b), partner)
        for d in range(1, n):
            at_distance(d, pass_p0)
        got("g0f", 0, p0.at[o, most])
        got("g2", 0, gz.at[most])
        got("gs", 0, sc.at[pl.ds(0, n - 1)])
        for b in range(n):
            scaled = unpack(sc[b])[:, 1:2]
            ga[blk(b)] = (scaled * gz[blk(b)].astype(F32)).astype(BF)
            gc[blk(b)] = (scaled * dp1[t, blk(b)].astype(F32)).astype(BF)
        dw2[...] = dot(ga[...], us[...], 0, 0) * scale
        total = dot(xg[...], gc[...], 0, 0)
        for h in range(2):
            total += dot(b0g[h], dot(p0[h], gc[...], 0, 0).astype(BF), 0, 0)
        dw1[...] = total * scale
        drain_common(us, xs, 2)

        @pl.when(t == y)
        def _():
            sent("ax1", a1f.at[t])
            sent("by", b0f.at[t])
        sent("gn", gx)
        sent("g1", gz.at[most])
        sent("g2", gz.at[most])
        sent("gx", ga.at[most])
        sent("in", inr)
        sent("w", wsend)
        sent("d1", part.at[pl.ds(0, 2), 0])

    pl.when(s == 0)(first_section)
    pl.when(s == 1)(second_section)


def local_pair(
    hidden, unembed, value_proj, output_proj, norm_gains, survive, lengths, assign,
    advantage, reference_logit, recorded_gap,
):
    n = lax.axis_size("dp")
    count, positions, width = hidden.shape
    rows = count * positions
    chunk, v = value_proj.shape[1:]
    total = n * rows
    kinds, _, slots = pair_slots(n)
    vm = pl.BlockSpec(memory_space=pltpu.VMEM)
    hbm = pl.BlockSpec(memory_space=pl.ANY)
    dw1, dw2 = pl.pallas_call(
        functools.partial(pair_kernel, n, width),
        out_shape=(
            pltpu.VMEM((chunk, v), F32),
            pltpu.VMEM((v, chunk), F32),
        ),
        in_specs=[hbm] * 4 + [vm] * 7,
        out_specs=(vm, vm),
        scratch_shapes=[
            pltpu.VMEM((total, chunk), BF),
            pltpu.VMEM((total, chunk), BF),
            pltpu.VMEM((total, chunk), BF),
            pltpu.VMEM((chunk, v), BF),
            pltpu.VMEM((v, chunk), BF),
            pltpu.VMEM((2, v, chunk), BF),
            pltpu.VMEM((2, chunk, v), BF),
            pltpu.VMEM((2, v, chunk), BF),
            pltpu.VMEM((1, chunk), F32),
            pltpu.VMEM((n, v // n, v), BF),
            pltpu.VMEM((n, v // n, v), BF),
            pltpu.VMEM((2 * v, v), BF),
            pltpu.VMEM((3, n, rows, v), BF),
            pltpu.VMEM((3, rows, v), F32),
            pltpu.VMEM((2, 3, n, rows, v), BF),
            pltpu.VMEM((2, total, v), BF),
            pltpu.VMEM((2, total, v), BF),
            pltpu.VMEM((total, v), BF),
            pltpu.VMEM((total, v), BF),
            pltpu.VMEM((2, total, v), BF),
            pltpu.VMEM((total, v), BF),
            pltpu.VMEM((2, rows, v), BF),
            pltpu.VMEM((2, rows, v), BF),
            pltpu.VMEM((n, 8, rows), F32),
            pltpu.VMEM((n, 8, rows), F32),
            pltpu.VMEM((8, rows), F32),
            pltpu.VMEM((8, rows), F32),
            pltpu.VMEM((8, rows), F32),
            pltpu.VMEM((2, 8, rows), F32),
            pltpu.VMEM((n, 8, rows), F32),
            pltpu.VMEM((rows, LANES), F32),
            pltpu.VMEM((8, LANES), F32),
            pltpu.VMEM((n, 8, LANES), F32),
            pltpu.SemaphoreType.DMA((len(kinds),)),
            pltpu.SemaphoreType.DMA((slots,)),
            pltpu.SemaphoreType.DMA((4,)),
        ],
        compiler_params=pltpu.CompilerParams(
            collective_id=0, has_side_effects=True, vmem_limit_bytes=60 * 1024 * 1024
        ),
    )(
        hidden.reshape(rows, width), unembed.reshape(rows, width), value_proj[0], output_proj[0],
        norm_gains[0].reshape(n, 1, chunk), survive.reshape(1, -1), lengths.reshape(1, count),
        assign.reshape(1, count), advantage.reshape(1, count), reference_logit.T, recorded_gap.T,
    )
    return dw1[None], dw2[None]


def solution(mesh):
    rowwise = P(("groups", "dp"))
    placed = (
        P(("groups", "dp"), None, None),
        P(("groups", "dp"), None, None),
        P("section", "dp", "tensor"),
        P("section", "tensor", "dp"),
        P("section", None),
        rowwise,
        rowwise,
        rowwise,
        rowwise,
        P(("groups", "dp"), None),
        P(("groups", "dp"), None),
    )
    shape = mesh.shape
    paired = shape["section"] == 2 and shape["tensor"] == 2 and shape["groups"] == 2
    return jax.shard_map(
        local_pair if paired else local_chain,
        mesh=mesh,
        in_specs=placed,
        out_specs=(
            P(("groups", "section"), "dp", "tensor"),
            P(("groups", "section"), "tensor", "dp"),
        ),
        check_vma=False,
    )
```
